32 devices in a mesh: ap: 16 (over z, x, core), pass: 2 (over y).
Axes of the slice: x: 2, y: 2, z: 4, core: 2. Of those that a mesh axis runs over, the one named last changes fastest.
Arguments:
- echo_record: bfloat16 [2, 16, 2048, 512], P(None, 'pass', 'ap'), may hold values from -6 to 6
- along_track_kernel: bfloat16 [2, 1024, 2048], P(None, None, 'ap'), may hold values from -0.125 to 0.125
- slant_distance_kernel: bfloat16 [2, 512, 256], replicated, may hold values from -0.1875 to 0.1875
- vertical_lags: int32 [16], P('pass'), may hold values from 0 to 128
- lateral_lags: int32 [16], P('pass'), may hold values from 0 to 32
- orbit_source_survey: int32 [16], replicated, may hold values from 0 to 15, each once
- normal_spacings: float32 [16], replicated, may hold values from -1 to 1
Outputs:
- profile: float32 [2, 1024, 256, 512], P(None, ('ap', 'pass'))
The draws below stay inside these ranges and needn't reach their ends.
All inputs are finite; a program needn't handle non-finite values.
Results may differ from the reference program's by a relative error of at most 0.02.
Values may be sent and summed in bfloat16 or wider, within the bound.
A program may use at most 192 MiB of HBM per device.

```python
import jax
import jax.numpy as jnp
from jax import lax

ORBIT_SUM = 16
PULSES = 2048
FREQS = 512
ROWS = 1024
COLS = 256
HEIGHT_CELLS = 512
ITERS = 4
COL_MAX = 32
OFF_MAX = 128


def touch_ends(entries, rng, low, largest):
    index_at = [jax.random.randint(jax.random.fold_in(rng, axis), (), 0, length) for axis, length in enumerate(entries.shape)]
    widest = entries.shape.index(max(entries.shape))
    neighbour = index_at[:widest] + [(index_at[widest] + 1) % entries.shape[widest]] + index_at[widest + 1:]
    return entries.at[tuple(index_at)].set(low).at[tuple(neighbour)].set(largest)


def raised(entries, stream_key, source, target, blocks, factor):
    def block_of(position):
        return (jnp.arange(entries.shape[position]) // (entries.shape[position] // blocks)).reshape((-1,) + (1,) * (entries.ndim - 1 - position))

    near = jax.random.permutation(stream_key, blocks)[block_of(target)]
    other_side = (block_of(target) + blocks // 2) % blocks
    return jnp.where((block_of(source) == near) | (block_of(source) == other_side), factor * entries, entries)


def level_of(rng, dims, cuts, least, largest):
    loudness = 1.0
    for position, parts in cuts:
        draws = jax.random.uniform(jax.random.fold_in(jax.random.fold_in(rng, 6), position), (parts,), jnp.float32, least / len(cuts), largest / len(cuts))
        loudness = loudness * jnp.repeat(jnp.exp(draws), dims[position] // parts).reshape((-1,) + (1,) * (len(dims) - 1 - position))
    return loudness


def normal_values(own_key, extent, width, reach, shards=(), kind=jnp.bfloat16):
    result = jax.random.normal(own_key, extent, jnp.float32) * width
    if len(shards) > 0:
        result = level_of(own_key, extent, shards, -0.22, 0.18) * result
    return jnp.clip(result, min=-reach, max=reach).astype(kind)


def bell_draw_with(key, shape, spread, bound, split, heavy, held_as=jnp.bfloat16):
    array = spread * jax.random.normal(key, shape, jnp.float32)
    if split:
        array = array * level_of(key, shape, split, -0.22, 0.18)
    return jnp.clip(raised(array, jax.random.fold_in(key, 3), *heavy), -bound, bound).astype(held_as)


def setup_inputs(seed: int = 0) -> dict:
    key_of = jax.random.split(jax.random.key(seed), 8)
    return {
        "echo_record": normal_values(key_of[0], (2, ORBIT_SUM, PULSES, FREQS), 1.0, 6.0, ((1, 2), (2, 16))),
        "along_track_kernel": bell_draw_with(key_of[1], (2, ROWS, PULSES), (2 * PULSES) ** -0.5, 0.125, ((2, 16),), (2, 1, 16, 2.0)),
        "slant_distance_kernel": normal_values(key_of[2], (2, FREQS, COLS), (2 * FREQS) ** -0.5, 0.1875),
        "vertical_lags": touch_ends(jax.random.randint(key_of[3], (ORBIT_SUM,), 0, OFF_MAX + 1), jax.random.fold_in(key_of[3], 1), 0, OFF_MAX).astype(jnp.int32),
        "lateral_lags": touch_ends(jax.random.randint(key_of[4], (ORBIT_SUM,), 0, COL_MAX + 1), jax.random.fold_in(key_of[4], 1), 0, COL_MAX).astype(jnp.int32),
        "orbit_source_survey": jax.random.permutation(key_of[5], ORBIT_SUM).astype(jnp.int32),
        "normal_spacings": jnp.clip(jax.random.uniform(key_of[6], (ORBIT_SUM,), jnp.float32, -1.0, 1.0), -1.0, 1.0),
    }


shrink_level = 0.1


def phasor_dictionary(normal_spacings, orbit_source_survey, height_cell_number):
    chosen_height_cells = normal_spacings[orbit_source_survey]
    orbit_start_positions = jnp.arange(height_cell_number).astype(normal_spacings.dtype) - height_cell_number // 2
    phases = jnp.pi * chosen_height_cells[:, None] * orbit_start_positions[None, :]
    return jnp.cos(phases), jnp.sin(phases)


def shrink_steps(obs_re, obs_im, inphase_phasor_part, quadrature_phasor_part):
    passes = inphase_phasor_part.shape[0]
    height_cell_number = inphase_phasor_part.shape[1]
    precise = lax.Precision.HIGHEST
    prof_re = jnp.zeros((obs_re.shape[0], height_cell_number), jnp.float32)
    prof_im = jnp.zeros((obs_re.shape[0], height_cell_number), jnp.float32)
    for sweep_index in range(ITERS):
        if sweep_index == 0:
            resid_re = obs_re
            resid_im = obs_im
        else:
            pred_re = jnp.dot(prof_re, inphase_phasor_part.T, precision=precise) - jnp.dot(prof_im, quadrature_phasor_part.T, precision=precise)
            pred_im = jnp.dot(prof_re, quadrature_phasor_part.T, precision=precise) + jnp.dot(prof_im, inphase_phasor_part.T, precision=precise)
            resid_re = obs_re - pred_re / height_cell_number
            resid_im = obs_im - pred_im / height_cell_number
        grad_re = jnp.dot(resid_re, inphase_phasor_part, precision=precise) + jnp.dot(resid_im, quadrature_phasor_part, precision=precise)
        grad_im = jnp.dot(resid_im, inphase_phasor_part, precision=precise) - jnp.dot(resid_re, quadrature_phasor_part, precision=precise)
        moved_re = prof_re + grad_re / passes
        moved_im = prof_im + grad_im / passes
        prof_re = moved_re - jnp.clip(moved_re, -shrink_level, shrink_level)
        prof_im = moved_im - jnp.clip(moved_im, -shrink_level, shrink_level)
    return prof_re, prof_im


def reference(echo_record, along_track_kernel, slant_distance_kernel, vertical_lags, lateral_lags, orbit_source_survey, normal_spacings):
    def form_pass(inputs):
        planes, row_offset, col_offset = inputs
        focus_re = (jnp.dot(planes[0], slant_distance_kernel[0], preferred_element_type=jnp.float32)
                    - jnp.dot(planes[1], slant_distance_kernel[1], preferred_element_type=jnp.float32)).astype(jnp.bfloat16)
        focus_im = (jnp.dot(planes[0], slant_distance_kernel[1], preferred_element_type=jnp.float32)
                    + jnp.dot(planes[1], slant_distance_kernel[0], preferred_element_type=jnp.float32)).astype(jnp.bfloat16)
        image_re = (jnp.dot(along_track_kernel[0], focus_re, preferred_element_type=jnp.float32)
                    - jnp.dot(along_track_kernel[1], focus_im, preferred_element_type=jnp.float32))
        image_im = (jnp.dot(along_track_kernel[0], focus_im, preferred_element_type=jnp.float32)
                    + jnp.dot(along_track_kernel[1], focus_re, preferred_element_type=jnp.float32))
        stacked = jnp.stack([image_re, image_im])
        padded = jnp.pad(stacked, ((0, 0), (OFF_MAX, 0), (COL_MAX, 0)))
        starts = (jnp.int32(0), (OFF_MAX - row_offset).astype(jnp.int32), (COL_MAX - col_offset).astype(jnp.int32))
        return lax.dynamic_slice(padded, starts, (2, ROWS, COLS)).astype(jnp.bfloat16)

    aligned = lax.map(form_pass, (jnp.moveaxis(echo_record, 1, 0), vertical_lags, lateral_lags))
    inphase_phasor_part, quadrature_phasor_part = phasor_dictionary(normal_spacings, orbit_source_survey, HEIGHT_CELLS)
    blocks = 16
    block_rows = ROWS // blocks
    grouped = jnp.moveaxis(aligned.reshape(ORBIT_SUM, 2, blocks, block_rows * COLS), 2, 0)

    def solve_block(portion):
        values = portion.astype(jnp.float32)
        prof_re, prof_im = shrink_steps(values[:, 0].T, values[:, 1].T, inphase_phasor_part, quadrature_phasor_part)
        return jnp.stack([prof_re, prof_im])

    solved = lax.map(solve_block, grouped)
    return jnp.moveaxis(solved, 1, 0).reshape(2, ROWS, COLS, HEIGHT_CELLS)
```

```python
import functools

import jax
import jax.numpy as jnp
from jax import lax
from jax.experimental import pallas as pl
from jax.experimental.pallas import tpu as pltpu
from jax.sharding import PartitionSpec as P

HEIGHT_CELLS = 512
ITERS = 4
SPAN = 2
CHUNKS = 4

shrink_level = 0.1


def phasor_dictionary(normal_spacings, orbit_source_survey, height_cell_number):
    support_mask = (
        orbit_source_survey[:, None]
        == jnp.arange(normal_spacings.shape[0], dtype=jnp.int32)[None, :]
    ).astype(normal_spacings.dtype)
    chosen_height_cells = jnp.sum(support_mask * normal_spacings[None, :], axis=1)
    orbit_start_positions = (
        jnp.arange(height_cell_number).astype(normal_spacings.dtype) - height_cell_number // 2
    )
    phases = jnp.pi * chosen_height_cells[:, None] * orbit_start_positions[None, :]
    return (jnp.cos(phases), jnp.sin(phases))


def focus_kernel(lags_ref, echo_ref, slant_ref, out_ref):
    dot = functools.partial(jnp.dot, preferred_element_type=jnp.float32)
    echo_re, echo_im = echo_ref[0, 0], echo_ref[1, 0]
    slant_re, slant_im = slant_ref[0], slant_ref[1]
    lag = lags_ref[pl.program_id(0)]
    focus_re = dot(echo_re, slant_re) - dot(echo_im, slant_im)
    focus_im = dot(echo_re, slant_im) + dot(echo_im, slant_re)
    inside = lax.broadcasted_iota(jnp.int32, focus_re.shape, 1) >= lag
    for plane, values in enumerate((focus_re, focus_im)):
        moved = jnp.where(inside, pltpu.roll(values, lag, 1), 0.0)
        out_ref[plane, 0] = moved.astype(out_ref.dtype)


def focus_range(echo, slant, lateral_lags):
    _, passes, pulses, freqs = echo.shape
    cols = slant.shape[2]
    return pl.pallas_call(
        focus_kernel,
        grid_spec=pltpu.PrefetchScalarGridSpec(
            num_scalar_prefetch=1,
            grid=(passes,),
            in_specs=[
                pl.BlockSpec((2, 1, pulses, freqs), lambda p, lags: (0, p, 0, 0)),
                pl.BlockSpec((2, freqs, cols), lambda p, lags: (0, 0, 0)),
            ],
            out_specs=pl.BlockSpec((2, 1, pulses, cols), lambda p, lags: (0, p, 0, 0)),
        ),
        out_shape=jax.ShapeDtypeStruct((2, passes, pulses, cols), jnp.bfloat16),
        cost_estimate=pl.CostEstimate(
            flops=8 * passes * pulses * freqs * cols,
            bytes_accessed=6 * passes * pulses * freqs,
            transcendentals=0,
        ),
        name="focus",
    )(lateral_lags, echo, slant)


def image_kernel(direct, chunks, pass_count, strip, margin, lags_ref, side_ref, *refs):
    kernels, focuses = refs[0:2], refs[2:4]
    outs, padded = refs[4:-1], refs[-1]
    owners = kernels[0].shape[1] // strip // 2
    rows = kernels[0].shape[1]
    pulses = kernels[0].shape[2]
    cols = outs[0].shape[-1]

    @pl.when(pl.program_id(0) == 0)
    def _():
        for s in range(2):
            for plane in range(2):
                padded[2 * s + plane, 0:margin, :] = jnp.zeros((margin, pulses), jnp.float32)
                padded[2 * s + plane, margin : margin + rows, :] = kernels[s][plane].astype(
                    jnp.float32
                )

    base = margin - lags_ref[pl.program_id(0)] + side_ref[0] * strip
    half = strip // pass_count
    starts = []
    for o in range(owners):
        if direct:
            first = base + 2 * lax.rem(side_ref[1] + o, owners) * strip
            for q in range(pass_count):
                starts.append((first + lax.rem(side_ref[2] + q, pass_count) * half, half))
        else:
            starts.append((base + 2 * o * strip, strip))
    total_re = jnp.zeros((owners * strip, cols), jnp.float32)
    total_im = jnp.zeros((owners * strip, cols), jnp.float32)
    dot = functools.partial(jnp.dot, preferred_element_type=jnp.float32)
    for s in range(2):
        kernel_re, kernel_im = (
            jnp.concatenate(
                [padded[2 * s + plane, pl.ds(start, size), :] for start, size in starts],
                axis=0,
            ).astype(jnp.bfloat16)
            for plane in range(2)
        )
        focus_re, focus_im = focuses[s][0, 0], focuses[s][1, 0]
        if pulses % 128 == 0:
            both = jnp.concatenate([kernel_re, kernel_im], axis=1)
            total_re += dot(both, jnp.concatenate([focus_re, -focus_im], axis=0))
            total_im += dot(both, jnp.concatenate([focus_im, focus_re], axis=0))
        else:
            total_re += dot(kernel_re, focus_re) - dot(kernel_im, focus_im)
            total_im += dot(kernel_re, focus_im) + dot(kernel_im, focus_re)
    height = strip // pass_count // chunks
    for plane, total in enumerate((total_re, total_im)):
        if chunks == 1 and not direct:
            outs[0][:, plane, 0] = total.reshape(owners, strip, cols).astype(jnp.bfloat16)
        else:
            split = total.reshape(owners, pass_count, chunks, height, cols)
            for c in range(chunks):
                part = split[:, :, c].reshape(owners, pass_count * height, cols)
                part = part.astype(jnp.bfloat16)
                if direct:
                    for o in range(owners):
                        outs[c * owners + o][plane, 0] = part[o]
                else:
                    outs[c][:, plane, 0] = part


def form_images(direct, kernel, kernel_far, focus, focus_far, vertical_lags, side, chunks, pass_count, strip):
    _, rows, pulses = kernel.shape
    passes, cols = focus.shape[1], focus.shape[3]
    owners = rows // strip // 2
    margin = SPAN * strip
    piece = strip // chunks
    whole = pl.BlockSpec((2, rows, pulses), lambda p, *_: (0, 0, 0))
    one = pl.BlockSpec((2, 1, pulses, cols), lambda p, *_: (0, p, 0, 0))
    if direct:
        out_specs = [pl.BlockSpec((2, 1, piece, cols), lambda p, *_: (0, p, 0, 0))]
        out_shape = [jax.ShapeDtypeStruct((2, passes, piece, cols), jnp.bfloat16)]
        out_specs, out_shape = out_specs * (chunks * owners), out_shape * (chunks * owners)
    else:
        out_specs = [pl.BlockSpec((owners, 2, 1, piece, cols), lambda p, *_: (0, 0, p, 0, 0))]
        out_shape = [jax.ShapeDtypeStruct((owners, 2, passes, piece, cols), jnp.bfloat16)]
        out_specs, out_shape = out_specs * chunks, out_shape * chunks
    return pl.pallas_call(
        functools.partial(image_kernel, direct, chunks, pass_count, strip, margin),
        grid_spec=pltpu.PrefetchScalarGridSpec(
            num_scalar_prefetch=2,
            grid=(passes,),
            in_specs=[whole, whole, one, one],
            out_specs=out_specs,
            scratch_shapes=[pltpu.VMEM((4, margin + rows, pulses), jnp.float32)],
        ),
        out_shape=out_shape,
        cost_estimate=pl.CostEstimate(
            flops=8 * passes * pulses * rows * cols,
            bytes_accessed=2 * passes * rows * cols,
            transcendentals=0,
        ),
        name="image",
    )(vertical_lags, side, kernel, kernel_far, focus, focus_far)


def shrink_kernel(rows_at_once, y_ref, grad_ref, pred_ref, *refs):
    out_ref = refs[-1]
    cells = out_ref.shape[3]
    cols = out_ref.shape[2]
    width = grad_ref.shape[0]
    block = width // 4
    dot = functools.partial(jnp.dot, preferred_element_type=jnp.float32)
    coarse = (lax.broadcasted_iota(jnp.int32, (cols, width), 1) // block) % 2 == 0
    observed = []
    for i in range(rows_at_once):
        y = y_ref[:, i * cols : (i + 1) * cols].astype(jnp.float32)
        observed.append(jnp.concatenate([y] * 4, axis=0).T)
    resid = list(observed)
    for sweep in range(ITERS):
        for i in range(rows_at_once):
            high = resid[i].astype(jnp.bfloat16)
            low = (resid[i] - high.astype(jnp.float32)).astype(jnp.bfloat16)
            moving = jnp.where(coarse, high, low)
            planes = []
            for plane in range(2):
                v = dot(moving, grad_ref[:, plane * cells : (plane + 1) * cells])
                if sweep > 0:
                    v += out_ref[plane, i]
                u = v - jnp.clip(v, -shrink_level, shrink_level)
                out_ref[plane, i] = u
                planes.append(u.astype(jnp.bfloat16))
            if sweep < ITERS - 1:
                resid[i] = observed[i] - dot(jnp.concatenate(planes, axis=1), pred_ref[...])


def shrink_chunk(c, chunks, y, grad, pred, profile, shape):
    _, rows, cols, cells = shape
    height = rows // chunks
    rows_at_once = 2 if height % 2 == 0 else 1
    steps = height // rows_at_once
    width, span = grad.shape
    specs = [
        pl.BlockSpec((y.shape[0], rows_at_once * cols), lambda i: (0, i)),
        pl.BlockSpec((width, span), lambda i: (0, 0)),
        pl.BlockSpec((span, width), lambda i: (0, 0)),
    ]
    operands = [y, grad, pred]
    aliases = {}
    if profile is not None:
        specs.append(pl.BlockSpec(memory_space=pl.ANY))
        operands.append(profile)
        aliases = {3: 0}
    return pl.pallas_call(
        functools.partial(shrink_kernel, rows_at_once),
        grid=(steps,),
        in_specs=specs,
        out_specs=pl.BlockSpec(
            (2, rows_at_once, cols, cells), lambda i: (0, c * steps + i, 0, 0)
        ),
        out_shape=jax.ShapeDtypeStruct(shape, jnp.float32),
        input_output_aliases=aliases,
        cost_estimate=pl.CostEstimate(
            flops=7 * 2 * height * cols * span * 256,
            bytes_accessed=8 * height * cols * cells,
            transcendentals=0,
        ),
        name="shrink_%d" % c,
    )(*operands)


def split_high_low(matrix):
    high = matrix.astype(jnp.bfloat16)
    return high, (matrix - high.astype(jnp.float32)).astype(jnp.bfloat16)


def body(
    echo_record,
    along_track_kernel,
    slant_distance_kernel,
    vertical_lags,
    lateral_lags,
    orbit_source_survey,
    normal_spacings,
):
    ap_count = lax.axis_size("ap")
    pass_count = lax.axis_size("pass")
    rows = along_track_kernel.shape[1]
    cols = slant_distance_kernel.shape[2]
    strip = rows // ap_count
    own_rows = strip // pass_count
    chunks = max(1, min(CHUNKS, own_rows // 8))
    passes = normal_spacings.shape[0]
    swap = [(i, i ^ 1) for i in range(ap_count)]
    same_side = [[i for i in range(ap_count) if i % 2 == side] for side in range(2)]

    kernel_far = lax.ppermute(along_track_kernel, "ap", swap)
    focus = focus_range(echo_record, slant_distance_kernel, lateral_lags)
    focus_far = lax.ppermute(focus, "ap", swap)
    place, own_pass = lax.axis_index("ap"), lax.axis_index("pass")
    side = jnp.stack([place % 2, place // 2, own_pass]).astype(jnp.int32)
    direct = pass_count == 2 and own_rows % 8 == 0
    if direct:
        orbit_source_survey = jnp.where(
            own_pass == 0, orbit_source_survey, jnp.roll(orbit_source_survey, passes // 2)
        )
    pieces = form_images(
        direct, along_track_kernel, kernel_far, focus, focus_far, vertical_lags, side,
        chunks, pass_count, strip,
    )

    inphase, quadrature = phasor_dictionary(normal_spacings, orbit_source_survey, HEIGHT_CELLS)
    adjoint = (
        jnp.concatenate(
            [
                jnp.concatenate([inphase, -quadrature], axis=1),
                jnp.concatenate([quadrature, inphase], axis=1),
            ],
            axis=0,
        )
    )
    grad_high, grad_low = split_high_low(adjoint / passes)
    grad = jnp.concatenate([grad_high, grad_high, grad_low, grad_low], axis=0)
    forward = (adjoint.T / HEIGHT_CELLS).astype(jnp.bfloat16)
    pred = jnp.concatenate([forward] * 4, axis=1)

    profile = None
    shape = (2, own_rows, cols, HEIGHT_CELLS)
    if direct:
        owners = ap_count // 2
        height = strip // chunks // 2
        arrived = []
        for c in range(chunks):
            received = [pieces[c * owners]]
            for d in range(1, owners):
                ring = [(i, (i + 2 * d) % ap_count) for i in range(ap_count)]
                received.append(lax.ppermute(pieces[c * owners + d], "ap", ring))
            arrived.append(received)
        for c, received in enumerate(arrived):
            if c > 0:
                received, profile = lax.optimization_barrier((received, profile))
            summed = sum(r.astype(jnp.float32) for r in received).astype(jnp.bfloat16)
            theirs = lax.ppermute(summed[:, :, height:], "pass", [(0, 1), (1, 0)])
            stacked = jnp.concatenate([summed[:, :, :height], theirs], axis=1)
            y = stacked.reshape(2 * passes, -1)
            if profile is not None:
                y, profile = lax.optimization_barrier((y, profile))
            profile = shrink_chunk(c, chunks, y, grad, pred, profile, shape)
        return profile
    arrived = []
    for piece in pieces:
        arrived.append(
            lax.all_to_all(
                piece, "ap", split_axis=0, concat_axis=0, axis_index_groups=same_side
            )
        )
    for c, received in enumerate(arrived):
        if profile is not None:
            received, profile = lax.optimization_barrier((received, profile))
        summed = jnp.sum(received.astype(jnp.float32), axis=0).astype(jnp.bfloat16)
        stacked = lax.all_to_all(summed, "pass", split_axis=2, concat_axis=1, tiled=True)
        y = stacked.reshape(2 * passes, -1)
        profile = shrink_chunk(c, chunks, y, grad, pred, profile, shape)
    return profile


def solution(mesh):
    return jax.shard_map(
        body,
        mesh=mesh,
        in_specs=(
            P(None, "pass", "ap", None),
            P(None, None, "ap"),
            P(),
            P("pass"),
            P("pass"),
            P(),
            P(),
        ),
        out_specs=P(None, ("ap", "pass"), None, None),
        check_vma=False,
    )
```

```python
import functools

import jax
import jax.numpy as jnp
from jax import lax
from jax.experimental import pallas as pl
from jax.experimental.pallas import tpu as pltpu
from jax.sharding import PartitionSpec as P

HEIGHT_CELLS = 512
ITERS = 4
SPAN = 2
CHUNKS = 4
EARLY = 3
MESH = pl.DeviceIdType.MESH

shrink_level = 0.1


def phasor_dictionary(normal_spacings, orbit_source_survey, height_cell_number):
    support_mask = (
        orbit_source_survey[:, None]
        == jnp.arange(normal_spacings.shape[0], dtype=jnp.int32)[None, :]
    ).astype(normal_spacings.dtype)
    chosen_height_cells = jnp.sum(support_mask * normal_spacings[None, :], axis=1)
    orbit_start_positions = (
        jnp.arange(height_cell_number).astype(normal_spacings.dtype) - height_cell_number // 2
    )
    phases = jnp.pi * chosen_height_cells[:, None] * orbit_start_positions[None, :]
    return (jnp.cos(phases), jnp.sin(phases))


def focus_kernel(lags_ref, echo_ref, slant_ref, out_ref):
    dot = functools.partial(jnp.dot, preferred_element_type=jnp.float32)
    echo_re, echo_im = echo_ref[0, 0], echo_ref[1, 0]
    slant_re, slant_im = slant_ref[0], slant_ref[1]
    lag = lags_ref[pl.program_id(0)]
    focus_re = dot(echo_re, slant_re) - dot(echo_im, slant_im)
    focus_im = dot(echo_re, slant_im) + dot(echo_im, slant_re)
    inside = lax.broadcasted_iota(jnp.int32, focus_re.shape, 1) >= lag
    for plane, values in enumerate((focus_re, focus_im)):
        moved = jnp.where(inside, pltpu.roll(values, lag, 1), 0.0)
        out_ref[plane, 0] = moved.astype(out_ref.dtype)


def focus_range(echo, slant, lateral_lags):
    _, passes, pulses, freqs = echo.shape
    cols = slant.shape[2]
    return pl.pallas_call(
        focus_kernel,
        grid_spec=pltpu.PrefetchScalarGridSpec(
            num_scalar_prefetch=1,
            grid=(passes,),
            in_specs=[
                pl.BlockSpec((2, 1, pulses, freqs), lambda p, lags: (0, p, 0, 0)),
                pl.BlockSpec((2, freqs, cols), lambda p, lags: (0, 0, 0)),
            ],
            out_specs=pl.BlockSpec((2, 1, pulses, cols), lambda p, lags: (0, p, 0, 0)),
        ),
        out_shape=jax.ShapeDtypeStruct((2, passes, pulses, cols), jnp.bfloat16),
        cost_estimate=pl.CostEstimate(
            flops=8 * passes * pulses * freqs * cols,
            bytes_accessed=6 * passes * pulses * freqs,
            transcendentals=0,
        ),
        name="focus",
    )(lateral_lags, echo, slant)


def image_kernel(direct, chunks, pass_count, strip, margin, lags_ref, side_ref, *refs):
    kernels, focuses = refs[0:2], refs[2:4]
    outs, padded = refs[4:-1], refs[-1]
    owners = kernels[0].shape[1] // strip // 2
    rows = kernels[0].shape[1]
    pulses = kernels[0].shape[2]
    cols = outs[0].shape[-1]

    @pl.when(pl.program_id(0) == 0)
    def _():
        for s in range(2):
            for plane in range(2):
                padded[2 * s + plane, 0:margin, :] = jnp.zeros((margin, pulses), jnp.float32)
                padded[2 * s + plane, margin : margin + rows, :] = kernels[s][plane].astype(
                    jnp.float32
                )

    base = margin - lags_ref[pl.program_id(0)] + side_ref[0] * strip
    half = strip // pass_count
    starts = []
    for o in range(owners):
        if direct:
            first = base + 2 * lax.rem(side_ref[1] + o, owners) * strip
            for q in range(pass_count):
                starts.append((first + lax.rem(side_ref[2] + q, pass_count) * half, half))
        else:
            starts.append((base + 2 * o * strip, strip))
    total_re = jnp.zeros((owners * strip, cols), jnp.float32)
    total_im = jnp.zeros((owners * strip, cols), jnp.float32)
    dot = functools.partial(jnp.dot, preferred_element_type=jnp.float32)
    for s in range(2):
        kernel_re, kernel_im = (
            jnp.concatenate(
                [padded[2 * s + plane, pl.ds(start, size), :] for start, size in starts],
                axis=0,
            ).astype(jnp.bfloat16)
            for plane in range(2)
        )
        focus_re, focus_im = focuses[s][0, 0], focuses[s][1, 0]
        if pulses % 128 == 0:
            both = jnp.concatenate([kernel_re, kernel_im], axis=1)
            total_re += dot(both, jnp.concatenate([focus_re, -focus_im], axis=0))
            total_im += dot(both, jnp.concatenate([focus_im, focus_re], axis=0))
        else:
            total_re += dot(kernel_re, focus_re) - dot(kernel_im, focus_im)
            total_im += dot(kernel_re, focus_im) + dot(kernel_im, focus_re)
    height = strip // pass_count // chunks
    for plane, total in enumerate((total_re, total_im)):
        if chunks == 1 and not direct:
            outs[0][:, plane, 0] = total.reshape(owners, strip, cols).astype(jnp.bfloat16)
        else:
            split = total.reshape(owners, pass_count, chunks, height, cols)
            for c in range(chunks):
                part = split[:, :, c].reshape(owners, pass_count * height, cols)
                part = part.astype(jnp.bfloat16)
                if direct:
                    for o in range(owners):
                        outs[c * owners + o][plane, 0] = part[o]
                else:
                    outs[c][:, plane, 0] = part


def form_images(direct, kernel, kernel_far, focus, focus_far, vertical_lags, side, chunks, pass_count, strip):
    _, rows, pulses = kernel.shape
    passes, cols = focus.shape[1], focus.shape[3]
    owners = rows // strip // 2
    margin = SPAN * strip
    piece = strip // chunks
    whole = pl.BlockSpec((2, rows, pulses), lambda p, *_: (0, 0, 0))
    one = pl.BlockSpec((2, 1, pulses, cols), lambda p, *_: (0, p, 0, 0))
    if direct:
        out_specs = [pl.BlockSpec((2, 1, piece, cols), lambda p, *_: (0, p, 0, 0))]
        out_shape = [jax.ShapeDtypeStruct((2, passes, piece, cols), jnp.bfloat16)]
        out_specs, out_shape = out_specs * (chunks * owners), out_shape * (chunks * owners)
    else:
        out_specs = [pl.BlockSpec((owners, 2, 1, piece, cols), lambda p, *_: (0, 0, p, 0, 0))]
        out_shape = [jax.ShapeDtypeStruct((owners, 2, passes, piece, cols), jnp.bfloat16)]
        out_specs, out_shape = out_specs * chunks, out_shape * chunks
    return pl.pallas_call(
        functools.partial(image_kernel, direct, chunks, pass_count, strip, margin),
        grid_spec=pltpu.PrefetchScalarGridSpec(
            num_scalar_prefetch=2,
            grid=(passes,),
            in_specs=[whole, whole, one, one],
            out_specs=out_specs,
            scratch_shapes=[pltpu.VMEM((4, margin + rows, pulses), jnp.float32)],
        ),
        out_shape=out_shape,
        cost_estimate=pl.CostEstimate(
            flops=8 * passes * pulses * rows * cols,
            bytes_accessed=2 * passes * rows * cols,
            transcendentals=0,
        ),
        name="image",
    )(vertical_lags, side, kernel, kernel_far, focus, focus_far)


def shrink_kernel(rows_at_once, y_ref, grad_ref, pred_ref, *refs):
    out_ref = refs[-1]
    cells = out_ref.shape[3]
    cols = out_ref.shape[2]
    width = grad_ref.shape[0]
    block = width // 4
    dot = functools.partial(jnp.dot, preferred_element_type=jnp.float32)
    coarse = (lax.broadcasted_iota(jnp.int32, (cols, width), 1) // block) % 2 == 0
    observed = []
    for i in range(rows_at_once):
        y = y_ref[:, i * cols : (i + 1) * cols].astype(jnp.float32)
        observed.append(jnp.concatenate([y] * 4, axis=0).T)
    resid = list(observed)
    for sweep in range(ITERS):
        for i in range(rows_at_once):
            high = resid[i].astype(jnp.bfloat16)
            low = (resid[i] - high.astype(jnp.float32)).astype(jnp.bfloat16)
            moving = jnp.where(coarse, high, low)
            planes = []
            for plane in range(2):
                v = dot(moving, grad_ref[:, plane * cells : (plane + 1) * cells])
                if sweep > 0:
                    v += out_ref[plane, i]
                u = v - jnp.clip(v, -shrink_level, shrink_level)
                out_ref[plane, i] = u
                planes.append(u.astype(jnp.bfloat16))
            if sweep < ITERS - 1:
                resid[i] = observed[i] - dot(jnp.concatenate(planes, axis=1), pred_ref[...])


def shrink_chunk(c, chunks, y, grad, pred, profile, shape):
    _, rows, cols, cells = shape
    height = rows // chunks
    rows_at_once = 2 if height % 2 == 0 else 1
    steps = height // rows_at_once
    width, span = grad.shape
    specs = [
        pl.BlockSpec((y.shape[0], rows_at_once * cols), lambda i: (0, i)),
        pl.BlockSpec((width, span), lambda i: (0, 0)),
        pl.BlockSpec((span, width), lambda i: (0, 0)),
    ]
    operands = [y, grad, pred]
    aliases = {}
    if profile is not None:
        specs.append(pl.BlockSpec(memory_space=pl.ANY))
        operands.append(profile)
        aliases = {3: 0}
    return pl.pallas_call(
        functools.partial(shrink_kernel, rows_at_once),
        grid=(steps,),
        in_specs=specs,
        out_specs=pl.BlockSpec(
            (2, rows_at_once, cols, cells), lambda i: (0, c * steps + i, 0, 0)
        ),
        out_shape=jax.ShapeDtypeStruct(shape, jnp.float32),
        input_output_aliases=aliases,
        cost_estimate=pl.CostEstimate(
            flops=7 * 2 * height * cols * span * 256,
            bytes_accessed=8 * height * cols * cells,
            transcendentals=0,
        ),
        name="shrink_%d" % c,
    )(*operands)


def shrink_pixels(observed, grad_ref, pred_ref, state):
    cells = state[0].shape[-1]
    pixels, width = observed[0].shape
    dot = functools.partial(jnp.dot, preferred_element_type=jnp.float32)
    coarse = (lax.broadcasted_iota(jnp.int32, (pixels, width), 1) // (width // 4)) % 2 == 0
    resid = list(observed)
    last = [[None, None] for _ in observed]
    for sweep in range(ITERS):
        for i in range(len(observed)):
            high = resid[i].astype(jnp.bfloat16)
            low = (resid[i] - high.astype(jnp.float32)).astype(jnp.bfloat16)
            moving = jnp.where(coarse, high, low)
            planes = []
            for plane in range(2):
                v = dot(moving, grad_ref[:, plane * cells : (plane + 1) * cells])
                if sweep > 0:
                    v += state[i][plane]
                u = v - jnp.clip(v, -shrink_level, shrink_level)
                if sweep < ITERS - 1:
                    state[i][plane] = u
                    planes.append(u.astype(jnp.bfloat16))
                else:
                    last[i][plane] = u
            if sweep < ITERS - 1:
                resid[i] = observed[i] - dot(jnp.concatenate(planes, axis=1), pred_ref[...])
    return last


def gather_kernel(
    sizes, lags_ref, kernel_near, kernel_far, focus_near, focus_far, grad_ref, pred_ref,
    early_ref, rest_ref,
    padded, keep, send, land, mid, zland, ysend, yland, ready, state, result,
    x_out, x_in, z_out, z_in, y_out, y_in, flush,
):
    strip, own_rows, margin, levels, groups, halves, early = sizes
    rows, pulses = kernel_near.shape[1:]
    passes = focus_near.shape[1]
    place, plane_y = lax.axis_index("ap"), lax.axis_index("pass")
    core, x, z = place % 2, (place // 2) % 2, place // 4
    peer_x = (place + 2 - 4 * x, plane_y)
    peer_y = (place, 1 - plane_y)
    peers_z = [(lax.rem(z + d, levels) * 4 + place % 4, plane_y) for d in range(levels)]
    barrier = pltpu.get_barrier_semaphore()
    for peer in [peer_x, peer_y] + peers_z[1:]:
        pl.semaphore_signal(barrier, inc=1, device_id=peer, device_id_type=MESH)
    pl.semaphore_wait(barrier, levels + 1)

    for s, ref in enumerate((kernel_near, kernel_far)):
        for plane in range(2):
            padded[2 * s + plane, 0:margin, :] = jnp.zeros((margin, pulses), jnp.float32)
            padded[2 * s + plane, margin : margin + rows, :] = ref[plane].astype(jnp.float32)

    def copy_x(c):
        return pltpu.make_async_remote_copy(
            src_ref=send.at[c], dst_ref=land.at[c], send_sem=x_out.at[c], recv_sem=x_in.at[c],
            device_id=peer_x, device_id_type=MESH,
        )

    def copy_z(c, d):
        return pltpu.make_async_remote_copy(
            src_ref=mid.at[c, d - 1], dst_ref=zland.at[c, d - 1],
            send_sem=z_out.at[c, d - 1], recv_sem=z_in.at[c, d - 1],
            device_id=peers_z[d], device_id_type=MESH,
        )

    def copy_y(c):
        return pltpu.make_async_remote_copy(
            src_ref=ysend.at[c], dst_ref=yland.at[c], send_sem=y_out.at[c], recv_sem=y_in.at[c],
            device_id=peer_y, device_id_type=MESH,
        )

    dot = functools.partial(jnp.dot, preferred_element_type=jnp.float32)

    def form(g):
        def one(p, carry):
            base = margin - lags_ref[p] + g * 8
            starts = []
            for side in range(2):
                for d in range(levels):
                    owner = lax.rem(z + d, levels) * 4 + lax.rem(x + side, 2) * 2 + core
                    for q in range(2):
                        starts.append(base + owner * strip + lax.rem(plane_y + q, 2) * own_rows)
            parts = []
            for n in range(4):
                parts.append(
                    jnp.concatenate([padded[n, pl.ds(start, 8), :] for start in starts], axis=0)
                    .astype(jnp.bfloat16)
                )
            taken = jnp.concatenate(parts, axis=1)
            near_re, near_im = focus_near[0, p], focus_near[1, p]
            far_re, far_im = focus_far[0, p], focus_far[1, p]
            out_re = dot(taken, jnp.concatenate([near_re, -near_im, far_re, -far_im], axis=0))
            out_im = dot(taken, jnp.concatenate([near_im, near_re, far_im, far_re], axis=0))
            for plane, out in enumerate((out_re, out_im)):
                out = out.astype(jnp.bfloat16)
                n = 0
                for buffer in (keep, send):
                    for d in range(levels):
                        for q in range(2):
                            for h in range(halves):
                                buffer[g * halves + h, d, q, plane, p] = out[
                                    8 * n : 8 * n + 8, 128 * h : 128 * h + 128
                                ]
                            n += 1
            return carry

        lax.fori_loop(0, passes, one, 0)

    def reduce_x(c):
        copy_x(c).wait()
        for d in range(1, levels):
            total = keep[c, d].astype(jnp.float32) + land[c, d].astype(jnp.float32)
            mid[c, d - 1] = total.astype(jnp.bfloat16)
        for d in range(1, levels):
            copy_z(c, d).start()

    def reduce_z(c):
        for d in range(1, levels):
            copy_z(c, d).wait()
        total = keep[c, 0].astype(jnp.float32) + land[c, 0].astype(jnp.float32)
        for d in range(1, levels):
            total += zland[c, d - 1].astype(jnp.float32)
        total = total.astype(jnp.bfloat16)
        ysend[c] = total[1]
        copy_y(c).start()
        ready[c, :, 0] = total[0].astype(jnp.float32)

    def finish(c):
        copy_y(c).wait()
        ready[c, :, 1] = yland[c].astype(jnp.float32)

    def observe(c, r):
        y = ready[c, :, :, :, r, :].reshape(4 * passes, 128)
        return jnp.concatenate([y] * 4, axis=0).T

    def flushed(slot):
        return pltpu.make_async_copy(
            result.at[slot], early_ref.at[:, pl.ds(0, 4), pl.ds(0, 128), :], flush.at[slot]
        )

    def shrink(c):
        g, h = c // halves, c % halves

        def pair(i, carry):
            slot = i % 2

            @pl.when(c * 2 + i >= 2)
            def _():
                flushed(slot).wait()

            observed = []
            for k in range(2):
                observed.append(
                    jnp.concatenate(
                        [observe(c, i * 4 + 2 * k), observe(c, i * 4 + 2 * k + 1)], axis=0
                    )
                )
            last = shrink_pixels(observed, grad_ref, pred_ref, [state.at[0], state.at[1]])
            for k in range(2):
                for plane in range(2):
                    u = last[k][plane].astype(jnp.bfloat16)
                    result[slot, plane, 2 * k] = u[0:128]
                    result[slot, plane, 2 * k + 1] = u[128:256]
            pltpu.make_async_copy(
                result.at[slot],
                early_ref.at[:, pl.ds(pl.multiple_of(g * 8 + i * 4, 4), 4), pl.ds(128 * h, 128), :],
                flush.at[slot],
            ).start()
            return carry

        lax.fori_loop(0, 2, pair, 0)

    count = groups * halves
    for g in range(groups):
        form(g)
        for h in range(halves):
            copy_x(g * halves + h).start()
    for step in range(count + 2):
        if step < count:
            reduce_x(step)
        if 1 <= step <= count:
            reduce_z(step - 1)
        if step >= 2:
            finish(step - 2)
            if step - 2 < early * halves:
                shrink(step - 2)
    for slot in range(2):
        flushed(slot).wait()
    for g in range(early, groups):
        for h in range(halves):
            c = g * halves + h
            rest_ref[:, (g - early) * 8 : (g - early) * 8 + 8, 128 * h : 128 * h + 128] = (
                ready[c].reshape(4 * passes, 8, 128)
            )


def gather_images(kernel, kernel_far, focus, focus_far, vertical_lags, grad, pred, strip, levels, early):
    _, rows, pulses = kernel.shape
    passes, cols = focus.shape[1], focus.shape[3]
    own_rows = strip // 2
    groups, halves = own_rows // 8, cols // 128
    count = groups * halves
    cells = grad.shape[1] // 2
    margin = SPAN * strip
    sizes = (strip, own_rows, margin, levels, groups, halves, early)
    vmem = pl.BlockSpec(memory_space=pltpu.VMEM)
    block = (2, 2, passes, 8, 128)
    return pl.pallas_call(
        functools.partial(gather_kernel, sizes),
        in_specs=[pl.BlockSpec(memory_space=pltpu.SMEM)] + [vmem] * 6,
        out_specs=[pl.BlockSpec(memory_space=pl.ANY), vmem],
        out_shape=[
            jax.ShapeDtypeStruct((2, early * 8, cols, cells), jnp.bfloat16),
            jax.ShapeDtypeStruct((4 * passes, (groups - early) * 8, cols), jnp.float32),
        ],
        scratch_shapes=[
            pltpu.VMEM((4, margin + rows, pulses), jnp.float32),
            pltpu.VMEM((count, levels) + block, jnp.bfloat16),
            pltpu.VMEM((count, levels) + block, jnp.bfloat16),
            pltpu.VMEM((count, levels) + block, jnp.bfloat16),
            pltpu.VMEM((count, levels - 1) + block, jnp.bfloat16),
            pltpu.VMEM((count, levels - 1) + block, jnp.bfloat16),
            pltpu.VMEM((count, 2, passes, 8, 128), jnp.bfloat16),
            pltpu.VMEM((count, 2, passes, 8, 128), jnp.bfloat16),
            pltpu.VMEM((count, 2, 2, passes, 8, 128), jnp.float32),
            pltpu.VMEM((2, 2, 256, cells), jnp.float32),
            pltpu.VMEM((2, 2, 4, 128, cells), jnp.bfloat16),
            pltpu.SemaphoreType.DMA((count,)),
            pltpu.SemaphoreType.DMA((count,)),
            pltpu.SemaphoreType.DMA((count, levels - 1)),
            pltpu.SemaphoreType.DMA((count, levels - 1)),
            pltpu.SemaphoreType.DMA((count,)),
            pltpu.SemaphoreType.DMA((count,)),
            pltpu.SemaphoreType.DMA((2,)),
        ],
        compiler_params=pltpu.CompilerParams(collective_id=0, has_side_effects=True),
        name="gather",
    )(vertical_lags, kernel, kernel_far, focus, focus_far, grad, pred)


def merge_kernel(ratio, early_ref, rest_ref, grad_ref, pred_ref, out_ref):
    step = pl.program_id(0)
    rows = out_ref.shape[1]

    @pl.when(step % (ratio + 1) < ratio)
    def _():
        out_ref[...] = early_ref[...].astype(jnp.float32)

    @pl.when(step % (ratio + 1) == ratio)
    def _():
        observed = []
        for i in range(rows):
            y = rest_ref[:, rows * (step // (ratio + 1)) + i, :]
            observed.append(jnp.concatenate([y] * 4, axis=0).T)

        last = shrink_pixels(
            observed, grad_ref, pred_ref, [out_ref.at[:, i] for i in range(rows)]
        )
        for i in range(rows):
            for plane in range(2):
                out_ref[plane, i] = last[i][plane]


def merge_profiles(early_part, rest, grad, pred, shape):
    _, rows, cols, cells = shape
    at_once = 2
    copies, computes = early_part.shape[1] // at_once, rest.shape[1] // at_once
    ratio = copies // computes

    def source(i):
        return (0, (i // (ratio + 1)) * ratio + jnp.minimum(i % (ratio + 1), ratio - 1), 0, 0)

    def target(i):
        own = i % (ratio + 1) == ratio
        return (0, jnp.where(own, copies + i // (ratio + 1), (i // (ratio + 1)) * ratio + i % (ratio + 1)), 0, 0)

    return pl.pallas_call(
        functools.partial(merge_kernel, ratio),
        grid=(copies + computes,),
        in_specs=[
            pl.BlockSpec((2, at_once, cols, cells), source),
            pl.BlockSpec(rest.shape, lambda i: (0, 0, 0)),
            pl.BlockSpec(grad.shape, lambda i: (0, 0)),
            pl.BlockSpec(pred.shape, lambda i: (0, 0)),
        ],
        out_specs=pl.BlockSpec((2, at_once, cols, cells), target),
        out_shape=jax.ShapeDtypeStruct(shape, jnp.float32),
        name="merge",
    )(early_part, rest, grad, pred)


def split_high_low(matrix):
    high = matrix.astype(jnp.bfloat16)
    return high, (matrix - high.astype(jnp.float32)).astype(jnp.bfloat16)


def body(
    echo_record,
    along_track_kernel,
    slant_distance_kernel,
    vertical_lags,
    lateral_lags,
    orbit_source_survey,
    normal_spacings,
):
    ap_count = lax.axis_size("ap")
    pass_count = lax.axis_size("pass")
    rows = along_track_kernel.shape[1]
    cols = slant_distance_kernel.shape[2]
    strip = rows // ap_count
    own_rows = strip // pass_count
    chunks = max(1, min(CHUNKS, own_rows // 8))
    passes = normal_spacings.shape[0]
    swap = [(i, i ^ 1) for i in range(ap_count)]
    same_side = [[i for i in range(ap_count) if i % 2 == side] for side in range(2)]

    kernel_far = lax.ppermute(along_track_kernel, "ap", swap)
    focus = focus_range(echo_record, slant_distance_kernel, lateral_lags)
    focus_far = lax.ppermute(focus, "ap", swap)
    place, own_pass = lax.axis_index("ap"), lax.axis_index("pass")
    side = jnp.stack([place % 2, place // 2, own_pass]).astype(jnp.int32)
    direct = pass_count == 2 and own_rows % 32 == 0 and ap_count % 4 == 0 and cols % 128 == 0
    if direct:
        orbit_source_survey = jnp.where(
            own_pass == 0, orbit_source_survey, jnp.roll(orbit_source_survey, passes // 2)
        )
    inphase, quadrature = phasor_dictionary(normal_spacings, orbit_source_survey, HEIGHT_CELLS)
    adjoint = (
        jnp.concatenate(
            [
                jnp.concatenate([inphase, -quadrature], axis=1),
                jnp.concatenate([quadrature, inphase], axis=1),
            ],
            axis=0,
        )
    )
    grad_high, grad_low = split_high_low(adjoint / passes)
    grad = jnp.concatenate([grad_high, grad_high, grad_low, grad_low], axis=0)
    forward = (adjoint.T / HEIGHT_CELLS).astype(jnp.bfloat16)
    pred = jnp.concatenate([forward] * 4, axis=1)

    shape = (2, own_rows, cols, HEIGHT_CELLS)
    if direct:
        early_part, rest = gather_images(
            along_track_kernel, kernel_far, focus, focus_far, vertical_lags, grad, pred,
            strip, ap_count // 4, own_rows // 8 * EARLY // 4,
        )
        return merge_profiles(early_part, rest, grad, pred, shape)
    profile = None
    pieces = form_images(
        direct, along_track_kernel, kernel_far, focus, focus_far, vertical_lags, side,
        chunks, pass_count, strip,
    )

    arrived = []
    for piece in pieces:
        arrived.append(
            lax.all_to_all(
                piece, "ap", split_axis=0, concat_axis=0, axis_index_groups=same_side
            )
        )
    for c, received in enumerate(arrived):
        if profile is not None:
            received, profile = lax.optimization_barrier((received, profile))
        summed = jnp.sum(received.astype(jnp.float32), axis=0).astype(jnp.bfloat16)
        stacked = lax.all_to_all(summed, "pass", split_axis=2, concat_axis=1, tiled=True)
        y = stacked.reshape(2 * passes, -1)
        profile = shrink_chunk(c, chunks, y, grad, pred, profile, shape)
    return profile


def solution(mesh):
    return jax.shard_map(
        body,
        mesh=mesh,
        in_specs=(
            P(None, "pass", "ap", None),
            P(None, None, "ap"),
            P(),
            P("pass"),
            P("pass"),
            P(),
            P(),
        ),
        out_specs=P(None, ("ap", "pass"), None, None),
        check_vma=False,
    )
```

```python
import functools

import jax
import jax.numpy as jnp
from jax import lax
from jax.experimental import pallas as pl
from jax.experimental.pallas import tpu as pltpu
from jax.sharding import PartitionSpec as P

HEIGHT_CELLS = 512
ITERS = 4
SPAN = 2
CHUNKS = 4
EARLY = 3
GATHER_VMEM = 20 * 2**20
MERGE_VMEM = 9 * 2**20
MESH = pl.DeviceIdType.MESH

shrink_level = 0.1


def phasor_dictionary(normal_spacings, orbit_source_survey, height_cell_number):
    support_mask = (
        orbit_source_survey[:, None]
        == jnp.arange(normal_spacings.shape[0], dtype=jnp.int32)[None, :]
    ).astype(normal_spacings.dtype)
    chosen_height_cells = jnp.sum(support_mask * normal_spacings[None, :], axis=1)
    orbit_start_positions = (
        jnp.arange(height_cell_number).astype(normal_spacings.dtype) - height_cell_number // 2
    )
    phases = jnp.pi * chosen_height_cells[:, None] * orbit_start_positions[None, :]
    return (jnp.cos(phases), jnp.sin(phases))


def focus_kernel(lags_ref, echo_ref, slant_ref, out_ref):
    dot = functools.partial(jnp.dot, preferred_element_type=jnp.float32)
    echo_re, echo_im = echo_ref[0, 0], echo_ref[1, 0]
    slant_re, slant_im = slant_ref[0], slant_ref[1]
    lag = lags_ref[pl.program_id(0)]
    focus_re = dot(echo_re, slant_re) - dot(echo_im, slant_im)
    focus_im = dot(echo_re, slant_im) + dot(echo_im, slant_re)
    inside = lax.broadcasted_iota(jnp.int32, focus_re.shape, 1) >= lag
    for plane, values in enumerate((focus_re, focus_im)):
        moved = jnp.where(inside, pltpu.roll(values, lag, 1), 0.0)
        out_ref[plane, 0] = moved.astype(out_ref.dtype)


def focus_range(echo, slant, lateral_lags):
    _, passes, pulses, freqs = echo.shape
    cols = slant.shape[2]
    return pl.pallas_call(
        focus_kernel,
        grid_spec=pltpu.PrefetchScalarGridSpec(
            num_scalar_prefetch=1,
            grid=(passes,),
            in_specs=[
                pl.BlockSpec((2, 1, pulses, freqs), lambda p, lags: (0, p, 0, 0)),
                pl.BlockSpec((2, freqs, cols), lambda p, lags: (0, 0, 0)),
            ],
            out_specs=pl.BlockSpec((2, 1, pulses, cols), lambda p, lags: (0, p, 0, 0)),
        ),
        out_shape=jax.ShapeDtypeStruct((2, passes, pulses, cols), jnp.bfloat16),
        cost_estimate=pl.CostEstimate(
            flops=8 * passes * pulses * freqs * cols,
            bytes_accessed=6 * passes * pulses * freqs,
            transcendentals=0,
        ),
        name="focus",
    )(lateral_lags, echo, slant)


def image_kernel(direct, chunks, pass_count, strip, margin, lags_ref, side_ref, *refs):
    kernels, focuses = refs[0:2], refs[2:4]
    outs, padded = refs[4:-1], refs[-1]
    owners = kernels[0].shape[1] // strip // 2
    rows = kernels[0].shape[1]
    pulses = kernels[0].shape[2]
    cols = outs[0].shape[-1]

    @pl.when(pl.program_id(0) == 0)
    def _():
        for s in range(2):
            for plane in range(2):
                padded[2 * s + plane, 0:margin, :] = jnp.zeros((margin, pulses), jnp.float32)
                padded[2 * s + plane, margin : margin + rows, :] = kernels[s][plane].astype(
                    jnp.float32
                )

    base = margin - lags_ref[pl.program_id(0)] + side_ref[0] * strip
    half = strip // pass_count
    starts = []
    for o in range(owners):
        if direct:
            first = base + 2 * lax.rem(side_ref[1] + o, owners) * strip
            for q in range(pass_count):
                starts.append((first + lax.rem(side_ref[2] + q, pass_count) * half, half))
        else:
            starts.append((base + 2 * o * strip, strip))
    total_re = jnp.zeros((owners * strip, cols), jnp.float32)
    total_im = jnp.zeros((owners * strip, cols), jnp.float32)
    dot = functools.partial(jnp.dot, preferred_element_type=jnp.float32)
    for s in range(2):
        kernel_re, kernel_im = (
            jnp.concatenate(
                [padded[2 * s + plane, pl.ds(start, size), :] for start, size in starts],
                axis=0,
            ).astype(jnp.bfloat16)
            for plane in range(2)
        )
        focus_re, focus_im = focuses[s][0, 0], focuses[s][1, 0]
        if pulses % 128 == 0:
            both = jnp.concatenate([kernel_re, kernel_im], axis=1)
            total_re += dot(both, jnp.concatenate([focus_re, -focus_im], axis=0))
            total_im += dot(both, jnp.concatenate([focus_im, focus_re], axis=0))
        else:
            total_re += dot(kernel_re, focus_re) - dot(kernel_im, focus_im)
            total_im += dot(kernel_re, focus_im) + dot(kernel_im, focus_re)
    height = strip // pass_count // chunks
    for plane, total in enumerate((total_re, total_im)):
        if chunks == 1 and not direct:
            outs[0][:, plane, 0] = total.reshape(owners, strip, cols).astype(jnp.bfloat16)
        else:
            split = total.reshape(owners, pass_count, chunks, height, cols)
            for c in range(chunks):
                part = split[:, :, c].reshape(owners, pass_count * height, cols)
                part = part.astype(jnp.bfloat16)
                if direct:
                    for o in range(owners):
                        outs[c * owners + o][plane, 0] = part[o]
                else:
                    outs[c][:, plane, 0] = part


def form_images(direct, kernel, kernel_far, focus, focus_far, vertical_lags, side, chunks, pass_count, strip):
    _, rows, pulses = kernel.shape
    passes, cols = focus.shape[1], focus.shape[3]
    owners = rows // strip // 2
    margin = SPAN * strip
    piece = strip // chunks
    whole = pl.BlockSpec((2, rows, pulses), lambda p, *_: (0, 0, 0))
    one = pl.BlockSpec((2, 1, pulses, cols), lambda p, *_: (0, p, 0, 0))
    if direct:
        out_specs = [pl.BlockSpec((2, 1, piece, cols), lambda p, *_: (0, p, 0, 0))]
        out_shape = [jax.ShapeDtypeStruct((2, passes, piece, cols), jnp.bfloat16)]
        out_specs, out_shape = out_specs * (chunks * owners), out_shape * (chunks * owners)
    else:
        out_specs = [pl.BlockSpec((owners, 2, 1, piece, cols), lambda p, *_: (0, 0, p, 0, 0))]
        out_shape = [jax.ShapeDtypeStruct((owners, 2, passes, piece, cols), jnp.bfloat16)]
        out_specs, out_shape = out_specs * chunks, out_shape * chunks
    return pl.pallas_call(
        functools.partial(image_kernel, direct, chunks, pass_count, strip, margin),
        grid_spec=pltpu.PrefetchScalarGridSpec(
            num_scalar_prefetch=2,
            grid=(passes,),
            in_specs=[whole, whole, one, one],
            out_specs=out_specs,
            scratch_shapes=[pltpu.VMEM((4, margin + rows, pulses), jnp.float32)],
        ),
        out_shape=out_shape,
        cost_estimate=pl.CostEstimate(
            flops=8 * passes * pulses * rows * cols,
            bytes_accessed=2 * passes * rows * cols,
            transcendentals=0,
        ),
        name="image",
    )(vertical_lags, side, kernel, kernel_far, focus, focus_far)


def shrink_kernel(rows_at_once, y_ref, grad_ref, pred_ref, *refs):
    out_ref = refs[-1]
    cells = out_ref.shape[3]
    cols = out_ref.shape[2]
    width = grad_ref.shape[0]
    block = width // 4
    dot = functools.partial(jnp.dot, preferred_element_type=jnp.float32)
    coarse = (lax.broadcasted_iota(jnp.int32, (cols, width), 1) // block) % 2 == 0
    observed = []
    for i in range(rows_at_once):
        y = y_ref[:, i * cols : (i + 1) * cols].astype(jnp.float32)
        observed.append(jnp.concatenate([y] * 4, axis=0).T)
    resid = list(observed)
    for sweep in range(ITERS):
        for i in range(rows_at_once):
            high = resid[i].astype(jnp.bfloat16)
            low = (resid[i] - high.astype(jnp.float32)).astype(jnp.bfloat16)
            moving = jnp.where(coarse, high, low)
            planes = []
            for plane in range(2):
                v = dot(moving, grad_ref[:, plane * cells : (plane + 1) * cells])
                if sweep > 0:
                    v += out_ref[plane, i]
                u = v - jnp.clip(v, -shrink_level, shrink_level)
                out_ref[plane, i] = u
                planes.append(u.astype(jnp.bfloat16))
            if sweep < ITERS - 1:
                resid[i] = observed[i] - dot(jnp.concatenate(planes, axis=1), pred_ref[...])


def shrink_chunk(c, chunks, y, grad, pred, profile, shape):
    _, rows, cols, cells = shape
    height = rows // chunks
    rows_at_once = 2 if height % 2 == 0 else 1
    steps = height // rows_at_once
    width, span = grad.shape
    specs = [
        pl.BlockSpec((y.shape[0], rows_at_once * cols), lambda i: (0, i)),
        pl.BlockSpec((width, span), lambda i: (0, 0)),
        pl.BlockSpec((span, width), lambda i: (0, 0)),
    ]
    operands = [y, grad, pred]
    aliases = {}
    if profile is not None:
        specs.append(pl.BlockSpec(memory_space=pl.ANY))
        operands.append(profile)
        aliases = {3: 0}
    return pl.pallas_call(
        functools.partial(shrink_kernel, rows_at_once),
        grid=(steps,),
        in_specs=specs,
        out_specs=pl.BlockSpec(
            (2, rows_at_once, cols, cells), lambda i: (0, c * steps + i, 0, 0)
        ),
        out_shape=jax.ShapeDtypeStruct(shape, jnp.float32),
        input_output_aliases=aliases,
        cost_estimate=pl.CostEstimate(
            flops=7 * 2 * height * cols * span * 256,
            bytes_accessed=8 * height * cols * cells,
            transcendentals=0,
        ),
        name="shrink_%d" % c,
    )(*operands)


def shrink_pixels(observed, grad_ref, pred_ref, load, store):
    pixels, width = observed[0].shape
    cells = grad_ref.shape[1] // 2
    dot = functools.partial(jnp.dot, preferred_element_type=jnp.float32)
    coarse = (lax.broadcasted_iota(jnp.int32, (pixels, width), 1) // (width // 4)) % 2 == 0
    resid = list(observed)
    for sweep in range(ITERS):
        for i in range(len(observed)):
            high = resid[i].astype(jnp.bfloat16)
            low = (resid[i] - high.astype(jnp.float32)).astype(jnp.bfloat16)
            moving = jnp.where(coarse, high, low)
            planes = []
            for plane in range(2):
                v = dot(moving, grad_ref[:, plane * cells : (plane + 1) * cells])
                if sweep > 0:
                    v += load(i, plane)
                u = v - jnp.clip(v, -shrink_level, shrink_level)
                store(i, plane, u)
                planes.append(u.astype(jnp.bfloat16))
            if sweep < ITERS - 1:
                resid[i] = observed[i] - dot(jnp.concatenate(planes, axis=1), pred_ref[...])


def gather_kernel(
    sizes, lags_ref, kernel_near, kernel_far, focus_near, focus_far, grad_ref, pred_ref,
    *refs,
):
    strip, own_rows, margin, levels, groups, halves, early = sizes
    early_refs, rest_ref = refs[:early], refs[early]
    padded, keep, send, land, mid, zland, ysend, yland, ready = refs[early + 1 : early + 10]
    x_out, x_in, z_out, z_in, y_out, y_in = refs[early + 10 :]
    rows, pulses = kernel_near.shape[1:]
    passes = focus_near.shape[1]
    place, plane_y = lax.axis_index("ap"), lax.axis_index("pass")
    core, x, z = place % 2, (place // 2) % 2, place // 4
    peer_x = (place + 2 - 4 * x, plane_y)
    peer_y = (place, 1 - plane_y)
    peers_z = [(lax.rem(z + d, levels) * 4 + place % 4, plane_y) for d in range(levels)]
    barrier = pltpu.get_barrier_semaphore()
    for peer in [peer_x, peer_y] + peers_z[1:]:
        pl.semaphore_signal(barrier, inc=1, device_id=peer, device_id_type=MESH)
    pl.semaphore_wait(barrier, levels + 1)

    for s, ref in enumerate((kernel_near, kernel_far)):
        for plane in range(2):
            padded[2 * s + plane, 0:margin, :] = jnp.zeros((margin, pulses), jnp.float32)
            padded[2 * s + plane, margin : margin + rows, :] = ref[plane].astype(jnp.float32)

    def copy_x(c):
        return pltpu.make_async_remote_copy(
            src_ref=send.at[c], dst_ref=land.at[c], send_sem=x_out.at[c], recv_sem=x_in.at[c],
            device_id=peer_x, device_id_type=MESH,
        )

    def copy_z(c, d):
        return pltpu.make_async_remote_copy(
            src_ref=mid.at[c, d - 1], dst_ref=zland.at[c, d - 1],
            send_sem=z_out.at[c, d - 1], recv_sem=z_in.at[c, d - 1],
            device_id=peers_z[d], device_id_type=MESH,
        )

    def copy_y(c):
        return pltpu.make_async_remote_copy(
            src_ref=ysend.at[c], dst_ref=yland.at[c], send_sem=y_out.at[c], recv_sem=y_in.at[c],
            device_id=peer_y, device_id_type=MESH,
        )

    dot = functools.partial(jnp.dot, preferred_element_type=jnp.float32)

    def form(g):
        def one(p, carry):
            base = margin - lags_ref[p] + g * 8
            starts = []
            for side in range(2):
                for d in range(levels):
                    owner = lax.rem(z + d, levels) * 4 + lax.rem(x + side, 2) * 2 + core
                    for q in range(2):
                        starts.append(base + owner * strip + lax.rem(plane_y + q, 2) * own_rows)
            parts = []
            for n in range(4):
                parts.append(
                    jnp.concatenate([padded[n, pl.ds(start, 8), :] for start in starts], axis=0)
                    .astype(jnp.bfloat16)
                )
            taken = jnp.concatenate(parts, axis=1)
            near_re, near_im = focus_near[0, p], focus_near[1, p]
            far_re, far_im = focus_far[0, p], focus_far[1, p]
            out_re = dot(taken, jnp.concatenate([near_re, -near_im, far_re, -far_im], axis=0))
            out_im = dot(taken, jnp.concatenate([near_im, near_re, far_im, far_re], axis=0))
            for plane, out in enumerate((out_re, out_im)):
                out = out.astype(jnp.bfloat16)
                n = 0
                for buffer in (keep, send):
                    for d in range(levels):
                        for q in range(2):
                            for h in range(halves):
                                buffer[g * halves + h, d, q, plane, p] = out[
                                    8 * n : 8 * n + 8, 128 * h : 128 * h + 128
                                ]
                            n += 1
            return carry

        lax.fori_loop(0, passes, one, 0)

    def reduce_x(c):
        copy_x(c).wait()
        for d in range(1, levels):
            total = keep[c, d].astype(jnp.float32) + land[c, d].astype(jnp.float32)
            mid[c, d - 1] = total.astype(jnp.bfloat16)
        for d in range(1, levels):
            copy_z(c, d).start()

    def reduce_z(c):
        for d in range(1, levels):
            copy_z(c, d).wait()
        total = keep[c, 0].astype(jnp.float32) + land[c, 0].astype(jnp.float32)
        for d in range(1, levels):
            total += zland[c, d - 1].astype(jnp.float32)
        total = total.astype(jnp.bfloat16)
        ysend[c] = total[1]
        copy_y(c).start()
        ready[c, :, 0] = total[0].astype(jnp.float32)

    def finish(c):
        copy_y(c).wait()
        ready[c, :, 1] = yland[c].astype(jnp.float32)

    def observe(c, r):
        y = ready[c, :, :, :, r, :].reshape(4 * passes, 128)
        return jnp.concatenate([y] * 4, axis=0).T

    def shrink(c):
        g, h = c // halves, c % halves

        def pair(i, carry):
            def where(k):
                row = i * 4 + 2 * k
                return pl.ds(row, 2), pl.ds(128 * h, 128)

            def load(k, plane):
                rows_of, cols_of = where(k)
                return early_refs[g][plane, rows_of, cols_of, :].reshape(256, -1)

            def store(k, plane, value):
                rows_of, cols_of = where(k)
                early_refs[g][plane, rows_of, cols_of, :] = value.reshape(2, 128, -1)

            observed = []
            for k in range(2):
                observed.append(
                    jnp.concatenate(
                        [observe(c, i * 4 + 2 * k), observe(c, i * 4 + 2 * k + 1)], axis=0
                    )
                )
            shrink_pixels(observed, grad_ref, pred_ref, load, store)
            return carry

        lax.fori_loop(0, 2, pair, 0)

    count = groups * halves
    for g in range(groups):
        form(g)
        for h in range(halves):
            copy_x(g * halves + h).start()
    for step in range(count + 2):
        if step < count:
            reduce_x(step)
        if 1 <= step <= count:
            reduce_z(step - 1)
        if step >= 2:
            finish(step - 2)
            if step - 2 < early * halves:
                shrink(step - 2)
    for g in range(early, groups):
        for h in range(halves):
            c = g * halves + h
            rest_ref[:, (g - early) * 8 : (g - early) * 8 + 8, 128 * h : 128 * h + 128] = (
                ready[c].reshape(4 * passes, 8, 128)
            )


def gather_images(kernel, kernel_far, focus, focus_far, vertical_lags, grad, pred, strip, levels, early):
    _, rows, pulses = kernel.shape
    passes, cols = focus.shape[1], focus.shape[3]
    own_rows = strip // 2
    groups, halves = own_rows // 8, cols // 128
    count = groups * halves
    cells = grad.shape[1] // 2
    margin = SPAN * strip
    sizes = (strip, own_rows, margin, levels, groups, halves, early)
    vmem = pl.BlockSpec(memory_space=pltpu.VMEM)
    block = (2, 2, passes, 8, 128)
    return pl.pallas_call(
        functools.partial(gather_kernel, sizes),
        in_specs=[pl.BlockSpec(memory_space=pltpu.SMEM)] + [vmem] * 6,
        out_specs=[vmem] * (early + 1),
        out_shape=[
            jax.ShapeDtypeStruct((2, 8, cols, cells), jnp.float32)
            for _ in range(early)
        ] + [
            jax.ShapeDtypeStruct((4 * passes, (groups - early) * 8, cols), jnp.float32),
        ],
        scratch_shapes=[
            pltpu.VMEM((4, margin + rows, pulses), jnp.float32),
            pltpu.VMEM((count, levels) + block, jnp.bfloat16),
            pltpu.VMEM((count, levels) + block, jnp.bfloat16),
            pltpu.VMEM((count, levels) + block, jnp.bfloat16),
            pltpu.VMEM((count, levels - 1) + block, jnp.bfloat16),
            pltpu.VMEM((count, levels - 1) + block, jnp.bfloat16),
            pltpu.VMEM((count, 2, passes, 8, 128), jnp.bfloat16),
            pltpu.VMEM((count, 2, passes, 8, 128), jnp.bfloat16),
            pltpu.VMEM((count, 2, 2, passes, 8, 128), jnp.float32),
            pltpu.SemaphoreType.DMA((count,)),
            pltpu.SemaphoreType.DMA((count,)),
            pltpu.SemaphoreType.DMA((count, levels - 1)),
            pltpu.SemaphoreType.DMA((count, levels - 1)),
            pltpu.SemaphoreType.DMA((count,)),
            pltpu.SemaphoreType.DMA((count,)),
        ],
        compiler_params=pltpu.CompilerParams(
            collective_id=0, has_side_effects=True, vmem_limit_bytes=GATHER_VMEM
        ),
        name="gather",
    )(vertical_lags, kernel, kernel_far, focus, focus_far, grad, pred)


def merge_kernel(count, *refs):
    early_refs = refs[:count]
    rest_ref, grad_ref, pred_ref, out_ref, work, early_sems, rest_sems = refs[count:]
    height, at_once = early_refs[0].shape[1], work.shape[2]
    early = count * height

    def early_copy(n):
        return pltpu.make_async_copy(
            early_refs[n], out_ref.at[:, pl.ds(n * height, height)], early_sems.at[n]
        )

    def rest_copy(i):
        rows = pl.ds(early + at_once * i, at_once)
        return pltpu.make_async_copy(work.at[i], out_ref.at[:, rows], rest_sems.at[i])

    for n in range(count):
        early_copy(n).start()

    def pair(i, carry):
        def load(k, plane):
            return work[i, plane, k]

        def store(k, plane, value):
            work[i, plane, k] = value

        observed = []
        for k in range(at_once):
            observed.append(jnp.concatenate([rest_ref[:, at_once * i + k, :]] * 4, axis=0).T)
        shrink_pixels(observed, grad_ref, pred_ref, load, store)
        rest_copy(i).start()
        return carry

    lax.fori_loop(0, work.shape[0], pair, 0)
    for n in range(count):
        early_copy(n).wait()
    for i in range(work.shape[0]):
        rest_copy(i).wait()


def merge_profiles(early_parts, rest, grad, pred, shape):
    _, rows, cols, cells = shape
    at_once = 2
    steps = rest.shape[1] // at_once
    count = len(early_parts)
    vmem = pl.BlockSpec(memory_space=pltpu.VMEM)
    return pl.pallas_call(
        functools.partial(merge_kernel, count),
        in_specs=[vmem] * (count + 3),
        out_specs=pl.BlockSpec(memory_space=pl.ANY),
        out_shape=jax.ShapeDtypeStruct(shape, jnp.float32),
        scratch_shapes=[
            pltpu.VMEM((steps, 2, at_once, cols, cells), jnp.float32),
            pltpu.SemaphoreType.DMA((count,)),
            pltpu.SemaphoreType.DMA((steps,)),
        ],
        compiler_params=pltpu.CompilerParams(vmem_limit_bytes=MERGE_VMEM),
        name="merge",
    )(*early_parts, rest, grad, pred)


def split_high_low(matrix):
    high = matrix.astype(jnp.bfloat16)
    return high, (matrix - high.astype(jnp.float32)).astype(jnp.bfloat16)


def body(
    echo_record,
    along_track_kernel,
    slant_distance_kernel,
    vertical_lags,
    lateral_lags,
    orbit_source_survey,
    normal_spacings,
):
    ap_count = lax.axis_size("ap")
    pass_count = lax.axis_size("pass")
    rows = along_track_kernel.shape[1]
    cols = slant_distance_kernel.shape[2]
    strip = rows // ap_count
    own_rows = strip // pass_count
    chunks = max(1, min(CHUNKS, own_rows // 8))
    passes = normal_spacings.shape[0]
    swap = [(i, i ^ 1) for i in range(ap_count)]
    same_side = [[i for i in range(ap_count) if i % 2 == side] for side in range(2)]

    kernel_far = lax.ppermute(along_track_kernel, "ap", swap)
    focus = focus_range(echo_record, slant_distance_kernel, lateral_lags)
    focus_far = lax.ppermute(focus, "ap", swap)
    place, own_pass = lax.axis_index("ap"), lax.axis_index("pass")
    side = jnp.stack([place % 2, place // 2, own_pass]).astype(jnp.int32)
    direct = pass_count == 2 and own_rows % 32 == 0 and ap_count % 4 == 0 and cols % 128 == 0
    if direct:
        orbit_source_survey = jnp.where(
            own_pass == 0, orbit_source_survey, jnp.roll(orbit_source_survey, passes // 2)
        )
    inphase, quadrature = phasor_dictionary(normal_spacings, orbit_source_survey, HEIGHT_CELLS)
    adjoint = (
        jnp.concatenate(
            [
                jnp.concatenate([inphase, -quadrature], axis=1),
                jnp.concatenate([quadrature, inphase], axis=1),
            ],
            axis=0,
        )
    )
    grad_high, grad_low = split_high_low(adjoint / passes)
    grad = jnp.concatenate([grad_high, grad_high, grad_low, grad_low], axis=0)
    forward = (adjoint.T / HEIGHT_CELLS).astype(jnp.bfloat16)
    pred = jnp.concatenate([forward] * 4, axis=1)

    shape = (2, own_rows, cols, HEIGHT_CELLS)
    if direct:
        *early_parts, rest = gather_images(
            along_track_kernel, kernel_far, focus, focus_far, vertical_lags, grad, pred,
            strip, ap_count // 4, own_rows // 8 * EARLY // 4,
        )
        return merge_profiles(early_parts, rest, grad, pred, shape)
    profile = None
    pieces = form_images(
        direct, along_track_kernel, kernel_far, focus, focus_far, vertical_lags, side,
        chunks, pass_count, strip,
    )

    arrived = []
    for piece in pieces:
        arrived.append(
            lax.all_to_all(
                piece, "ap", split_axis=0, concat_axis=0, axis_index_groups=same_side
            )
        )
    for c, received in enumerate(arrived):
        if profile is not None:
            received, profile = lax.optimization_barrier((received, profile))
        summed = jnp.sum(received.astype(jnp.float32), axis=0).astype(jnp.bfloat16)
        stacked = lax.all_to_all(summed, "pass", split_axis=2, concat_axis=1, tiled=True)
        y = stacked.reshape(2 * passes, -1)
        profile = shrink_chunk(c, chunks, y, grad, pred, profile, shape)
    return profile


def solution(mesh):
    return jax.shard_map(
        body,
        mesh=mesh,
        in_specs=(
            P(None, "pass", "ap", None),
            P(None, None, "ap"),
            P(),
            P("pass"),
            P("pass"),
            P(),
            P(),
        ),
        out_specs=P(None, ("ap", "pass"), None, None),
        check_vma=False,
    )
```

```python
import functools

import jax
import jax.numpy as jnp
from jax import lax
from jax.experimental import pallas as pl
from jax.experimental.pallas import tpu as pltpu
from jax.sharding import PartitionSpec as P

HEIGHT_CELLS = 512
ITERS = 4
SPAN = 2
CHUNKS = 4
EARLY = 3
GATHER_VMEM = 18 * 2**20
PREPARE_VMEM = 16 * 2**20
MERGE_VMEM = 9 * 2**20
MESH = pl.DeviceIdType.MESH

shrink_level = 0.1


def phasor_dictionary(normal_spacings, orbit_source_survey, height_cell_number):
    support_mask = (
        orbit_source_survey[:, None]
        == jnp.arange(normal_spacings.shape[0], dtype=jnp.int32)[None, :]
    ).astype(normal_spacings.dtype)
    chosen_height_cells = jnp.sum(support_mask * normal_spacings[None, :], axis=1)
    orbit_start_positions = (
        jnp.arange(height_cell_number).astype(normal_spacings.dtype) - height_cell_number // 2
    )
    phases = jnp.pi * chosen_height_cells[:, None] * orbit_start_positions[None, :]
    return (jnp.cos(phases), jnp.sin(phases))


def focus_kernel(lags_ref, echo_ref, slant_ref, out_ref):
    dot = functools.partial(jnp.dot, preferred_element_type=jnp.float32)
    echo_re, echo_im = echo_ref[0, 0], echo_ref[1, 0]
    slant_re, slant_im = slant_ref[0], slant_ref[1]
    lag = lags_ref[pl.program_id(0)]
    focus_re = dot(echo_re, slant_re) - dot(echo_im, slant_im)
    focus_im = dot(echo_re, slant_im) + dot(echo_im, slant_re)
    inside = lax.broadcasted_iota(jnp.int32, focus_re.shape, 1) >= lag
    for plane, values in enumerate((focus_re, focus_im)):
        moved = jnp.where(inside, pltpu.roll(values, lag, 1), 0.0)
        out_ref[plane, 0] = moved.astype(out_ref.dtype)


def focus_range(echo, slant, lateral_lags):
    _, passes, pulses, freqs = echo.shape
    cols = slant.shape[2]
    return pl.pallas_call(
        focus_kernel,
        grid_spec=pltpu.PrefetchScalarGridSpec(
            num_scalar_prefetch=1,
            grid=(passes,),
            in_specs=[
                pl.BlockSpec((2, 1, pulses, freqs), lambda p, lags: (0, p, 0, 0)),
                pl.BlockSpec((2, freqs, cols), lambda p, lags: (0, 0, 0)),
            ],
            out_specs=pl.BlockSpec((2, 1, pulses, cols), lambda p, lags: (0, p, 0, 0)),
        ),
        out_shape=jax.ShapeDtypeStruct((2, passes, pulses, cols), jnp.bfloat16),
        cost_estimate=pl.CostEstimate(
            flops=8 * passes * pulses * freqs * cols,
            bytes_accessed=6 * passes * pulses * freqs,
            transcendentals=0,
        ),
        name="focus",
    )(lateral_lags, echo, slant)


def image_kernel(direct, chunks, pass_count, strip, margin, lags_ref, side_ref, *refs):
    kernels, focuses = refs[0:2], refs[2:4]
    outs, padded = refs[4:-1], refs[-1]
    owners = kernels[0].shape[1] // strip // 2
    rows = kernels[0].shape[1]
    pulses = kernels[0].shape[2]
    cols = outs[0].shape[-1]

    @pl.when(pl.program_id(0) == 0)
    def _():
        for s in range(2):
            for plane in range(2):
                padded[2 * s + plane, 0:margin, :] = jnp.zeros((margin, pulses), jnp.float32)
                padded[2 * s + plane, margin : margin + rows, :] = kernels[s][plane].astype(
                    jnp.float32
                )

    base = margin - lags_ref[pl.program_id(0)] + side_ref[0] * strip
    half = strip // pass_count
    starts = []
    for o in range(owners):
        if direct:
            first = base + 2 * lax.rem(side_ref[1] + o, owners) * strip
            for q in range(pass_count):
                starts.append((first + lax.rem(side_ref[2] + q, pass_count) * half, half))
        else:
            starts.append((base + 2 * o * strip, strip))
    total_re = jnp.zeros((owners * strip, cols), jnp.float32)
    total_im = jnp.zeros((owners * strip, cols), jnp.float32)
    dot = functools.partial(jnp.dot, preferred_element_type=jnp.float32)
    for s in range(2):
        kernel_re, kernel_im = (
            jnp.concatenate(
                [padded[2 * s + plane, pl.ds(start, size), :] for start, size in starts],
                axis=0,
            ).astype(jnp.bfloat16)
            for plane in range(2)
        )
        focus_re, focus_im = focuses[s][0, 0], focuses[s][1, 0]
        if pulses % 128 == 0:
            both = jnp.concatenate([kernel_re, kernel_im], axis=1)
            total_re += dot(both, jnp.concatenate([focus_re, -focus_im], axis=0))
            total_im += dot(both, jnp.concatenate([focus_im, focus_re], axis=0))
        else:
            total_re += dot(kernel_re, focus_re) - dot(kernel_im, focus_im)
            total_im += dot(kernel_re, focus_im) + dot(kernel_im, focus_re)
    height = strip // pass_count // chunks
    for plane, total in enumerate((total_re, total_im)):
        if chunks == 1 and not direct:
            outs[0][:, plane, 0] = total.reshape(owners, strip, cols).astype(jnp.bfloat16)
        else:
            split = total.reshape(owners, pass_count, chunks, height, cols)
            for c in range(chunks):
                part = split[:, :, c].reshape(owners, pass_count * height, cols)
                part = part.astype(jnp.bfloat16)
                if direct:
                    for o in range(owners):
                        outs[c * owners + o][plane, 0] = part[o]
                else:
                    outs[c][:, plane, 0] = part


def form_images(direct, kernel, kernel_far, focus, focus_far, vertical_lags, side, chunks, pass_count, strip):
    _, rows, pulses = kernel.shape
    passes, cols = focus.shape[1], focus.shape[3]
    owners = rows // strip // 2
    margin = SPAN * strip
    piece = strip // chunks
    whole = pl.BlockSpec((2, rows, pulses), lambda p, *_: (0, 0, 0))
    one = pl.BlockSpec((2, 1, pulses, cols), lambda p, *_: (0, p, 0, 0))
    if direct:
        out_specs = [pl.BlockSpec((2, 1, piece, cols), lambda p, *_: (0, p, 0, 0))]
        out_shape = [jax.ShapeDtypeStruct((2, passes, piece, cols), jnp.bfloat16)]
        out_specs, out_shape = out_specs * (chunks * owners), out_shape * (chunks * owners)
    else:
        out_specs = [pl.BlockSpec((owners, 2, 1, piece, cols), lambda p, *_: (0, 0, p, 0, 0))]
        out_shape = [jax.ShapeDtypeStruct((owners, 2, passes, piece, cols), jnp.bfloat16)]
        out_specs, out_shape = out_specs * chunks, out_shape * chunks
    return pl.pallas_call(
        functools.partial(image_kernel, direct, chunks, pass_count, strip, margin),
        grid_spec=pltpu.PrefetchScalarGridSpec(
            num_scalar_prefetch=2,
            grid=(passes,),
            in_specs=[whole, whole, one, one],
            out_specs=out_specs,
            scratch_shapes=[pltpu.VMEM((4, margin + rows, pulses), jnp.float32)],
        ),
        out_shape=out_shape,
        cost_estimate=pl.CostEstimate(
            flops=8 * passes * pulses * rows * cols,
            bytes_accessed=2 * passes * rows * cols,
            transcendentals=0,
        ),
        name="image",
    )(vertical_lags, side, kernel, kernel_far, focus, focus_far)


def shrink_kernel(rows_at_once, y_ref, grad_ref, pred_ref, *refs):
    out_ref = refs[-1]
    cells = out_ref.shape[3]
    cols = out_ref.shape[2]
    width = grad_ref.shape[0]
    block = width // 4
    dot = functools.partial(jnp.dot, preferred_element_type=jnp.float32)
    coarse = (lax.broadcasted_iota(jnp.int32, (cols, width), 1) // block) % 2 == 0
    observed = []
    for i in range(rows_at_once):
        y = y_ref[:, i * cols : (i + 1) * cols].astype(jnp.float32)
        observed.append(jnp.concatenate([y] * 4, axis=0).T)
    resid = list(observed)
    for sweep in range(ITERS):
        for i in range(rows_at_once):
            high = resid[i].astype(jnp.bfloat16)
            low = (resid[i] - high.astype(jnp.float32)).astype(jnp.bfloat16)
            moving = jnp.where(coarse, high, low)
            planes = []
            for plane in range(2):
                v = dot(moving, grad_ref[:, plane * cells : (plane + 1) * cells])
                if sweep > 0:
                    v += out_ref[plane, i]
                u = v - jnp.clip(v, -shrink_level, shrink_level)
                out_ref[plane, i] = u
                planes.append(u.astype(jnp.bfloat16))
            if sweep < ITERS - 1:
                resid[i] = observed[i] - dot(jnp.concatenate(planes, axis=1), pred_ref[...])


def shrink_chunk(c, chunks, y, grad, pred, profile, shape):
    _, rows, cols, cells = shape
    height = rows // chunks
    rows_at_once = 2 if height % 2 == 0 else 1
    steps = height // rows_at_once
    width, span = grad.shape
    specs = [
        pl.BlockSpec((y.shape[0], rows_at_once * cols), lambda i: (0, i)),
        pl.BlockSpec((width, span), lambda i: (0, 0)),
        pl.BlockSpec((span, width), lambda i: (0, 0)),
    ]
    operands = [y, grad, pred]
    aliases = {}
    if profile is not None:
        specs.append(pl.BlockSpec(memory_space=pl.ANY))
        operands.append(profile)
        aliases = {3: 0}
    return pl.pallas_call(
        functools.partial(shrink_kernel, rows_at_once),
        grid=(steps,),
        in_specs=specs,
        out_specs=pl.BlockSpec(
            (2, rows_at_once, cols, cells), lambda i: (0, c * steps + i, 0, 0)
        ),
        out_shape=jax.ShapeDtypeStruct(shape, jnp.float32),
        input_output_aliases=aliases,
        cost_estimate=pl.CostEstimate(
            flops=7 * 2 * height * cols * span * 256,
            bytes_accessed=8 * height * cols * cells,
            transcendentals=0,
        ),
        name="shrink_%d" % c,
    )(*operands)


def shrink_pixels(observed, grad_ref, pred_ref, load, store):
    pixels, width = observed[0].shape
    cells = grad_ref.shape[1] // 2
    dot = functools.partial(jnp.dot, preferred_element_type=jnp.float32)
    coarse = (lax.broadcasted_iota(jnp.int32, (pixels, width), 1) // (width // 4)) % 2 == 0
    resid = list(observed)
    for sweep in range(ITERS):
        for i in range(len(observed)):
            high = resid[i].astype(jnp.bfloat16)
            low = (resid[i] - high.astype(jnp.float32)).astype(jnp.bfloat16)
            moving = jnp.where(coarse, high, low)
            planes = []
            for plane in range(2):
                v = dot(moving, grad_ref[:, plane * cells : (plane + 1) * cells])
                if sweep > 0:
                    v += load(i, plane)
                u = v - jnp.clip(v, -shrink_level, shrink_level)
                store(i, plane, u)
                planes.append(u.astype(jnp.bfloat16))
            if sweep < ITERS - 1:
                resid[i] = observed[i] - dot(jnp.concatenate(planes, axis=1), pred_ref[...])


def prepare_kernel(
    margin, *refs,
):
    sources, (focus_ref, padded_ref, grad_ref, pred_ref) = refs[:6], refs[6:10]
    held, sems = refs[10:16], refs[16]
    lags_ref, survey_ref, spacings_ref, kernel_ref, slant_ref, echo_ref = held
    _, passes, pulses, freqs = echo_ref.shape
    copies = [
        pltpu.make_async_copy(source, target, sems.at[n])
        for n, (source, target) in enumerate(zip(sources, held))
    ]
    for copy in copies:
        copy.start()
    for copy in copies[:3]:
        copy.wait()
    rows, cols = kernel_ref.shape[1], slant_ref.shape[2]
    total = survey_ref.shape[0]
    cells = grad_ref.shape[1] // 2
    own = lax.axis_index("pass")
    row = lax.broadcasted_iota(jnp.int32, (total, cells), 0)
    chosen = jnp.zeros((total, cells), jnp.float32)
    for k in range(total):
        value = spacings_ref[survey_ref[lax.rem(k + own * (total // 2), total)]]
        chosen = jnp.where(row == k, value, chosen)
    place = lax.broadcasted_iota(jnp.int32, (total, cells), 1) - cells // 2
    phases = jnp.pi * chosen * place.astype(jnp.float32)
    inphase, quadrature = jnp.cos(phases), jnp.sin(phases)
    adjoint = jnp.concatenate(
        [
            jnp.concatenate([inphase, -quadrature], axis=1),
            jnp.concatenate([quadrature, inphase], axis=1),
        ],
        axis=0,
    )
    high, low = split_high_low(adjoint / total)
    grad_ref[...] = jnp.concatenate([high, high, low, low], axis=0)
    pred_ref[...] = jnp.concatenate([adjoint / cells] * 4, axis=0).T.astype(jnp.bfloat16)
    copies[3].wait()
    for plane in range(2):
        padded_ref[plane, 0:margin, :] = jnp.zeros((margin, pulses), jnp.float32)
        padded_ref[plane, margin : margin + rows, :] = kernel_ref[plane].astype(jnp.float32)
    copies[4].wait()
    copies[5].wait()
    dot = functools.partial(jnp.dot, preferred_element_type=jnp.float32)
    slant_re, slant_im = slant_ref[0], slant_ref[1]
    into = (
        jnp.concatenate([slant_re, -slant_im], axis=0),
        jnp.concatenate([slant_im, slant_re], axis=0),
    )
    at_once = 4 if passes % 4 == 0 else 1
    for first in range(0, passes, at_once):
        taken = jnp.concatenate(
            [echo_ref[n, first : first + at_once].reshape(at_once * pulses, freqs) for n in range(2)],
            axis=1,
        )
        for plane in range(2):
            values = dot(taken, into[plane])
            for n in range(at_once):
                lag = lags_ref[first + n]
                one = values[n * pulses : (n + 1) * pulses]
                inside = lax.broadcasted_iota(jnp.int32, one.shape, 1) >= lag
                moved = jnp.where(inside, pltpu.roll(one, lag, 1), 0.0)
                focus_ref[first + n, plane] = moved.astype(jnp.bfloat16)


def prepare(lateral_lags, survey, spacings, echo, slant, kernel, margin):
    _, passes, pulses, _ = echo.shape
    rows, cols, total = kernel.shape[1], slant.shape[2], survey.shape[0]
    vmem = pl.BlockSpec(memory_space=pltpu.VMEM)
    return pl.pallas_call(
        functools.partial(prepare_kernel, margin),
        in_specs=[pl.BlockSpec(memory_space=pltpu.HBM)] * 6,
        out_specs=[vmem] * 4,
        out_shape=[
            jax.ShapeDtypeStruct((passes, 2, pulses, cols), jnp.bfloat16),
            jax.ShapeDtypeStruct((2, margin + rows, pulses), jnp.float32),
            jax.ShapeDtypeStruct((8 * total, 2 * HEIGHT_CELLS), jnp.bfloat16),
            jax.ShapeDtypeStruct((2 * HEIGHT_CELLS, 8 * total), jnp.bfloat16),
        ],
        scratch_shapes=[
            pltpu.SMEM(lateral_lags.shape, lateral_lags.dtype),
            pltpu.SMEM(survey.shape, survey.dtype),
            pltpu.SMEM(spacings.shape, spacings.dtype),
            pltpu.VMEM(kernel.shape, kernel.dtype),
            pltpu.VMEM(slant.shape, slant.dtype),
            pltpu.VMEM(echo.shape, echo.dtype),
            pltpu.SemaphoreType.DMA((6,)),
        ],
        compiler_params=pltpu.CompilerParams(vmem_limit_bytes=PREPARE_VMEM),
        cost_estimate=pl.CostEstimate(
            flops=8 * passes * pulses * echo.shape[3] * cols,
            bytes_accessed=6 * passes * pulses * echo.shape[3],
            transcendentals=0,
        ),
        name="prepare",
    )(*(pltpu.with_memory_space_constraint(v, pltpu.HBM) for v in (lateral_lags, survey, spacings, kernel, slant, echo)))


def gather_kernel(
    sizes, lags_hbm, padded_near, kernel_far, focus_near, grad_ref, pred_ref, *refs
):
    strip, own_rows, margin, levels, groups, halves, early = sizes
    early_refs, rest_ref = refs[:early], refs[early]
    lags_ref, padded_far, focus_far, keep, send, land, mid, zland, ysend, yland, ready = refs[
        early + 1 : early + 12
    ]
    l_in, f_out, f_in, x_out, x_in, z_out, z_in, y_out, y_in = refs[early + 12 :]
    copy_lags = pltpu.make_async_copy(lags_hbm, lags_ref, l_in.at[0])
    copy_lags.start()
    rows, pulses = kernel_far.shape[1:]
    passes = focus_near.shape[0]
    place, plane_y = lax.axis_index("ap"), lax.axis_index("pass")
    core, x, z = place % 2, (place // 2) % 2, place // 4
    peer_core = (place + 1 - 2 * core, plane_y)
    peer_x = (place + 2 - 4 * x, plane_y)
    peer_y = (place, 1 - plane_y)
    peers_z = [(lax.rem(z + d, levels) * 4 + place % 4, plane_y) for d in range(levels)]
    barrier = pltpu.get_barrier_semaphore()
    for peer in [peer_core, peer_x, peer_y] + peers_z[1:]:
        pl.semaphore_signal(barrier, inc=1, device_id=peer, device_id_type=MESH)
    pl.semaphore_wait(barrier, levels + 2)

    def copy_focus(p):
        return pltpu.make_async_remote_copy(
            src_ref=focus_near.at[p], dst_ref=focus_far.at[p],
            send_sem=f_out.at[p], recv_sem=f_in.at[p],
            device_id=peer_core, device_id_type=MESH,
        )

    def copy_x(c, n):
        return pltpu.make_async_remote_copy(
            src_ref=send.at[c, n], dst_ref=land.at[c, n],
            send_sem=x_out.at[c, n], recv_sem=x_in.at[c, n],
            device_id=peer_x, device_id_type=MESH,
        )

    def copy_z(c, n, d):
        return pltpu.make_async_remote_copy(
            src_ref=mid.at[c, n, d - 1], dst_ref=zland.at[c, n, d - 1],
            send_sem=z_out.at[c, n, d - 1], recv_sem=z_in.at[c, n, d - 1],
            device_id=peers_z[d], device_id_type=MESH,
        )

    def copy_y(c, n):
        return pltpu.make_async_remote_copy(
            src_ref=ysend.at[c, n], dst_ref=yland.at[c, n],
            send_sem=y_out.at[c, n], recv_sem=y_in.at[c, n],
            device_id=peer_y, device_id_type=MESH,
        )

    for p in range(passes):
        copy_focus(p).start()
    for n in range(2):
        padded_far[n, 0:margin, :] = jnp.zeros((margin, pulses), jnp.float32)
        padded_far[n, margin : margin + rows, :] = kernel_far[n].astype(jnp.float32)
    copy_lags.wait()

    dot = functools.partial(jnp.dot, preferred_element_type=jnp.float32)

    def form(g):
        def one(p, carry):
            base = margin - lags_ref[p] + g * 8
            starts = []
            for side in range(2):
                for d in range(levels):
                    owner = lax.rem(z + d, levels) * 4 + lax.rem(x + side, 2) * 2 + core
                    for q in range(2):
                        starts.append(base + owner * strip + lax.rem(plane_y + q, 2) * own_rows)
            parts = []
            for ref in (padded_near, padded_far):
                for n in range(2):
                    parts.append(
                        jnp.concatenate([ref[n, pl.ds(start, 8), :] for start in starts], axis=0)
                        .astype(jnp.bfloat16)
                    )
            taken = jnp.concatenate(parts, axis=1)
            if g == 0:
                copy_focus(p).wait()
            near_re, near_im = focus_near[p, 0], focus_near[p, 1]
            far_re, far_im = focus_far[p, 0], focus_far[p, 1]
            out_re = dot(taken, jnp.concatenate([near_re, -near_im, far_re, -far_im], axis=0))
            out_im = dot(taken, jnp.concatenate([near_im, near_re, far_im, far_re], axis=0))
            for n, out in enumerate((out_re, out_im)):
                out = out.astype(jnp.bfloat16)
                start = 0
                for buffer in (keep, send):
                    for d in range(levels):
                        for q in range(2):
                            for h in range(halves):
                                buffer[g * halves + h, n, d, q, p] = out[
                                    start : start + 8, 128 * h : 128 * h + 128
                                ]
                            start += 8
            return carry

        lax.fori_loop(0, passes, one, 0)
        for h in range(halves):
            for n in range(2):
                copy_x(g * halves + h, n).start()

    def reduce_x(e):
        c, n = e // 2, e % 2
        copy_x(c, n).wait()
        for d in range(1, levels):
            total = keep[c, n, d].astype(jnp.float32) + land[c, n, d].astype(jnp.float32)
            mid[c, n, d - 1] = total.astype(jnp.bfloat16)
        for d in range(1, levels):
            copy_z(c, n, d).start()

    def reduce_z(e):
        c, n = e // 2, e % 2
        for d in range(1, levels):
            copy_z(c, n, d).wait()
        total = keep[c, n, 0].astype(jnp.float32) + land[c, n, 0].astype(jnp.float32)
        for d in range(1, levels):
            total += zland[c, n, d - 1].astype(jnp.float32)
        total = total.astype(jnp.bfloat16)
        ysend[c, n] = total[1]
        copy_y(c, n).start()
        ready[c, n, 0] = total[0].astype(jnp.float32)

    def finish(e):
        c, n = e // 2, e % 2
        copy_y(c, n).wait()
        ready[c, n, 1] = yland[c, n].astype(jnp.float32)

    def observe(c, r):
        y = ready[c, :, :, :, r, :].reshape(4 * passes, 128)
        return jnp.concatenate([y] * 4, axis=0).T

    def shrink(g, e):
        c, i = e // 2, e % 2
        h = c % halves
        early_ref = early_refs[g]

        def where(k):
            columns = pl.ds(pl.multiple_of(128 * h, 128), 128)
            return pl.ds(i * 4 + 2 * k, 2), columns

        def load(k, plane):
            rows_of, cols_of = where(k)
            return early_ref[plane, rows_of, cols_of, :].reshape(256, -1)

        def store(k, plane, value):
            rows_of, cols_of = where(k)
            early_ref[plane, rows_of, cols_of, :] = value.reshape(2, 128, -1)

        observed = []
        for k in range(2):
            r = i * 4 + 2 * k
            observed.append(jnp.concatenate([observe(c, r), observe(c, r + 1)], axis=0))
        shrink_pixels(observed, grad_ref, pred_ref, load, store)

    count = 2 * groups * halves
    todo = 2 * early * halves

    def step(e):
        if e < count:
            reduce_x(e)
        if 2 <= e < count + 2:
            reduce_z(e - 2)
        if 4 <= e:
            finish(e - 4)
        if 5 <= e < todo + 5:
            shrink((e - 5) // (2 * halves), e - 5)

    form(0)
    form(1)
    step(0)
    step(1)
    form(2)
    step(2)
    step(3)
    form(3)
    step(4)
    for g in range(early):

        def steady(e, carry):
            reduce_x(e)
            reduce_z(e - 2)
            finish(e - 4)
            shrink(g, e - 5)
            return carry

        first = 5 + 2 * halves * g
        last = min(first + 2 * halves, count)
        lax.fori_loop(first, last, steady, 0)
    for e in range(last, count + 4):
        step(e)
    for g in range(early, groups):
        for h in range(halves):
            rest_ref[:, (g - early) * 8 : (g - early) * 8 + 8, 128 * h : 128 * h + 128] = (
                ready[g * halves + h].reshape(4 * passes, 8, 128)
            )


def gather_images(padded, kernel_far, focus, vertical_lags, grad, pred, strip, levels, early):
    _, rows, pulses = kernel_far.shape
    passes, cols = focus.shape[0], focus.shape[3]
    own_rows = strip // 2
    groups, halves = own_rows // 8, cols // 128
    count = groups * halves
    cells = grad.shape[1] // 2
    margin = SPAN * strip
    sizes = (strip, own_rows, margin, levels, groups, halves, early)
    vmem = pl.BlockSpec(memory_space=pltpu.VMEM)
    block = (2, passes, 8, 128)
    dma = pltpu.SemaphoreType.DMA
    return pl.pallas_call(
        functools.partial(gather_kernel, sizes),
        in_specs=[pl.BlockSpec(memory_space=pltpu.HBM)] + [vmem] * 5,
        out_specs=[vmem] * (early + 1),
        out_shape=[
            jax.ShapeDtypeStruct((2, 8, cols, cells), jnp.float32)
            for _ in range(early)
        ] + [
            jax.ShapeDtypeStruct((4 * passes, (groups - early) * 8, cols), jnp.float32),
        ],
        scratch_shapes=[
            pltpu.SMEM(vertical_lags.shape, vertical_lags.dtype),
            pltpu.VMEM((2, margin + rows, pulses), jnp.float32),
            pltpu.VMEM(focus.shape, jnp.bfloat16),
            pltpu.VMEM((count, 2, levels) + block, jnp.bfloat16),
            pltpu.VMEM((count, 2, levels) + block, jnp.bfloat16),
            pltpu.VMEM((count, 2, levels) + block, jnp.bfloat16),
            pltpu.VMEM((count, 2, levels - 1) + block, jnp.bfloat16),
            pltpu.VMEM((count, 2, levels - 1) + block, jnp.bfloat16),
            pltpu.VMEM((count, 2, passes, 8, 128), jnp.bfloat16),
            pltpu.VMEM((count, 2, passes, 8, 128), jnp.bfloat16),
            pltpu.VMEM((count, 2, 2, passes, 8, 128), jnp.float32),
            dma((1,)),
            dma((passes,)),
            dma((passes,)),
            dma((count, 2)),
            dma((count, 2)),
            dma((count, 2, levels - 1)),
            dma((count, 2, levels - 1)),
            dma((count, 2)),
            dma((count, 2)),
        ],
        compiler_params=pltpu.CompilerParams(
            collective_id=0, has_side_effects=True, vmem_limit_bytes=GATHER_VMEM
        ),
        name="gather",
    )(pltpu.with_memory_space_constraint(vertical_lags, pltpu.HBM), padded, kernel_far, focus, grad, pred)


def merge_kernel(count, *refs):
    early_refs = refs[:count]
    rest_ref, grad_ref, pred_ref, out_ref, work, early_sems, rest_sems = refs[count:]
    height, at_once = early_refs[0].shape[1], work.shape[2]
    early = count * height

    def early_copy(n):
        return pltpu.make_async_copy(
            early_refs[n], out_ref.at[:, pl.ds(n * height, height)], early_sems.at[n]
        )

    def rest_copy(i):
        rows = pl.ds(early + at_once * i, at_once)
        return pltpu.make_async_copy(work.at[i], out_ref.at[:, rows], rest_sems.at[i])

    for n in range(count):
        early_copy(n).start()

    def pair(i, carry):
        def load(k, plane):
            return work[i, plane, k]

        def store(k, plane, value):
            work[i, plane, k] = value

        observed = []
        for k in range(at_once):
            observed.append(jnp.concatenate([rest_ref[:, at_once * i + k, :]] * 4, axis=0).T)
        shrink_pixels(observed, grad_ref, pred_ref, load, store)
        rest_copy(i).start()
        return carry

    lax.fori_loop(0, work.shape[0], pair, 0)
    for n in range(count):
        early_copy(n).wait()
    for i in range(work.shape[0]):
        rest_copy(i).wait()


def merge_profiles(early_parts, rest, grad, pred, shape):
    _, rows, cols, cells = shape
    at_once = 2
    steps = rest.shape[1] // at_once
    count = len(early_parts)
    vmem = pl.BlockSpec(memory_space=pltpu.VMEM)
    return pl.pallas_call(
        functools.partial(merge_kernel, count),
        in_specs=[vmem] * (count + 3),
        out_specs=pl.BlockSpec(memory_space=pl.ANY),
        out_shape=jax.ShapeDtypeStruct(shape, jnp.float32),
        scratch_shapes=[
            pltpu.VMEM((steps, 2, at_once, cols, cells), jnp.float32),
            pltpu.SemaphoreType.DMA((count,)),
            pltpu.SemaphoreType.DMA((steps,)),
        ],
        compiler_params=pltpu.CompilerParams(vmem_limit_bytes=MERGE_VMEM),
        name="merge",
    )(*early_parts, rest, grad, pred)


def split_high_low(matrix):
    high = matrix.astype(jnp.bfloat16)
    return high, (matrix - high.astype(jnp.float32)).astype(jnp.bfloat16)


def body(
    echo_record,
    along_track_kernel,
    slant_distance_kernel,
    vertical_lags,
    lateral_lags,
    orbit_source_survey,
    normal_spacings,
):
    ap_count = lax.axis_size("ap")
    pass_count = lax.axis_size("pass")
    rows = along_track_kernel.shape[1]
    cols = slant_distance_kernel.shape[2]
    strip = rows // ap_count
    own_rows = strip // pass_count
    chunks = max(1, min(CHUNKS, own_rows // 8))
    passes = normal_spacings.shape[0]
    swap = [(i, i ^ 1) for i in range(ap_count)]
    same_side = [[i for i in range(ap_count) if i % 2 == side] for side in range(2)]

    kernel_far = lax.ppermute(along_track_kernel, "ap", swap)
    shape = (2, own_rows, cols, HEIGHT_CELLS)
    direct = (
        pass_count == 2 and own_rows == 32 and ap_count % 4 == 0 and cols % 128 == 0
        and passes == 16
    )
    if direct:
        focus, padded, grad, pred = prepare(
            lateral_lags, orbit_source_survey, normal_spacings, echo_record,
            slant_distance_kernel, along_track_kernel, SPAN * strip,
        )
        *early_parts, rest = gather_images(
            padded, kernel_far, focus, vertical_lags, grad, pred, strip, ap_count // 4, EARLY,
        )
        return merge_profiles(early_parts, rest, grad, pred, shape)
    focus = focus_range(echo_record, slant_distance_kernel, lateral_lags)
    focus_far = lax.ppermute(focus, "ap", swap)
    place, own_pass = lax.axis_index("ap"), lax.axis_index("pass")
    side = jnp.stack([place % 2, place // 2, own_pass]).astype(jnp.int32)

    inphase, quadrature = phasor_dictionary(normal_spacings, orbit_source_survey, HEIGHT_CELLS)
    adjoint = jnp.concatenate(
        [
            jnp.concatenate([inphase, -quadrature], axis=1),
            jnp.concatenate([quadrature, inphase], axis=1),
        ],
        axis=0,
    )
    grad_high, grad_low = split_high_low(adjoint / passes)
    grad = jnp.concatenate([grad_high, grad_high, grad_low, grad_low], axis=0)
    forward = (adjoint.T / HEIGHT_CELLS).astype(jnp.bfloat16)
    pred = jnp.concatenate([forward] * 4, axis=1)
    profile = None
    pieces = form_images(
        direct, along_track_kernel, kernel_far, focus, focus_far, vertical_lags, side,
        chunks, pass_count, strip,
    )

    arrived = []
    for piece in pieces:
        arrived.append(
            lax.all_to_all(
                piece, "ap", split_axis=0, concat_axis=0, axis_index_groups=same_side
            )
        )
    for c, received in enumerate(arrived):
        if profile is not None:
            received, profile = lax.optimization_barrier((received, profile))
        summed = jnp.sum(received.astype(jnp.float32), axis=0).astype(jnp.bfloat16)
        stacked = lax.all_to_all(summed, "pass", split_axis=2, concat_axis=1, tiled=True)
        y = stacked.reshape(2 * passes, -1)
        profile = shrink_chunk(c, chunks, y, grad, pred, profile, shape)
    return profile


def solution(mesh):
    return jax.shard_map(
        body,
        mesh=mesh,
        in_specs=(
            P(None, "pass", "ap", None),
            P(None, None, "ap"),
            P(),
            P("pass"),
            P("pass"),
            P(),
            P(),
        ),
        out_specs=P(None, ("ap", "pass"), None, None),
        check_vma=False,
    )
```

```python
import functools

import jax
import jax.numpy as jnp
from jax import lax
from jax.experimental import pallas as pl
from jax.experimental.pallas import tpu as pltpu
from jax.sharding import PartitionSpec as P

HEIGHT_CELLS = 512
ITERS = 4
SPAN = 2
CHUNKS = 4
EARLY = 3
GATHER_VMEM = 18 * 2**20
PREPARE_VMEM = 16 * 2**20
MERGE_VMEM = 9 * 2**20
MESH = pl.DeviceIdType.MESH

shrink_level = 0.1


def phasor_dictionary(normal_spacings, orbit_source_survey, height_cell_number):
    support_mask = (
        orbit_source_survey[:, None]
        == jnp.arange(normal_spacings.shape[0], dtype=jnp.int32)[None, :]
    ).astype(normal_spacings.dtype)
    chosen_height_cells = jnp.sum(support_mask * normal_spacings[None, :], axis=1)
    orbit_start_positions = (
        jnp.arange(height_cell_number).astype(normal_spacings.dtype) - height_cell_number // 2
    )
    phases = jnp.pi * chosen_height_cells[:, None] * orbit_start_positions[None, :]
    return (jnp.cos(phases), jnp.sin(phases))


def focus_kernel(lags_ref, echo_ref, slant_ref, out_ref):
    dot = functools.partial(jnp.dot, preferred_element_type=jnp.float32)
    echo_re, echo_im = echo_ref[0, 0], echo_ref[1, 0]
    slant_re, slant_im = slant_ref[0], slant_ref[1]
    lag = lags_ref[pl.program_id(0)]
    focus_re = dot(echo_re, slant_re) - dot(echo_im, slant_im)
    focus_im = dot(echo_re, slant_im) + dot(echo_im, slant_re)
    inside = lax.broadcasted_iota(jnp.int32, focus_re.shape, 1) >= lag
    for plane, values in enumerate((focus_re, focus_im)):
        moved = jnp.where(inside, pltpu.roll(values, lag, 1), 0.0)
        out_ref[plane, 0] = moved.astype(out_ref.dtype)


def focus_range(echo, slant, lateral_lags):
    _, passes, pulses, freqs = echo.shape
    cols = slant.shape[2]
    return pl.pallas_call(
        focus_kernel,
        grid_spec=pltpu.PrefetchScalarGridSpec(
            num_scalar_prefetch=1,
            grid=(passes,),
            in_specs=[
                pl.BlockSpec((2, 1, pulses, freqs), lambda p, lags: (0, p, 0, 0)),
                pl.BlockSpec((2, freqs, cols), lambda p, lags: (0, 0, 0)),
            ],
            out_specs=pl.BlockSpec((2, 1, pulses, cols), lambda p, lags: (0, p, 0, 0)),
        ),
        out_shape=jax.ShapeDtypeStruct((2, passes, pulses, cols), jnp.bfloat16),
        cost_estimate=pl.CostEstimate(
            flops=8 * passes * pulses * freqs * cols,
            bytes_accessed=6 * passes * pulses * freqs,
            transcendentals=0,
        ),
        name="focus",
    )(lateral_lags, echo, slant)


def image_kernel(direct, chunks, pass_count, strip, margin, lags_ref, side_ref, *refs):
    kernels, focuses = refs[0:2], refs[2:4]
    outs, padded = refs[4:-1], refs[-1]
    owners = kernels[0].shape[1] // strip // 2
    rows = kernels[0].shape[1]
    pulses = kernels[0].shape[2]
    cols = outs[0].shape[-1]

    @pl.when(pl.program_id(0) == 0)
    def _():
        for s in range(2):
            for plane in range(2):
                padded[2 * s + plane, 0:margin, :] = jnp.zeros((margin, pulses), jnp.float32)
                padded[2 * s + plane, margin : margin + rows, :] = kernels[s][plane].astype(
                    jnp.float32
                )

    base = margin - lags_ref[pl.program_id(0)] + side_ref[0] * strip
    half = strip // pass_count
    starts = []
    for o in range(owners):
        if direct:
            first = base + 2 * lax.rem(side_ref[1] + o, owners) * strip
            for q in range(pass_count):
                starts.append((first + lax.rem(side_ref[2] + q, pass_count) * half, half))
        else:
            starts.append((base + 2 * o * strip, strip))
    total_re = jnp.zeros((owners * strip, cols), jnp.float32)
    total_im = jnp.zeros((owners * strip, cols), jnp.float32)
    dot = functools.partial(jnp.dot, preferred_element_type=jnp.float32)
    for s in range(2):
        kernel_re, kernel_im = (
            jnp.concatenate(
                [padded[2 * s + plane, pl.ds(start, size), :] for start, size in starts],
                axis=0,
            ).astype(jnp.bfloat16)
            for plane in range(2)
        )
        focus_re, focus_im = focuses[s][0, 0], focuses[s][1, 0]
        if pulses % 128 == 0:
            both = jnp.concatenate([kernel_re, kernel_im], axis=1)
            total_re += dot(both, jnp.concatenate([focus_re, -focus_im], axis=0))
            total_im += dot(both, jnp.concatenate([focus_im, focus_re], axis=0))
        else:
            total_re += dot(kernel_re, focus_re) - dot(kernel_im, focus_im)
            total_im += dot(kernel_re, focus_im) + dot(kernel_im, focus_re)
    height = strip // pass_count // chunks
    for plane, total in enumerate((total_re, total_im)):
        if chunks == 1 and not direct:
            outs[0][:, plane, 0] = total.reshape(owners, strip, cols).astype(jnp.bfloat16)
        else:
            split = total.reshape(owners, pass_count, chunks, height, cols)
            for c in range(chunks):
                part = split[:, :, c].reshape(owners, pass_count * height, cols)
                part = part.astype(jnp.bfloat16)
                if direct:
                    for o in range(owners):
                        outs[c * owners + o][plane, 0] = part[o]
                else:
                    outs[c][:, plane, 0] = part


def form_images(direct, kernel, kernel_far, focus, focus_far, vertical_lags, side, chunks, pass_count, strip):
    _, rows, pulses = kernel.shape
    passes, cols = focus.shape[1], focus.shape[3]
    owners = rows // strip // 2
    margin = SPAN * strip
    piece = strip // chunks
    whole = pl.BlockSpec((2, rows, pulses), lambda p, *_: (0, 0, 0))
    one = pl.BlockSpec((2, 1, pulses, cols), lambda p, *_: (0, p, 0, 0))
    if direct:
        out_specs = [pl.BlockSpec((2, 1, piece, cols), lambda p, *_: (0, p, 0, 0))]
        out_shape = [jax.ShapeDtypeStruct((2, passes, piece, cols), jnp.bfloat16)]
        out_specs, out_shape = out_specs * (chunks * owners), out_shape * (chunks * owners)
    else:
        out_specs = [pl.BlockSpec((owners, 2, 1, piece, cols), lambda p, *_: (0, 0, p, 0, 0))]
        out_shape = [jax.ShapeDtypeStruct((owners, 2, passes, piece, cols), jnp.bfloat16)]
        out_specs, out_shape = out_specs * chunks, out_shape * chunks
    return pl.pallas_call(
        functools.partial(image_kernel, direct, chunks, pass_count, strip, margin),
        grid_spec=pltpu.PrefetchScalarGridSpec(
            num_scalar_prefetch=2,
            grid=(passes,),
            in_specs=[whole, whole, one, one],
            out_specs=out_specs,
            scratch_shapes=[pltpu.VMEM((4, margin + rows, pulses), jnp.float32)],
        ),
        out_shape=out_shape,
        cost_estimate=pl.CostEstimate(
            flops=8 * passes * pulses * rows * cols,
            bytes_accessed=2 * passes * rows * cols,
            transcendentals=0,
        ),
        name="image",
    )(vertical_lags, side, kernel, kernel_far, focus, focus_far)


def shrink_kernel(rows_at_once, y_ref, grad_ref, pred_ref, *refs):
    out_ref = refs[-1]
    cells = out_ref.shape[3]
    cols = out_ref.shape[2]
    width = grad_ref.shape[0]
    block = width // 4
    dot = functools.partial(jnp.dot, preferred_element_type=jnp.float32)
    coarse = (lax.broadcasted_iota(jnp.int32, (cols, width), 1) // block) % 2 == 0
    observed = []
    for i in range(rows_at_once):
        y = y_ref[:, i * cols : (i + 1) * cols].astype(jnp.float32)
        observed.append(jnp.concatenate([y] * 4, axis=0).T)
    resid = list(observed)
    for sweep in range(ITERS):
        for i in range(rows_at_once):
            high = resid[i].astype(jnp.bfloat16)
            low = (resid[i] - high.astype(jnp.float32)).astype(jnp.bfloat16)
            moving = jnp.where(coarse, high, low)
            planes = []
            for plane in range(2):
                v = dot(moving, grad_ref[:, plane * cells : (plane + 1) * cells])
                if sweep > 0:
                    v += out_ref[plane, i]
                u = v - jnp.clip(v, -shrink_level, shrink_level)
                out_ref[plane, i] = u
                planes.append(u.astype(jnp.bfloat16))
            if sweep < ITERS - 1:
                resid[i] = observed[i] - dot(jnp.concatenate(planes, axis=1), pred_ref[...])


def shrink_chunk(c, chunks, y, grad, pred, profile, shape):
    _, rows, cols, cells = shape
    height = rows // chunks
    rows_at_once = 2 if height % 2 == 0 else 1
    steps = height // rows_at_once
    width, span = grad.shape
    specs = [
        pl.BlockSpec((y.shape[0], rows_at_once * cols), lambda i: (0, i)),
        pl.BlockSpec((width, span), lambda i: (0, 0)),
        pl.BlockSpec((span, width), lambda i: (0, 0)),
    ]
    operands = [y, grad, pred]
    aliases = {}
    if profile is not None:
        specs.append(pl.BlockSpec(memory_space=pl.ANY))
        operands.append(profile)
        aliases = {3: 0}
    return pl.pallas_call(
        functools.partial(shrink_kernel, rows_at_once),
        grid=(steps,),
        in_specs=specs,
        out_specs=pl.BlockSpec(
            (2, rows_at_once, cols, cells), lambda i: (0, c * steps + i, 0, 0)
        ),
        out_shape=jax.ShapeDtypeStruct(shape, jnp.float32),
        input_output_aliases=aliases,
        cost_estimate=pl.CostEstimate(
            flops=7 * 2 * height * cols * span * 256,
            bytes_accessed=8 * height * cols * cells,
            transcendentals=0,
        ),
        name="shrink_%d" % c,
    )(*operands)


def shrink_pixels(observed, grad_ref, pred_ref, load, store):
    pixels, width = observed[0].shape
    cells = grad_ref.shape[1] // 2
    dot = functools.partial(jnp.dot, preferred_element_type=jnp.float32)
    coarse = (lax.broadcasted_iota(jnp.int32, (pixels, width), 1) // (width // 4)) % 2 == 0
    resid = list(observed)
    for sweep in range(ITERS):
        for i in range(len(observed)):
            high = resid[i].astype(jnp.bfloat16)
            low = (resid[i] - high.astype(jnp.float32)).astype(jnp.bfloat16)
            moving = jnp.where(coarse, high, low)
            planes = []
            for plane in range(2):
                v = dot(moving, grad_ref[:, plane * cells : (plane + 1) * cells])
                if sweep > 0:
                    v += load(i, plane)
                u = v - jnp.clip(v, -shrink_level, shrink_level)
                store(i, plane, u)
                planes.append(u.astype(jnp.bfloat16))
            if sweep < ITERS - 1:
                resid[i] = observed[i] - dot(jnp.concatenate(planes, axis=1), pred_ref[...])


def prepare_kernel(
    margin, *refs,
):
    sources, (focus_ref, padded_ref, grad_ref, pred_ref) = refs[:6], refs[6:10]
    held, sems = refs[10:16], refs[16]
    lags_ref, survey_ref, spacings_ref, kernel_ref, slant_ref, echo_ref = held
    _, passes, pulses, freqs = echo_ref.shape
    copies = [
        pltpu.make_async_copy(source, target, sems.at[n])
        for n, (source, target) in enumerate(zip(sources, held))
    ]
    for copy in copies:
        copy.start()
    for copy in copies[:3]:
        copy.wait()
    rows, cols = kernel_ref.shape[1], slant_ref.shape[2]
    total = survey_ref.shape[0]
    cells = grad_ref.shape[1] // 2
    own = lax.axis_index("pass")
    row = lax.broadcasted_iota(jnp.int32, (total, cells), 0)
    chosen = jnp.zeros((total, cells), jnp.float32)
    for k in range(total):
        value = spacings_ref[survey_ref[lax.rem(k + own * (total // 2), total)]]
        chosen = jnp.where(row == k, value, chosen)
    place = lax.broadcasted_iota(jnp.int32, (total, cells), 1) - cells // 2
    phases = jnp.pi * chosen * place.astype(jnp.float32)
    inphase, quadrature = jnp.cos(phases), jnp.sin(phases)
    adjoint = jnp.concatenate(
        [
            jnp.concatenate([inphase, -quadrature], axis=1),
            jnp.concatenate([quadrature, inphase], axis=1),
        ],
        axis=0,
    )
    high, low = split_high_low(adjoint / total)
    grad_ref[...] = jnp.concatenate([high, high, low, low], axis=0)
    pred_ref[...] = jnp.concatenate([adjoint / cells] * 4, axis=0).T.astype(jnp.bfloat16)
    copies[3].wait()
    for plane in range(2):
        padded_ref[plane, 0:margin, :] = jnp.zeros((margin, pulses), jnp.float32)
        padded_ref[plane, margin : margin + rows, :] = kernel_ref[plane].astype(jnp.float32)
    copies[4].wait()
    copies[5].wait()
    dot = functools.partial(jnp.dot, preferred_element_type=jnp.float32)
    slant_re, slant_im = slant_ref[0], slant_ref[1]
    into = (
        jnp.concatenate([slant_re, -slant_im], axis=0),
        jnp.concatenate([slant_im, slant_re], axis=0),
    )
    at_once = 4 if passes % 4 == 0 else 1
    for first in range(0, passes, at_once):
        taken = jnp.concatenate(
            [echo_ref[n, first : first + at_once].reshape(at_once * pulses, freqs) for n in range(2)],
            axis=1,
        )
        for plane in range(2):
            values = dot(taken, into[plane])
            for n in range(at_once):
                lag = lags_ref[first + n]
                one = values[n * pulses : (n + 1) * pulses]
                inside = lax.broadcasted_iota(jnp.int32, one.shape, 1) >= lag
                moved = jnp.where(inside, pltpu.roll(one, lag, 1), 0.0)
                focus_ref[first + n, plane] = moved.astype(jnp.bfloat16)


def prepare(lateral_lags, survey, spacings, echo, slant, kernel, margin):
    _, passes, pulses, _ = echo.shape
    rows, cols, total = kernel.shape[1], slant.shape[2], survey.shape[0]
    vmem = pl.BlockSpec(memory_space=pltpu.VMEM)
    return pl.pallas_call(
        functools.partial(prepare_kernel, margin),
        in_specs=[pl.BlockSpec(memory_space=pltpu.HBM)] * 6,
        out_specs=[vmem] * 4,
        out_shape=[
            jax.ShapeDtypeStruct((passes, 2, pulses, cols), jnp.bfloat16),
            jax.ShapeDtypeStruct((2, margin + rows, pulses), jnp.float32),
            jax.ShapeDtypeStruct((8 * total, 2 * HEIGHT_CELLS), jnp.bfloat16),
            jax.ShapeDtypeStruct((2 * HEIGHT_CELLS, 8 * total), jnp.bfloat16),
        ],
        scratch_shapes=[
            pltpu.SMEM(lateral_lags.shape, lateral_lags.dtype),
            pltpu.SMEM(survey.shape, survey.dtype),
            pltpu.SMEM(spacings.shape, spacings.dtype),
            pltpu.VMEM(kernel.shape, kernel.dtype),
            pltpu.VMEM(slant.shape, slant.dtype),
            pltpu.VMEM(echo.shape, echo.dtype),
            pltpu.SemaphoreType.DMA((6,)),
        ],
        compiler_params=pltpu.CompilerParams(vmem_limit_bytes=PREPARE_VMEM),
        cost_estimate=pl.CostEstimate(
            flops=8 * passes * pulses * echo.shape[3] * cols,
            bytes_accessed=6 * passes * pulses * echo.shape[3],
            transcendentals=0,
        ),
        name="prepare",
    )(*(pltpu.with_memory_space_constraint(v, pltpu.HBM) for v in (lateral_lags, survey, spacings, kernel, slant, echo)))


def gather_kernel(
    sizes, lags_hbm, padded_near, kernel_far, focus_near, grad_ref, pred_ref, *refs
):
    strip, own_rows, margin, levels, groups, halves, early = sizes
    early_refs, rest_ref = refs[:early], refs[early]
    lags_ref, padded_far, focus_far, keep, send, land, mid, zland, ready = refs[
        early + 1 : early + 10
    ]
    l_in, f_out, f_in, x_out, x_in, z_out, z_in = refs[early + 10 :]
    copy_lags = pltpu.make_async_copy(lags_hbm, lags_ref, l_in.at[0])
    copy_lags.start()
    rows, pulses = kernel_far.shape[1:]
    passes = focus_near.shape[0]
    part = passes // 2
    place, plane_y = lax.axis_index("ap"), lax.axis_index("pass")
    core, x, z = place % 2, (place // 2) % 2, place // 4
    peer_core = (place + 1 - 2 * core, plane_y)
    peer_x = (place + 2 - 4 * x, plane_y)
    others = [(d, q) for d in range(levels) for q in range(2) if d + q > 0]
    peer = {
        (d, q): (lax.rem(z + d, levels) * 4 + place % 4, plane_y + q - 2 * q * plane_y)
        for d, q in others
    }
    barrier = pltpu.get_barrier_semaphore()
    for target in [peer_core, peer_x] + [peer[t] for t in others]:
        pl.semaphore_signal(barrier, inc=1, device_id=target, device_id_type=MESH)
    pl.semaphore_wait(barrier, len(others) + 2)

    def copy_focus(p):
        return pltpu.make_async_remote_copy(
            src_ref=focus_near.at[p], dst_ref=focus_far.at[p],
            send_sem=f_out.at[p], recv_sem=f_in.at[p],
            device_id=peer_core, device_id_type=MESH,
        )

    def copy_x(e):
        return pltpu.make_async_remote_copy(
            src_ref=send.at[e], dst_ref=land.at[e], send_sem=x_out.at[e], recv_sem=x_in.at[e],
            device_id=peer_x, device_id_type=MESH,
        )

    def copy_z(e, d, q):
        return pltpu.make_async_remote_copy(
            src_ref=mid.at[e, d, q], dst_ref=zland.at[e, d, q],
            send_sem=z_out.at[e, d, q], recv_sem=z_in.at[e, d, q],
            device_id=peer[d, q], device_id_type=MESH,
        )

    for p in range(passes):
        copy_focus(p).start()
    for n in range(2):
        padded_far[n, 0:margin, :] = jnp.zeros((margin, pulses), jnp.float32)
        padded_far[n, margin : margin + rows, :] = kernel_far[n].astype(jnp.float32)
    copy_lags.wait()

    dot = functools.partial(jnp.dot, preferred_element_type=jnp.float32)

    def form(g):
        def one(n, p, carry):
            base = margin - lags_ref[p] + g * 8
            starts = []
            for side in range(2):
                for d in range(levels):
                    owner = lax.rem(z + d, levels) * 4 + lax.rem(x + side, 2) * 2 + core
                    for q in range(2):
                        starts.append(base + owner * strip + lax.rem(plane_y + q, 2) * own_rows)
            parts = []
            for ref in (padded_near, padded_far):
                for plane in range(2):
                    parts.append(
                        jnp.concatenate([ref[plane, pl.ds(start, 8), :] for start in starts], axis=0)
                        .astype(jnp.bfloat16)
                    )
            taken = jnp.concatenate(parts, axis=1)
            if g == 0:
                copy_focus(p).wait()
            near_re, near_im = focus_near[p, 0], focus_near[p, 1]
            far_re, far_im = focus_far[p, 0], focus_far[p, 1]
            out_re = dot(taken, jnp.concatenate([near_re, -near_im, far_re, -far_im], axis=0))
            out_im = dot(taken, jnp.concatenate([near_im, near_re, far_im, far_re], axis=0))
            for plane, out in enumerate((out_re, out_im)):
                out = out.astype(jnp.bfloat16)
                start = 0
                for buffer in (keep, send):
                    for d in range(levels):
                        for q in range(2):
                            for h in range(halves):
                                buffer[(2 * g + n) * halves + h, d, q, plane, p - n * part] = out[
                                    start : start + 8, 128 * h : 128 * h + 128
                                ]
                            start += 8
            return carry

        for n in range(2):
            lax.fori_loop(n * part, n * part + part, functools.partial(one, n), 0)
            for h in range(halves):
                copy_x((2 * g + n) * halves + h).start()

    def reduce_x(e):
        copy_x(e).wait()
        for d, q in others:
            total = keep[e, d, q].astype(jnp.float32) + land[e, d, q].astype(jnp.float32)
            mid[e, d, q] = total.astype(jnp.bfloat16)
        for d, q in others:
            copy_z(e, d, q).start()

    def reduce_z(e):
        c, n = e // (2 * halves) * halves + e % halves, e // halves % 2
        for d, q in others:
            copy_z(e, d, q).wait()
        for q in range(2):
            total = None if q else keep[e, 0, 0].astype(jnp.float32) + land[e, 0, 0].astype(jnp.float32)
            for d in range(1 - q, levels):
                term = zland[e, d, q].astype(jnp.float32)
                total = term if total is None else total + term
            ready[c, :, q, pl.ds(n * part, part)] = total.astype(jnp.bfloat16).astype(jnp.float32)

    def observe(c, r):
        y = ready[c, :, :, :, r, :].reshape(4 * passes, 128)
        return jnp.concatenate([y] * 4, axis=0).T

    def shrink(g, e):
        c, i = e // 2, e % 2
        h = c % halves
        early_ref = early_refs[g]

        def where(k):
            columns = pl.ds(pl.multiple_of(128 * h, 128), 128)
            return pl.ds(i * 4 + 2 * k, 2), columns

        def load(k, plane):
            rows_of, cols_of = where(k)
            return early_ref[plane, rows_of, cols_of, :].reshape(256, -1)

        def store(k, plane, value):
            rows_of, cols_of = where(k)
            early_ref[plane, rows_of, cols_of, :] = value.reshape(2, 128, -1)

        observed = []
        for k in range(2):
            r = i * 4 + 2 * k
            observed.append(jnp.concatenate([observe(c, r), observe(c, r + 1)], axis=0))
        shrink_pixels(observed, grad_ref, pred_ref, load, store)

    count = 2 * groups * halves

    form(0)
    form(1)
    reduce_x(0)
    reduce_x(1)
    form(2)
    reduce_x(2)
    reduce_z(0)
    reduce_x(3)
    reduce_z(1)
    form(3)
    for g in range(early):

        def steady(e, carry):
            reduce_x(e)
            reduce_z(e - 2)
            shrink(g, e - 4)
            return carry

        lax.fori_loop(4 + 4 * g, 8 + 4 * g, steady, 0)
    reduce_z(count - 2)
    reduce_z(count - 1)
    for g in range(early, groups):
        for h in range(halves):
            rest_ref[:, (g - early) * 8 : (g - early) * 8 + 8, 128 * h : 128 * h + 128] = (
                ready[g * halves + h].reshape(4 * passes, 8, 128)
            )


def gather_images(padded, kernel_far, focus, vertical_lags, grad, pred, strip, levels, early):
    _, rows, pulses = kernel_far.shape
    passes, cols = focus.shape[0], focus.shape[3]
    own_rows = strip // 2
    groups, halves = own_rows // 8, cols // 128
    count = groups * halves
    cells = grad.shape[1] // 2
    margin = SPAN * strip
    sizes = (strip, own_rows, margin, levels, groups, halves, early)
    vmem = pl.BlockSpec(memory_space=pltpu.VMEM)
    block = (2, passes // 2, 8, 128)
    dma = pltpu.SemaphoreType.DMA
    return pl.pallas_call(
        functools.partial(gather_kernel, sizes),
        in_specs=[pl.BlockSpec(memory_space=pltpu.HBM)] + [vmem] * 5,
        out_specs=[vmem] * (early + 1),
        out_shape=[
            jax.ShapeDtypeStruct((2, 8, cols, cells), jnp.float32)
            for _ in range(early)
        ] + [
            jax.ShapeDtypeStruct((4 * passes, (groups - early) * 8, cols), jnp.float32),
        ],
        scratch_shapes=[
            pltpu.SMEM(vertical_lags.shape, vertical_lags.dtype),
            pltpu.VMEM((2, margin + rows, pulses), jnp.float32),
            pltpu.VMEM(focus.shape, jnp.bfloat16),
        ]
        + [pltpu.VMEM((2 * count, levels, 2) + block, jnp.bfloat16)] * 5
        + [
            pltpu.VMEM((count, 2, 2, passes, 8, 128), jnp.float32),
            dma((1,)),
            dma((passes,)),
            dma((passes,)),
            dma((2 * count,)),
            dma((2 * count,)),
            dma((2 * count, levels, 2)),
            dma((2 * count, levels, 2)),
        ],
        compiler_params=pltpu.CompilerParams(
            collective_id=0, has_side_effects=True, vmem_limit_bytes=GATHER_VMEM
        ),
        name="gather",
    )(pltpu.with_memory_space_constraint(vertical_lags, pltpu.HBM), padded, kernel_far, focus, grad, pred)


def merge_kernel(count, *refs):
    early_refs = refs[:count]
    rest_ref, grad_ref, pred_ref, out_ref, work, early_sems, rest_sems = refs[count:]
    height, at_once = early_refs[0].shape[1], work.shape[2]
    early = count * height

    def early_copy(n):
        return pltpu.make_async_copy(
            early_refs[n], out_ref.at[:, pl.ds(n * height, height)], early_sems.at[n]
        )

    def rest_copy(i):
        rows = pl.ds(early + at_once * i, at_once)
        return pltpu.make_async_copy(work.at[i], out_ref.at[:, rows], rest_sems.at[i])

    for n in range(count):
        early_copy(n).start()

    def pair(i, carry):
        def load(k, plane):
            return work[i, plane, k]

        def store(k, plane, value):
            work[i, plane, k] = value

        observed = []
        for k in range(at_once):
            observed.append(jnp.concatenate([rest_ref[:, at_once * i + k, :]] * 4, axis=0).T)
        shrink_pixels(observed, grad_ref, pred_ref, load, store)
        rest_copy(i).start()
        return carry

    lax.fori_loop(0, work.shape[0], pair, 0)
    for n in range(count):
        early_copy(n).wait()
    for i in range(work.shape[0]):
        rest_copy(i).wait()


def merge_profiles(early_parts, rest, grad, pred, shape):
    _, rows, cols, cells = shape
    at_once = 2
    steps = rest.shape[1] // at_once
    count = len(early_parts)
    vmem = pl.BlockSpec(memory_space=pltpu.VMEM)
    return pl.pallas_call(
        functools.partial(merge_kernel, count),
        in_specs=[vmem] * (count + 3),
        out_specs=pl.BlockSpec(memory_space=pl.ANY),
        out_shape=jax.ShapeDtypeStruct(shape, jnp.float32),
        scratch_shapes=[
            pltpu.VMEM((steps, 2, at_once, cols, cells), jnp.float32),
            pltpu.SemaphoreType.DMA((count,)),
            pltpu.SemaphoreType.DMA((steps,)),
        ],
        compiler_params=pltpu.CompilerParams(vmem_limit_bytes=MERGE_VMEM),
        name="merge",
    )(*early_parts, rest, grad, pred)


def split_high_low(matrix):
    high = matrix.astype(jnp.bfloat16)
    return high, (matrix - high.astype(jnp.float32)).astype(jnp.bfloat16)


def body(
    echo_record,
    along_track_kernel,
    slant_distance_kernel,
    vertical_lags,
    lateral_lags,
    orbit_source_survey,
    normal_spacings,
):
    ap_count = lax.axis_size("ap")
    pass_count = lax.axis_size("pass")
    rows = along_track_kernel.shape[1]
    cols = slant_distance_kernel.shape[2]
    strip = rows // ap_count
    own_rows = strip // pass_count
    chunks = max(1, min(CHUNKS, own_rows // 8))
    passes = normal_spacings.shape[0]
    swap = [(i, i ^ 1) for i in range(ap_count)]
    same_side = [[i for i in range(ap_count) if i % 2 == side] for side in range(2)]

    kernel_far = lax.ppermute(along_track_kernel, "ap", swap)
    shape = (2, own_rows, cols, HEIGHT_CELLS)
    direct = (
        pass_count == 2 and own_rows == 32 and ap_count % 4 == 0 and cols % 128 == 0
        and cols == 256 and EARLY == 3 and passes == 16
    )
    if direct:
        focus, padded, grad, pred = prepare(
            lateral_lags, orbit_source_survey, normal_spacings, echo_record,
            slant_distance_kernel, along_track_kernel, SPAN * strip,
        )
        *early_parts, rest = gather_images(
            padded, kernel_far, focus, vertical_lags, grad, pred, strip, ap_count // 4, EARLY,
        )
        return merge_profiles(early_parts, rest, grad, pred, shape)
    focus = focus_range(echo_record, slant_distance_kernel, lateral_lags)
    focus_far = lax.ppermute(focus, "ap", swap)
    place, own_pass = lax.axis_index("ap"), lax.axis_index("pass")
    side = jnp.stack([place % 2, place // 2, own_pass]).astype(jnp.int32)

    inphase, quadrature = phasor_dictionary(normal_spacings, orbit_source_survey, HEIGHT_CELLS)
    adjoint = jnp.concatenate(
        [
            jnp.concatenate([inphase, -quadrature], axis=1),
            jnp.concatenate([quadrature, inphase], axis=1),
        ],
        axis=0,
    )
    grad_high, grad_low = split_high_low(adjoint / passes)
    grad = jnp.concatenate([grad_high, grad_high, grad_low, grad_low], axis=0)
    forward = (adjoint.T / HEIGHT_CELLS).astype(jnp.bfloat16)
    pred = jnp.concatenate([forward] * 4, axis=1)
    profile = None
    pieces = form_images(
        direct, along_track_kernel, kernel_far, focus, focus_far, vertical_lags, side,
        chunks, pass_count, strip,
    )

    arrived = []
    for piece in pieces:
        arrived.append(
            lax.all_to_all(
                piece, "ap", split_axis=0, concat_axis=0, axis_index_groups=same_side
            )
        )
    for c, received in enumerate(arrived):
        if profile is not None:
            received, profile = lax.optimization_barrier((received, profile))
        summed = jnp.sum(received.astype(jnp.float32), axis=0).astype(jnp.bfloat16)
        stacked = lax.all_to_all(summed, "pass", split_axis=2, concat_axis=1, tiled=True)
        y = stacked.reshape(2 * passes, -1)
        profile = shrink_chunk(c, chunks, y, grad, pred, profile, shape)
    return profile


def solution(mesh):
    return jax.shard_map(
        body,
        mesh=mesh,
        in_specs=(
            P(None, "pass", "ap", None),
            P(None, None, "ap"),
            P(),
            P("pass"),
            P("pass"),
            P(),
            P(),
        ),
        out_specs=P(None, ("ap", "pass"), None, None),
        check_vma=False,
    )
```

```python
import functools

import jax
import jax.numpy as jnp
from jax import lax
from jax.experimental import pallas as pl
from jax.experimental.pallas import tpu as pltpu
from jax.sharding import PartitionSpec as P

HEIGHT_CELLS = 512
ITERS = 4
SPAN = 2
CHUNKS = 4
EARLY = 3
GATHER_VMEM = 22 * 2**20
MERGE_VMEM = 9 * 2**20
MESH = pl.DeviceIdType.MESH

shrink_level = 0.1


def phasor_dictionary(normal_spacings, orbit_source_survey, height_cell_number):
    support_mask = (
        orbit_source_survey[:, None]
        == jnp.arange(normal_spacings.shape[0], dtype=jnp.int32)[None, :]
    ).astype(normal_spacings.dtype)
    chosen_height_cells = jnp.sum(support_mask * normal_spacings[None, :], axis=1)
    orbit_start_positions = (
        jnp.arange(height_cell_number).astype(normal_spacings.dtype) - height_cell_number // 2
    )
    phases = jnp.pi * chosen_height_cells[:, None] * orbit_start_positions[None, :]
    return (jnp.cos(phases), jnp.sin(phases))


def focus_kernel(lags_ref, echo_ref, slant_ref, out_ref):
    dot = functools.partial(jnp.dot, preferred_element_type=jnp.float32)
    echo_re, echo_im = echo_ref[0, 0], echo_ref[1, 0]
    slant_re, slant_im = slant_ref[0], slant_ref[1]
    lag = lags_ref[pl.program_id(0)]
    focus_re = dot(echo_re, slant_re) - dot(echo_im, slant_im)
    focus_im = dot(echo_re, slant_im) + dot(echo_im, slant_re)
    inside = lax.broadcasted_iota(jnp.int32, focus_re.shape, 1) >= lag
    for plane, values in enumerate((focus_re, focus_im)):
        moved = jnp.where(inside, pltpu.roll(values, lag, 1), 0.0)
        out_ref[plane, 0] = moved.astype(out_ref.dtype)


def focus_range(echo, slant, lateral_lags):
    _, passes, pulses, freqs = echo.shape
    cols = slant.shape[2]
    return pl.pallas_call(
        focus_kernel,
        grid_spec=pltpu.PrefetchScalarGridSpec(
            num_scalar_prefetch=1,
            grid=(passes,),
            in_specs=[
                pl.BlockSpec((2, 1, pulses, freqs), lambda p, lags: (0, p, 0, 0)),
                pl.BlockSpec((2, freqs, cols), lambda p, lags: (0, 0, 0)),
            ],
            out_specs=pl.BlockSpec((2, 1, pulses, cols), lambda p, lags: (0, p, 0, 0)),
        ),
        out_shape=jax.ShapeDtypeStruct((2, passes, pulses, cols), jnp.bfloat16),
        cost_estimate=pl.CostEstimate(
            flops=8 * passes * pulses * freqs * cols,
            bytes_accessed=6 * passes * pulses * freqs,
            transcendentals=0,
        ),
        name="focus",
    )(lateral_lags, echo, slant)


def image_kernel(direct, chunks, pass_count, strip, margin, lags_ref, side_ref, *refs):
    kernels, focuses = refs[0:2], refs[2:4]
    outs, padded = refs[4:-1], refs[-1]
    owners = kernels[0].shape[1] // strip // 2
    rows = kernels[0].shape[1]
    pulses = kernels[0].shape[2]
    cols = outs[0].shape[-1]

    @pl.when(pl.program_id(0) == 0)
    def _():
        for s in range(2):
            for plane in range(2):
                padded[2 * s + plane, 0:margin, :] = jnp.zeros((margin, pulses), jnp.float32)
                padded[2 * s + plane, margin : margin + rows, :] = kernels[s][plane].astype(
                    jnp.float32
                )

    base = margin - lags_ref[pl.program_id(0)] + side_ref[0] * strip
    half = strip // pass_count
    starts = []
    for o in range(owners):
        if direct:
            first = base + 2 * lax.rem(side_ref[1] + o, owners) * strip
            for q in range(pass_count):
                starts.append((first + lax.rem(side_ref[2] + q, pass_count) * half, half))
        else:
            starts.append((base + 2 * o * strip, strip))
    total_re = jnp.zeros((owners * strip, cols), jnp.float32)
    total_im = jnp.zeros((owners * strip, cols), jnp.float32)
    dot = functools.partial(jnp.dot, preferred_element_type=jnp.float32)
    for s in range(2):
        kernel_re, kernel_im = (
            jnp.concatenate(
                [padded[2 * s + plane, pl.ds(start, size), :] for start, size in starts],
                axis=0,
            ).astype(jnp.bfloat16)
            for plane in range(2)
        )
        focus_re, focus_im = focuses[s][0, 0], focuses[s][1, 0]
        if pulses % 128 == 0:
            both = jnp.concatenate([kernel_re, kernel_im], axis=1)
            total_re += dot(both, jnp.concatenate([focus_re, -focus_im], axis=0))
            total_im += dot(both, jnp.concatenate([focus_im, focus_re], axis=0))
        else:
            total_re += dot(kernel_re, focus_re) - dot(kernel_im, focus_im)
            total_im += dot(kernel_re, focus_im) + dot(kernel_im, focus_re)
    height = strip // pass_count // chunks
    for plane, total in enumerate((total_re, total_im)):
        if chunks == 1 and not direct:
            outs[0][:, plane, 0] = total.reshape(owners, strip, cols).astype(jnp.bfloat16)
        else:
            split = total.reshape(owners, pass_count, chunks, height, cols)
            for c in range(chunks):
                part = split[:, :, c].reshape(owners, pass_count * height, cols)
                part = part.astype(jnp.bfloat16)
                if direct:
                    for o in range(owners):
                        outs[c * owners + o][plane, 0] = part[o]
                else:
                    outs[c][:, plane, 0] = part


def form_images(direct, kernel, kernel_far, focus, focus_far, vertical_lags, side, chunks, pass_count, strip):
    _, rows, pulses = kernel.shape
    passes, cols = focus.shape[1], focus.shape[3]
    owners = rows // strip // 2
    margin = SPAN * strip
    piece = strip // chunks
    whole = pl.BlockSpec((2, rows, pulses), lambda p, *_: (0, 0, 0))
    one = pl.BlockSpec((2, 1, pulses, cols), lambda p, *_: (0, p, 0, 0))
    if direct:
        out_specs = [pl.BlockSpec((2, 1, piece, cols), lambda p, *_: (0, p, 0, 0))]
        out_shape = [jax.ShapeDtypeStruct((2, passes, piece, cols), jnp.bfloat16)]
        out_specs, out_shape = out_specs * (chunks * owners), out_shape * (chunks * owners)
    else:
        out_specs = [pl.BlockSpec((owners, 2, 1, piece, cols), lambda p, *_: (0, 0, p, 0, 0))]
        out_shape = [jax.ShapeDtypeStruct((owners, 2, passes, piece, cols), jnp.bfloat16)]
        out_specs, out_shape = out_specs * chunks, out_shape * chunks
    return pl.pallas_call(
        functools.partial(image_kernel, direct, chunks, pass_count, strip, margin),
        grid_spec=pltpu.PrefetchScalarGridSpec(
            num_scalar_prefetch=2,
            grid=(passes,),
            in_specs=[whole, whole, one, one],
            out_specs=out_specs,
            scratch_shapes=[pltpu.VMEM((4, margin + rows, pulses), jnp.float32)],
        ),
        out_shape=out_shape,
        cost_estimate=pl.CostEstimate(
            flops=8 * passes * pulses * rows * cols,
            bytes_accessed=2 * passes * rows * cols,
            transcendentals=0,
        ),
        name="image",
    )(vertical_lags, side, kernel, kernel_far, focus, focus_far)


def shrink_kernel(rows_at_once, y_ref, grad_ref, pred_ref, *refs):
    out_ref = refs[-1]
    cells = out_ref.shape[3]
    cols = out_ref.shape[2]
    width = grad_ref.shape[0]
    block = width // 4
    dot = functools.partial(jnp.dot, preferred_element_type=jnp.float32)
    coarse = (lax.broadcasted_iota(jnp.int32, (cols, width), 1) // block) % 2 == 0
    observed = []
    for i in range(rows_at_once):
        y = y_ref[:, i * cols : (i + 1) * cols].astype(jnp.float32)
        observed.append(jnp.concatenate([y] * 4, axis=0).T)
    resid = list(observed)
    for sweep in range(ITERS):
        for i in range(rows_at_once):
            high = resid[i].astype(jnp.bfloat16)
            low = (resid[i] - high.astype(jnp.float32)).astype(jnp.bfloat16)
            moving = jnp.where(coarse, high, low)
            planes = []
            for plane in range(2):
                v = dot(moving, grad_ref[:, plane * cells : (plane + 1) * cells])
                if sweep > 0:
                    v += out_ref[plane, i]
                u = v - jnp.clip(v, -shrink_level, shrink_level)
                out_ref[plane, i] = u
                planes.append(u.astype(jnp.bfloat16))
            if sweep < ITERS - 1:
                resid[i] = observed[i] - dot(jnp.concatenate(planes, axis=1), pred_ref[...])


def shrink_chunk(c, chunks, y, grad, pred, profile, shape):
    _, rows, cols, cells = shape
    height = rows // chunks
    rows_at_once = 2 if height % 2 == 0 else 1
    steps = height // rows_at_once
    width, span = grad.shape
    specs = [
        pl.BlockSpec((y.shape[0], rows_at_once * cols), lambda i: (0, i)),
        pl.BlockSpec((width, span), lambda i: (0, 0)),
        pl.BlockSpec((span, width), lambda i: (0, 0)),
    ]
    operands = [y, grad, pred]
    aliases = {}
    if profile is not None:
        specs.append(pl.BlockSpec(memory_space=pl.ANY))
        operands.append(profile)
        aliases = {3: 0}
    return pl.pallas_call(
        functools.partial(shrink_kernel, rows_at_once),
        grid=(steps,),
        in_specs=specs,
        out_specs=pl.BlockSpec(
            (2, rows_at_once, cols, cells), lambda i: (0, c * steps + i, 0, 0)
        ),
        out_shape=jax.ShapeDtypeStruct(shape, jnp.float32),
        input_output_aliases=aliases,
        cost_estimate=pl.CostEstimate(
            flops=7 * 2 * height * cols * span * 256,
            bytes_accessed=8 * height * cols * cells,
            transcendentals=0,
        ),
        name="shrink_%d" % c,
    )(*operands)


def shrink_pixels(observed, grad_ref, pred_ref, load, store):
    pixels, width = observed[0].shape
    cells = grad_ref.shape[1] // 2
    dot = functools.partial(jnp.dot, preferred_element_type=jnp.float32)
    coarse = (lax.broadcasted_iota(jnp.int32, (pixels, width), 1) // (width // 4)) % 2 == 0
    resid = list(observed)
    for sweep in range(ITERS):
        for i in range(len(observed)):
            high = resid[i].astype(jnp.bfloat16)
            low = (resid[i] - high.astype(jnp.float32)).astype(jnp.bfloat16)
            moving = jnp.where(coarse, high, low)
            planes = []
            for plane in range(2):
                v = dot(moving, grad_ref[:, plane * cells : (plane + 1) * cells])
                if sweep > 0:
                    v += load(i, plane)
                u = v - jnp.clip(v, -shrink_level, shrink_level)
                store(i, plane, u)
                planes.append(u.astype(jnp.bfloat16))
            if sweep < ITERS - 1:
                resid[i] = observed[i] - dot(jnp.concatenate(planes, axis=1), pred_ref[...])


def gather_kernel(
    sizes, *refs
):
    strip, own_rows, margin, levels, groups, halves, early = sizes
    sources, refs = refs[:7], refs[7:]
    early_refs, (rest_ref, grad_ref, pred_ref) = refs[:early], refs[early : early + 3]
    held, refs = refs[early + 3 : early + 10], refs[early + 10 :]
    lags_ref, side_lags_ref, survey_ref, spacings_ref, kernel_near, slant_ref, echo_ref = held
    (
        padded_near, padded_far, kernel_far, focus_near, focus_far,
        keep, send, land, mid, zland, ready,
    ) = refs[:11]
    l_in, k_out, k_in, f_out, f_in, x_out, x_in, z_out, z_in = refs[11:]
    copies = [
        pltpu.make_async_copy(source, target, l_in.at[n])
        for n, (source, target) in enumerate(zip(sources, held))
    ]
    for copy in copies[::-1]:
        copy.start()
    rows, pulses = kernel_far.shape[1:]
    passes, freqs, cols = echo_ref.shape[1], echo_ref.shape[3], slant_ref.shape[2]
    part = passes // 2
    place, plane_y = lax.axis_index("ap"), lax.axis_index("pass")
    core, x, z = place % 2, (place // 2) % 2, place // 4
    peer_core = (place + 1 - 2 * core, plane_y)
    peer_x = (place + 2 - 4 * x, plane_y)
    others = [(d, q) for d in range(levels) for q in range(2) if d + q > 0]
    peer = {
        (d, q): (lax.rem(z + d, levels) * 4 + place % 4, plane_y + q - 2 * q * plane_y)
        for d, q in others
    }
    barrier = pltpu.get_barrier_semaphore()
    for target in [peer_core, peer_x] + [peer[t] for t in others]:
        pl.semaphore_signal(barrier, inc=1, device_id=target, device_id_type=MESH)
    pl.semaphore_wait(barrier, len(others) + 2)

    def copy_focus(p):
        return pltpu.make_async_remote_copy(
            src_ref=focus_near.at[p], dst_ref=focus_far.at[p],
            send_sem=f_out.at[p], recv_sem=f_in.at[p],
            device_id=peer_core, device_id_type=MESH,
        )

    def copy_x(e):
        return pltpu.make_async_remote_copy(
            src_ref=send.at[e], dst_ref=land.at[e], send_sem=x_out.at[e], recv_sem=x_in.at[e],
            device_id=peer_x, device_id_type=MESH,
        )

    def copy_z(e, d, q):
        return pltpu.make_async_remote_copy(
            src_ref=mid.at[e, d, q], dst_ref=zland.at[e, d, q],
            send_sem=z_out.at[e, d, q], recv_sem=z_in.at[e, d, q],
            device_id=peer[d, q], device_id_type=MESH,
        )

    swap_kernel = pltpu.make_async_remote_copy(
        src_ref=sources[4], dst_ref=kernel_far, send_sem=k_out.at[0], recv_sem=k_in.at[0],
        device_id=peer_core, device_id_type=MESH,
    )
    swap_kernel.start()
    for copy in (copies[1], copies[5], copies[6]):
        copy.wait()
    dot = functools.partial(jnp.dot, preferred_element_type=jnp.float32)
    slant_re, slant_im = slant_ref[0], slant_ref[1]
    into = (
        jnp.concatenate([slant_re, -slant_im], axis=0),
        jnp.concatenate([slant_im, slant_re], axis=0),
    )
    at_once = 4 if passes % 4 == 0 else 1
    for first in range(0, passes, at_once):
        taken = jnp.concatenate(
            [echo_ref[n, first : first + at_once].reshape(at_once * pulses, freqs) for n in range(2)],
            axis=1,
        )
        for plane in range(2):
            values = dot(taken, into[plane])
            for n in range(at_once):
                lag = side_lags_ref[first + n]
                one = values[n * pulses : (n + 1) * pulses]
                inside = lax.broadcasted_iota(jnp.int32, one.shape, 1) >= lag
                moved = jnp.where(inside, pltpu.roll(one, lag, 1), 0.0)
                focus_near[first + n, plane] = moved.astype(jnp.bfloat16)
        for n in range(at_once):
            copy_focus(first + n).start()
    for copy in (copies[0], copies[2], copies[3], copies[4], swap_kernel):
        copy.wait()
    for target, source in ((padded_near, kernel_near), (padded_far, kernel_far)):
        for n in range(2):
            target[n, 0:margin, :] = jnp.zeros((margin, pulses), jnp.float32)
            target[n, margin : margin + rows, :] = source[n].astype(jnp.float32)

    def dictionary():
        total = survey_ref.shape[0]
        cells = grad_ref.shape[1] // 2
        own = lax.axis_index("pass")
        row = lax.broadcasted_iota(jnp.int32, (total, cells), 0)
        chosen = jnp.zeros((total, cells), jnp.float32)
        for k in range(total):
            value = spacings_ref[survey_ref[lax.rem(k + own * (total // 2), total)]]
            chosen = jnp.where(row == k, value, chosen)
        place = lax.broadcasted_iota(jnp.int32, (total, cells), 1) - cells // 2
        phases = jnp.pi * chosen * place.astype(jnp.float32)
        inphase, quadrature = jnp.cos(phases), jnp.sin(phases)
        adjoint = jnp.concatenate(
            [
                jnp.concatenate([inphase, -quadrature], axis=1),
                jnp.concatenate([quadrature, inphase], axis=1),
            ],
            axis=0,
        )
        high, low = split_high_low(adjoint / total)
        grad_ref[...] = jnp.concatenate([high, high, low, low], axis=0)
        pred_ref[...] = jnp.concatenate([adjoint / cells] * 4, axis=0).T.astype(jnp.bfloat16)

    def form(g):
        def one(n, p, carry):
            base = margin - lags_ref[p] + g * 8
            starts = []
            for side in range(2):
                for d in range(levels):
                    owner = lax.rem(z + d, levels) * 4 + lax.rem(x + side, 2) * 2 + core
                    for q in range(2):
                        starts.append(base + owner * strip + lax.rem(plane_y + q, 2) * own_rows)
            parts = []
            for ref in (padded_near, padded_far):
                for plane in range(2):
                    parts.append(
                        jnp.concatenate([ref[plane, pl.ds(start, 8), :] for start in starts], axis=0)
                        .astype(jnp.bfloat16)
                    )
            taken = jnp.concatenate(parts, axis=1)
            if g == 0:
                copy_focus(p).wait()
            near_re, near_im = focus_near[p, 0], focus_near[p, 1]
            far_re, far_im = focus_far[p, 0], focus_far[p, 1]
            out_re = dot(taken, jnp.concatenate([near_re, -near_im, far_re, -far_im], axis=0))
            out_im = dot(taken, jnp.concatenate([near_im, near_re, far_im, far_re], axis=0))
            for plane, out in enumerate((out_re, out_im)):
                out = out.astype(jnp.bfloat16)
                start = 0
                for buffer in (keep, send):
                    for d in range(levels):
                        for q in range(2):
                            for h in range(halves):
                                buffer[(2 * g + n) * halves + h, d, q, plane, p - n * part] = out[
                                    start : start + 8, 128 * h : 128 * h + 128
                                ]
                            start += 8
            return carry

        for n in range(2):
            lax.fori_loop(n * part, n * part + part, functools.partial(one, n), 0)
            for h in range(halves):
                copy_x((2 * g + n) * halves + h).start()

    def reduce_x(e):
        copy_x(e).wait()
        for d, q in others:
            total = keep[e, d, q].astype(jnp.float32) + land[e, d, q].astype(jnp.float32)
            mid[e, d, q] = total.astype(jnp.bfloat16)
        for d, q in others:
            copy_z(e, d, q).start()

    def reduce_z(e):
        c, n = e // (2 * halves) * halves + e % halves, e // halves % 2
        for d, q in others:
            copy_z(e, d, q).wait()
        for q in range(2):
            total = None if q else keep[e, 0, 0].astype(jnp.float32) + land[e, 0, 0].astype(jnp.float32)
            for d in range(1 - q, levels):
                term = zland[e, d, q].astype(jnp.float32)
                total = term if total is None else total + term
            ready[c, :, q, pl.ds(n * part, part)] = total.astype(jnp.bfloat16).astype(jnp.float32)

    def observe(c, r):
        y = ready[c, :, :, :, r, :].reshape(4 * passes, 128)
        return jnp.concatenate([y] * 4, axis=0).T

    def shrink(g, e):
        c, i = e // 2, e % 2
        h = c % halves
        early_ref = early_refs[g]

        def where(k):
            columns = pl.ds(pl.multiple_of(128 * h, 128), 128)
            return pl.ds(i * 4 + 2 * k, 2), columns

        def load(k, plane):
            rows_of, cols_of = where(k)
            return early_ref[plane, rows_of, cols_of, :].reshape(256, -1)

        def store(k, plane, value):
            rows_of, cols_of = where(k)
            early_ref[plane, rows_of, cols_of, :] = value.reshape(2, 128, -1)

        observed = []
        for k in range(2):
            r = i * 4 + 2 * k
            observed.append(jnp.concatenate([observe(c, r), observe(c, r + 1)], axis=0))
        shrink_pixels(observed, grad_ref, pred_ref, load, store)

    count = 2 * groups * halves

    form(0)
    dictionary()
    reduce_x(0)
    form(1)
    reduce_x(1)
    form(2)
    reduce_x(2)
    form(3)
    reduce_z(0)
    reduce_x(3)
    reduce_z(1)
    for g in range(early):

        def steady(e, carry):
            reduce_x(e)
            reduce_z(e - 2)
            shrink(g, e - 4)
            return carry

        lax.fori_loop(4 + 4 * g, 8 + 4 * g, steady, 0)
    reduce_z(count - 2)
    reduce_z(count - 1)
    for g in range(early, groups):
        for h in range(halves):
            rest_ref[:, (g - early) * 8 : (g - early) * 8 + 8, 128 * h : 128 * h + 128] = (
                ready[g * halves + h].reshape(4 * passes, 8, 128)
            )


def gather_images(
    echo, kernel, slant, vertical_lags, lateral_lags, survey, spacings, strip, levels, early
):
    _, rows, pulses = kernel.shape
    passes, cols, total = echo.shape[1], slant.shape[2], survey.shape[0]
    focus = jax.ShapeDtypeStruct((passes, 2, pulses, cols), jnp.bfloat16)
    operands = (vertical_lags, lateral_lags, survey, spacings, kernel, slant, echo)
    cells = HEIGHT_CELLS
    own_rows = strip // 2
    groups, halves = own_rows // 8, cols // 128
    count = groups * halves
    margin = SPAN * strip
    sizes = (strip, own_rows, margin, levels, groups, halves, early)
    vmem = pl.BlockSpec(memory_space=pltpu.VMEM)
    block = (2, passes // 2, 8, 128)
    dma = pltpu.SemaphoreType.DMA
    return pl.pallas_call(
        functools.partial(gather_kernel, sizes),
        in_specs=[pl.BlockSpec(memory_space=pltpu.HBM)] * 7,
        out_specs=[vmem] * (early + 3),
        out_shape=[
            jax.ShapeDtypeStruct((2, 8, cols, cells), jnp.float32)
            for _ in range(early)
        ] + [
            jax.ShapeDtypeStruct((4 * passes, (groups - early) * 8, cols), jnp.float32),
            jax.ShapeDtypeStruct((8 * total, 2 * cells), jnp.bfloat16),
            jax.ShapeDtypeStruct((2 * cells, 8 * total), jnp.bfloat16),
        ],
        scratch_shapes=[pltpu.SMEM(v.shape, v.dtype) for v in operands[:4]]
        + [pltpu.VMEM(v.shape, v.dtype) for v in operands[4:]]
        + [pltpu.VMEM((2, margin + rows, pulses), jnp.float32)] * 2
        + [pltpu.VMEM(kernel.shape, jnp.bfloat16)]
        + [pltpu.VMEM(focus.shape, jnp.bfloat16)] * 2
        + [pltpu.VMEM((2 * count, levels, 2) + block, jnp.bfloat16)] * 5
        + [
            pltpu.VMEM((count, 2, 2, passes, 8, 128), jnp.float32),
            dma((7,)),
            dma((1,)),
            dma((1,)),
            dma((passes,)),
            dma((passes,)),
            dma((2 * count,)),
            dma((2 * count,)),
            dma((2 * count, levels, 2)),
            dma((2 * count, levels, 2)),
        ],
        compiler_params=pltpu.CompilerParams(
            collective_id=0, has_side_effects=True, vmem_limit_bytes=GATHER_VMEM
        ),
        name="gather",
    )(*(pltpu.with_memory_space_constraint(v, pltpu.HBM) for v in operands))


def merge_kernel(count, *refs):
    early_refs = refs[:count]
    rest_ref, grad_ref, pred_ref, out_ref, work, early_sems, rest_sems = refs[count:]
    height, at_once = early_refs[0].shape[1], work.shape[2]
    early = count * height

    def early_copy(n):
        return pltpu.make_async_copy(
            early_refs[n], out_ref.at[:, pl.ds(n * height, height)], early_sems.at[n]
        )

    def rest_copy(i):
        rows = pl.ds(early + at_once * i, at_once)
        return pltpu.make_async_copy(work.at[i], out_ref.at[:, rows], rest_sems.at[i])

    for n in range(count):
        early_copy(n).start()

    def pair(i, carry):
        def load(k, plane):
            return work[i, plane, k]

        def store(k, plane, value):
            work[i, plane, k] = value

        observed = []
        for k in range(at_once):
            observed.append(jnp.concatenate([rest_ref[:, at_once * i + k, :]] * 4, axis=0).T)
        shrink_pixels(observed, grad_ref, pred_ref, load, store)
        rest_copy(i).start()
        return carry

    lax.fori_loop(0, work.shape[0], pair, 0)
    for n in range(count):
        early_copy(n).wait()
    for i in range(work.shape[0]):
        rest_copy(i).wait()


def merge_profiles(early_parts, rest, grad, pred, shape):
    _, rows, cols, cells = shape
    at_once = 2
    steps = rest.shape[1] // at_once
    count = len(early_parts)
    vmem = pl.BlockSpec(memory_space=pltpu.VMEM)
    return pl.pallas_call(
        functools.partial(merge_kernel, count),
        in_specs=[vmem] * (count + 3),
        out_specs=pl.BlockSpec(memory_space=pl.ANY),
        out_shape=jax.ShapeDtypeStruct(shape, jnp.float32),
        scratch_shapes=[
            pltpu.VMEM((steps, 2, at_once, cols, cells), jnp.float32),
            pltpu.SemaphoreType.DMA((count,)),
            pltpu.SemaphoreType.DMA((steps,)),
        ],
        compiler_params=pltpu.CompilerParams(vmem_limit_bytes=MERGE_VMEM),
        name="merge",
    )(*early_parts, rest, grad, pred)


def split_high_low(matrix):
    high = matrix.astype(jnp.bfloat16)
    return high, (matrix - high.astype(jnp.float32)).astype(jnp.bfloat16)


def body(
    echo_record,
    along_track_kernel,
    slant_distance_kernel,
    vertical_lags,
    lateral_lags,
    orbit_source_survey,
    normal_spacings,
):
    ap_count = lax.axis_size("ap")
    pass_count = lax.axis_size("pass")
    rows = along_track_kernel.shape[1]
    cols = slant_distance_kernel.shape[2]
    strip = rows // ap_count
    own_rows = strip // pass_count
    chunks = max(1, min(CHUNKS, own_rows // 8))
    passes = normal_spacings.shape[0]
    swap = [(i, i ^ 1) for i in range(ap_count)]
    same_side = [[i for i in range(ap_count) if i % 2 == side] for side in range(2)]

    shape = (2, own_rows, cols, HEIGHT_CELLS)
    direct = (
        pass_count == 2 and own_rows == 32 and ap_count % 4 == 0 and cols % 128 == 0
        and cols == 256 and EARLY == 3 and passes == 16
    )
    if direct:
        *early_parts, rest, grad, pred = gather_images(
            echo_record, along_track_kernel, slant_distance_kernel, vertical_lags, lateral_lags,
            orbit_source_survey, normal_spacings, strip, ap_count // 4, EARLY,
        )
        return merge_profiles(early_parts, rest, grad, pred, shape)
    kernel_far = lax.ppermute(along_track_kernel, "ap", swap)
    focus = focus_range(echo_record, slant_distance_kernel, lateral_lags)
    focus_far = lax.ppermute(focus, "ap", swap)
    place, own_pass = lax.axis_index("ap"), lax.axis_index("pass")
    side = jnp.stack([place % 2, place // 2, own_pass]).astype(jnp.int32)

    inphase, quadrature = phasor_dictionary(normal_spacings, orbit_source_survey, HEIGHT_CELLS)
    adjoint = jnp.concatenate(
        [
            jnp.concatenate([inphase, -quadrature], axis=1),
            jnp.concatenate([quadrature, inphase], axis=1),
        ],
        axis=0,
    )
    grad_high, grad_low = split_high_low(adjoint / passes)
    grad = jnp.concatenate([grad_high, grad_high, grad_low, grad_low], axis=0)
    forward = (adjoint.T / HEIGHT_CELLS).astype(jnp.bfloat16)
    pred = jnp.concatenate([forward] * 4, axis=1)
    profile = None
    pieces = form_images(
        direct, along_track_kernel, kernel_far, focus, focus_far, vertical_lags, side,
        chunks, pass_count, strip,
    )

    arrived = []
    for piece in pieces:
        arrived.append(
            lax.all_to_all(
                piece, "ap", split_axis=0, concat_axis=0, axis_index_groups=same_side
            )
        )
    for c, received in enumerate(arrived):
        if profile is not None:
            received, profile = lax.optimization_barrier((received, profile))
        summed = jnp.sum(received.astype(jnp.float32), axis=0).astype(jnp.bfloat16)
        stacked = lax.all_to_all(summed, "pass", split_axis=2, concat_axis=1, tiled=True)
        y = stacked.reshape(2 * passes, -1)
        profile = shrink_chunk(c, chunks, y, grad, pred, profile, shape)
    return profile


def solution(mesh):
    return jax.shard_map(
        body,
        mesh=mesh,
        in_specs=(
            P(None, "pass", "ap", None),
            P(None, None, "ap"),
            P(),
            P("pass"),
            P("pass"),
            P(),
            P(),
        ),
        out_specs=P(None, ("ap", "pass"), None, None),
        check_vma=False,
    )
```

```python
import functools

import jax
import jax.numpy as jnp
from jax import lax
from jax.experimental import pallas as pl
from jax.experimental.pallas import tpu as pltpu
from jax.sharding import PartitionSpec as P

HEIGHT_CELLS = 512
ITERS = 4
SPAN = 2
CHUNKS = 4
EARLY = 3
GATHER_VMEM = 22 * 2**20
MERGE_VMEM = 9 * 2**20
MESH = pl.DeviceIdType.MESH

shrink_level = 0.1


def phasor_dictionary(normal_spacings, orbit_source_survey, height_cell_number):
    support_mask = (
        orbit_source_survey[:, None]
        == jnp.arange(normal_spacings.shape[0], dtype=jnp.int32)[None, :]
    ).astype(normal_spacings.dtype)
    chosen_height_cells = jnp.sum(support_mask * normal_spacings[None, :], axis=1)
    orbit_start_positions = (
        jnp.arange(height_cell_number).astype(normal_spacings.dtype) - height_cell_number // 2
    )
    phases = jnp.pi * chosen_height_cells[:, None] * orbit_start_positions[None, :]
    return (jnp.cos(phases), jnp.sin(phases))


def focus_kernel(lags_ref, echo_ref, slant_ref, out_ref):
    dot = functools.partial(jnp.dot, preferred_element_type=jnp.float32)
    echo_re, echo_im = echo_ref[0, 0], echo_ref[1, 0]
    slant_re, slant_im = slant_ref[0], slant_ref[1]
    lag = lags_ref[pl.program_id(0)]
    focus_re = dot(echo_re, slant_re) - dot(echo_im, slant_im)
    focus_im = dot(echo_re, slant_im) + dot(echo_im, slant_re)
    inside = lax.broadcasted_iota(jnp.int32, focus_re.shape, 1) >= lag
    for plane, values in enumerate((focus_re, focus_im)):
        moved = jnp.where(inside, pltpu.roll(values, lag, 1), 0.0)
        out_ref[plane, 0] = moved.astype(out_ref.dtype)


def focus_range(echo, slant, lateral_lags):
    _, passes, pulses, freqs = echo.shape
    cols = slant.shape[2]
    return pl.pallas_call(
        focus_kernel,
        grid_spec=pltpu.PrefetchScalarGridSpec(
            num_scalar_prefetch=1,
            grid=(passes,),
            in_specs=[
                pl.BlockSpec((2, 1, pulses, freqs), lambda p, lags: (0, p, 0, 0)),
                pl.BlockSpec((2, freqs, cols), lambda p, lags: (0, 0, 0)),
            ],
            out_specs=pl.BlockSpec((2, 1, pulses, cols), lambda p, lags: (0, p, 0, 0)),
        ),
        out_shape=jax.ShapeDtypeStruct((2, passes, pulses, cols), jnp.bfloat16),
        cost_estimate=pl.CostEstimate(
            flops=8 * passes * pulses * freqs * cols,
            bytes_accessed=6 * passes * pulses * freqs,
            transcendentals=0,
        ),
        name="focus",
    )(lateral_lags, echo, slant)


def image_kernel(direct, chunks, pass_count, strip, margin, lags_ref, side_ref, *refs):
    kernels, focuses = refs[0:2], refs[2:4]
    outs, padded = refs[4:-1], refs[-1]
    owners = kernels[0].shape[1] // strip // 2
    rows = kernels[0].shape[1]
    pulses = kernels[0].shape[2]
    cols = outs[0].shape[-1]

    @pl.when(pl.program_id(0) == 0)
    def _():
        for s in range(2):
            for plane in range(2):
                padded[2 * s + plane, 0:margin, :] = jnp.zeros((margin, pulses), jnp.float32)
                padded[2 * s + plane, margin : margin + rows, :] = kernels[s][plane].astype(
                    jnp.float32
                )

    base = margin - lags_ref[pl.program_id(0)] + side_ref[0] * strip
    half = strip // pass_count
    starts = []
    for o in range(owners):
        if direct:
            first = base + 2 * lax.rem(side_ref[1] + o, owners) * strip
            for q in range(pass_count):
                starts.append((first + lax.rem(side_ref[2] + q, pass_count) * half, half))
        else:
            starts.append((base + 2 * o * strip, strip))
    total_re = jnp.zeros((owners * strip, cols), jnp.float32)
    total_im = jnp.zeros((owners * strip, cols), jnp.float32)
    dot = functools.partial(jnp.dot, preferred_element_type=jnp.float32)
    for s in range(2):
        kernel_re, kernel_im = (
            jnp.concatenate(
                [padded[2 * s + plane, pl.ds(start, size), :] for start, size in starts],
                axis=0,
            ).astype(jnp.bfloat16)
            for plane in range(2)
        )
        focus_re, focus_im = focuses[s][0, 0], focuses[s][1, 0]
        if pulses % 128 == 0:
            both = jnp.concatenate([kernel_re, kernel_im], axis=1)
            total_re += dot(both, jnp.concatenate([focus_re, -focus_im], axis=0))
            total_im += dot(both, jnp.concatenate([focus_im, focus_re], axis=0))
        else:
            total_re += dot(kernel_re, focus_re) - dot(kernel_im, focus_im)
            total_im += dot(kernel_re, focus_im) + dot(kernel_im, focus_re)
    height = strip // pass_count // chunks
    for plane, total in enumerate((total_re, total_im)):
        if chunks == 1 and not direct:
            outs[0][:, plane, 0] = total.reshape(owners, strip, cols).astype(jnp.bfloat16)
        else:
            split = total.reshape(owners, pass_count, chunks, height, cols)
            for c in range(chunks):
                part = split[:, :, c].reshape(owners, pass_count * height, cols)
                part = part.astype(jnp.bfloat16)
                if direct:
                    for o in range(owners):
                        outs[c * owners + o][plane, 0] = part[o]
                else:
                    outs[c][:, plane, 0] = part


def form_images(direct, kernel, kernel_far, focus, focus_far, vertical_lags, side, chunks, pass_count, strip):
    _, rows, pulses = kernel.shape
    passes, cols = focus.shape[1], focus.shape[3]
    owners = rows // strip // 2
    margin = SPAN * strip
    piece = strip // chunks
    whole = pl.BlockSpec((2, rows, pulses), lambda p, *_: (0, 0, 0))
    one = pl.BlockSpec((2, 1, pulses, cols), lambda p, *_: (0, p, 0, 0))
    if direct:
        out_specs = [pl.BlockSpec((2, 1, piece, cols), lambda p, *_: (0, p, 0, 0))]
        out_shape = [jax.ShapeDtypeStruct((2, passes, piece, cols), jnp.bfloat16)]
        out_specs, out_shape = out_specs * (chunks * owners), out_shape * (chunks * owners)
    else:
        out_specs = [pl.BlockSpec((owners, 2, 1, piece, cols), lambda p, *_: (0, 0, p, 0, 0))]
        out_shape = [jax.ShapeDtypeStruct((owners, 2, passes, piece, cols), jnp.bfloat16)]
        out_specs, out_shape = out_specs * chunks, out_shape * chunks
    return pl.pallas_call(
        functools.partial(image_kernel, direct, chunks, pass_count, strip, margin),
        grid_spec=pltpu.PrefetchScalarGridSpec(
            num_scalar_prefetch=2,
            grid=(passes,),
            in_specs=[whole, whole, one, one],
            out_specs=out_specs,
            scratch_shapes=[pltpu.VMEM((4, margin + rows, pulses), jnp.float32)],
        ),
        out_shape=out_shape,
        cost_estimate=pl.CostEstimate(
            flops=8 * passes * pulses * rows * cols,
            bytes_accessed=2 * passes * rows * cols,
            transcendentals=0,
        ),
        name="image",
    )(vertical_lags, side, kernel, kernel_far, focus, focus_far)


def shrink_kernel(rows_at_once, y_ref, grad_ref, pred_ref, *refs):
    out_ref = refs[-1]
    cells = out_ref.shape[3]
    cols = out_ref.shape[2]
    width = grad_ref.shape[0]
    block = width // 4
    dot = functools.partial(jnp.dot, preferred_element_type=jnp.float32)
    coarse = (lax.broadcasted_iota(jnp.int32, (cols, width), 1) // block) % 2 == 0
    observed = []
    for i in range(rows_at_once):
        y = y_ref[:, i * cols : (i + 1) * cols].astype(jnp.float32)
        observed.append(jnp.concatenate([y] * 4, axis=0).T)
    resid = list(observed)
    for sweep in range(ITERS):
        for i in range(rows_at_once):
            high = resid[i].astype(jnp.bfloat16)
            low = (resid[i] - high.astype(jnp.float32)).astype(jnp.bfloat16)
            moving = jnp.where(coarse, high, low)
            planes = []
            for plane in range(2):
                v = dot(moving, grad_ref[:, plane * cells : (plane + 1) * cells])
                if sweep > 0:
                    v += out_ref[plane, i]
                u = v - jnp.clip(v, -shrink_level, shrink_level)
                out_ref[plane, i] = u
                planes.append(u.astype(jnp.bfloat16))
            if sweep < ITERS - 1:
                resid[i] = observed[i] - dot(jnp.concatenate(planes, axis=1), pred_ref[...])


def shrink_chunk(c, chunks, y, grad, pred, profile, shape):
    _, rows, cols, cells = shape
    height = rows // chunks
    rows_at_once = 2 if height % 2 == 0 else 1
    steps = height // rows_at_once
    width, span = grad.shape
    specs = [
        pl.BlockSpec((y.shape[0], rows_at_once * cols), lambda i: (0, i)),
        pl.BlockSpec((width, span), lambda i: (0, 0)),
        pl.BlockSpec((span, width), lambda i: (0, 0)),
    ]
    operands = [y, grad, pred]
    aliases = {}
    if profile is not None:
        specs.append(pl.BlockSpec(memory_space=pl.ANY))
        operands.append(profile)
        aliases = {3: 0}
    return pl.pallas_call(
        functools.partial(shrink_kernel, rows_at_once),
        grid=(steps,),
        in_specs=specs,
        out_specs=pl.BlockSpec(
            (2, rows_at_once, cols, cells), lambda i: (0, c * steps + i, 0, 0)
        ),
        out_shape=jax.ShapeDtypeStruct(shape, jnp.float32),
        input_output_aliases=aliases,
        cost_estimate=pl.CostEstimate(
            flops=7 * 2 * height * cols * span * 256,
            bytes_accessed=8 * height * cols * cells,
            transcendentals=0,
        ),
        name="shrink_%d" % c,
    )(*operands)


def shrink_pixels(observed, grad_ref, pred_ref, load, store):
    pixels, width = observed[0].shape
    cells = grad_ref.shape[1] // 2
    dot = functools.partial(jnp.dot, preferred_element_type=jnp.float32)
    coarse = (lax.broadcasted_iota(jnp.int32, (pixels, width), 1) // (width // 4)) % 2 == 0
    resid = list(observed)
    for sweep in range(ITERS):
        for i in range(len(observed)):
            high = resid[i].astype(jnp.bfloat16)
            low = (resid[i] - high.astype(jnp.float32)).astype(jnp.bfloat16)
            moving = jnp.where(coarse, high, low)
            planes = []
            for plane in range(2):
                v = dot(moving, grad_ref[:, plane * cells : (plane + 1) * cells])
                if sweep > 0:
                    v += load(i, plane)
                u = v - jnp.clip(v, -shrink_level, shrink_level)
                store(i, plane, u)
                planes.append(u.astype(jnp.bfloat16))
            if sweep < ITERS - 1:
                resid[i] = observed[i] - dot(jnp.concatenate(planes, axis=1), pred_ref[...])


def gather_kernel(
    sizes, *refs
):
    strip, own_rows, margin, levels, groups, halves, early = sizes
    sources, refs = refs[:7], refs[7:]
    early_refs, (rest_ref, grad_ref, pred_ref) = refs[:early], refs[early : early + 3]
    held, refs = refs[early + 3 : early + 10], refs[early + 10 :]
    lags_ref, side_lags_ref, survey_ref, spacings_ref, kernel_near, slant_ref, echo_ref = held
    (
        padded_near, padded_far, kernel_far, focus_near, focus_far,
        keep, send, land, mid, zland, ready,
    ) = refs[:11]
    l_in, k_out, k_in, f_out, f_in, x_out, x_in, z_out, z_in = refs[11:]
    copies = [
        pltpu.make_async_copy(source, target, l_in.at[n])
        for n, (source, target) in enumerate(zip(sources, held))
    ]
    for copy in copies[::-1]:
        copy.start()
    rows, pulses = kernel_far.shape[1:]
    passes, freqs, cols = echo_ref.shape[1], echo_ref.shape[3], slant_ref.shape[2]
    part = passes // 2
    place, plane_y = lax.axis_index("ap"), lax.axis_index("pass")
    core, x, z = place % 2, (place // 2) % 2, place // 4
    peer_core = (place + 1 - 2 * core, plane_y)
    peer_x = (place + 2 - 4 * x, plane_y)
    others = [(d, q) for d in range(levels) for q in range(2) if d + q > 0]
    peer = {
        (d, q): (lax.rem(z + d, levels) * 4 + place % 4, plane_y + q - 2 * q * plane_y)
        for d, q in others
    }
    barrier = pltpu.get_barrier_semaphore()
    for target in [peer_core, peer_x] + [peer[t] for t in others]:
        pl.semaphore_signal(barrier, inc=1, device_id=target, device_id_type=MESH)
    pl.semaphore_wait(barrier, len(others) + 2)

    def copy_focus(p):
        return pltpu.make_async_remote_copy(
            src_ref=focus_near.at[p], dst_ref=focus_far.at[p],
            send_sem=f_out.at[p], recv_sem=f_in.at[p],
            device_id=peer_core, device_id_type=MESH,
        )

    def copy_x(e):
        return pltpu.make_async_remote_copy(
            src_ref=send.at[e], dst_ref=land.at[e], send_sem=x_out.at[e], recv_sem=x_in.at[e],
            device_id=peer_x, device_id_type=MESH,
        )

    def copy_z(e, d, q):
        return pltpu.make_async_remote_copy(
            src_ref=mid.at[e, d, q], dst_ref=zland.at[e, d, q],
            send_sem=z_out.at[e, d, q], recv_sem=z_in.at[e, d, q],
            device_id=peer[d, q], device_id_type=MESH,
        )

    swap_kernel = pltpu.make_async_remote_copy(
        src_ref=sources[4], dst_ref=kernel_far, send_sem=k_out.at[0], recv_sem=k_in.at[0],
        device_id=peer_core, device_id_type=MESH,
    )
    swap_kernel.start()
    for copy in (copies[1], copies[5], copies[6]):
        copy.wait()
    dot = functools.partial(jnp.dot, preferred_element_type=jnp.float32)
    slant_re, slant_im = slant_ref[0], slant_ref[1]
    into = (
        jnp.concatenate([slant_re, -slant_im], axis=0),
        jnp.concatenate([slant_im, slant_re], axis=0),
    )
    at_once = 4 if passes % 4 == 0 else 1
    for first in range(0, passes, at_once):
        taken = jnp.concatenate(
            [echo_ref[n, first : first + at_once].reshape(at_once * pulses, freqs) for n in range(2)],
            axis=1,
        )
        for plane in range(2):
            values = dot(taken, into[plane])
            for n in range(at_once):
                lag = side_lags_ref[first + n]
                one = values[n * pulses : (n + 1) * pulses]
                inside = lax.broadcasted_iota(jnp.int32, one.shape, 1) >= lag
                moved = jnp.where(inside, pltpu.roll(one, lag, 1), 0.0)
                focus_near[first + n, plane] = moved.astype(jnp.bfloat16)
        for n in range(at_once):
            copy_focus(first + n).start()
    for copy in (copies[0], copies[2], copies[3]):
        copy.wait()
    for target, source, copy in (
        (padded_near, kernel_near, copies[4]), (padded_far, kernel_far, swap_kernel)
    ):
        copy.wait()
        for n in range(2):
            target[n, 0:margin, :] = jnp.zeros((margin, pulses), jnp.float32)
            target[n, margin : margin + rows, :] = source[n].astype(jnp.float32)

    def dictionary():
        total = survey_ref.shape[0]
        cells = grad_ref.shape[1] // 2
        own = lax.axis_index("pass")
        row = lax.broadcasted_iota(jnp.int32, (total, cells), 0)
        chosen = jnp.zeros((total, cells), jnp.float32)
        for k in range(total):
            value = spacings_ref[survey_ref[lax.rem(k + own * (total // 2), total)]]
            chosen = jnp.where(row == k, value, chosen)
        place = lax.broadcasted_iota(jnp.int32, (total, cells), 1) - cells // 2
        phases = jnp.pi * chosen * place.astype(jnp.float32)
        inphase, quadrature = jnp.cos(phases), jnp.sin(phases)
        adjoint = jnp.concatenate(
            [
                jnp.concatenate([inphase, -quadrature], axis=1),
                jnp.concatenate([quadrature, inphase], axis=1),
            ],
            axis=0,
        )
        high, low = split_high_low(adjoint / total)
        grad_ref[...] = jnp.concatenate([high, high, low, low], axis=0)
        pred_ref[...] = jnp.concatenate([adjoint / cells] * 4, axis=0).T.astype(jnp.bfloat16)

    def form(g):
        def one(n, p, carry):
            base = margin - lags_ref[p] + g * 8
            starts = []
            for side in range(2):
                for d in range(levels):
                    owner = lax.rem(z + d, levels) * 4 + lax.rem(x + side, 2) * 2 + core
                    for q in range(2):
                        starts.append(base + owner * strip + lax.rem(plane_y + q, 2) * own_rows)
            parts = []
            for ref in (padded_near, padded_far):
                for plane in range(2):
                    parts.append(
                        jnp.concatenate([ref[plane, pl.ds(start, 8), :] for start in starts], axis=0)
                        .astype(jnp.bfloat16)
                    )
            taken = jnp.concatenate(parts, axis=1)
            if g == 0:
                copy_focus(p).wait()
            near_re, near_im = focus_near[p, 0], focus_near[p, 1]
            far_re, far_im = focus_far[p, 0], focus_far[p, 1]
            out_re = dot(taken, jnp.concatenate([near_re, -near_im, far_re, -far_im], axis=0))
            out_im = dot(taken, jnp.concatenate([near_im, near_re, far_im, far_re], axis=0))
            for plane, out in enumerate((out_re, out_im)):
                out = out.astype(jnp.bfloat16)
                start = 0
                for buffer in (keep, send):
                    for d in range(levels):
                        for q in range(2):
                            for h in range(halves):
                                buffer[(2 * g + n) * halves + h, d, q, plane, p - n * part] = out[
                                    start : start + 8, 128 * h : 128 * h + 128
                                ]
                            start += 8
            return carry

        for n in range(2):
            lax.fori_loop(n * part, n * part + part, functools.partial(one, n), 0)
            for h in range(halves):
                copy_x((2 * g + n) * halves + h).start()

    def reduce_x(e):
        copy_x(e).wait()
        for d, q in others:
            total = keep[e, d, q].astype(jnp.float32) + land[e, d, q].astype(jnp.float32)
            mid[e, d, q] = total.astype(jnp.bfloat16)
        for d, q in others[::-1]:
            copy_z(e, d, q).start()

    def reduce_z(e):
        c, n = e // (2 * halves) * halves + e % halves, e // halves % 2
        for d, q in others:
            copy_z(e, d, q).wait()
        for q in range(2):
            total = None if q else keep[e, 0, 0].astype(jnp.float32) + land[e, 0, 0].astype(jnp.float32)
            for d in range(1 - q, levels):
                term = zland[e, d, q].astype(jnp.float32)
                total = term if total is None else total + term
            ready[c, :, q, pl.ds(n * part, part)] = total.astype(jnp.bfloat16).astype(jnp.float32)

    def observe(c, r):
        y = ready[c, :, :, :, r, :].reshape(4 * passes, 128)
        return jnp.concatenate([y] * 4, axis=0).T

    def shrink(g, e):
        c, i = e // 2, e % 2
        h = c % halves
        early_ref = early_refs[g]

        def where(k):
            columns = pl.ds(pl.multiple_of(128 * h, 128), 128)
            return pl.ds(i * 4 + 2 * k, 2), columns

        def load(k, plane):
            rows_of, cols_of = where(k)
            return early_ref[plane, rows_of, cols_of, :].reshape(256, -1)

        def store(k, plane, value):
            rows_of, cols_of = where(k)
            early_ref[plane, rows_of, cols_of, :] = value.reshape(2, 128, -1)

        observed = []
        for k in range(2):
            r = i * 4 + 2 * k
            observed.append(jnp.concatenate([observe(c, r), observe(c, r + 1)], axis=0))
        shrink_pixels(observed, grad_ref, pred_ref, load, store)

    count = 2 * groups * halves

    form(0)
    reduce_x(0)
    form(1)
    reduce_x(1)
    dictionary()
    form(2)
    reduce_x(2)
    form(3)
    reduce_z(0)
    reduce_x(3)
    reduce_z(1)
    for g in range(early):

        def steady(e, carry):
            reduce_x(e)
            reduce_z(e - 2)
            shrink(g, e - 4)
            return carry

        lax.fori_loop(4 + 4 * g, 8 + 4 * g, steady, 0)
    reduce_z(count - 2)
    reduce_z(count - 1)
    for g in range(early, groups):
        for h in range(halves):
            rest_ref[:, (g - early) * 8 : (g - early) * 8 + 8, 128 * h : 128 * h + 128] = (
                ready[g * halves + h].reshape(4 * passes, 8, 128)
            )


def gather_images(
    echo, kernel, slant, vertical_lags, lateral_lags, survey, spacings, strip, levels, early
):
    _, rows, pulses = kernel.shape
    passes, cols, total = echo.shape[1], slant.shape[2], survey.shape[0]
    focus = jax.ShapeDtypeStruct((passes, 2, pulses, cols), jnp.bfloat16)
    operands = (vertical_lags, lateral_lags, survey, spacings, kernel, slant, echo)
    cells = HEIGHT_CELLS
    own_rows = strip // 2
    groups, halves = own_rows // 8, cols // 128
    count = groups * halves
    margin = SPAN * strip
    sizes = (strip, own_rows, margin, levels, groups, halves, early)
    vmem = pl.BlockSpec(memory_space=pltpu.VMEM)
    block = (2, passes // 2, 8, 128)
    dma = pltpu.SemaphoreType.DMA
    return pl.pallas_call(
        functools.partial(gather_kernel, sizes),
        in_specs=[pl.BlockSpec(memory_space=pltpu.HBM)] * 7,
        out_specs=[vmem] * (early + 3),
        out_shape=[
            jax.ShapeDtypeStruct((2, 8, cols, cells), jnp.float32)
            for _ in range(early)
        ] + [
            jax.ShapeDtypeStruct((4 * passes, (groups - early) * 8, cols), jnp.float32),
            jax.ShapeDtypeStruct((8 * total, 2 * cells), jnp.bfloat16),
            jax.ShapeDtypeStruct((2 * cells, 8 * total), jnp.bfloat16),
        ],
        scratch_shapes=[pltpu.SMEM(v.shape, v.dtype) for v in operands[:4]]
        + [pltpu.VMEM(v.shape, v.dtype) for v in operands[4:]]
        + [pltpu.VMEM((2, margin + rows, pulses), jnp.float32)] * 2
        + [pltpu.VMEM(kernel.shape, jnp.bfloat16)]
        + [pltpu.VMEM(focus.shape, jnp.bfloat16)] * 2
        + [pltpu.VMEM((2 * count, levels, 2) + block, jnp.bfloat16)] * 5
        + [
            pltpu.VMEM((count, 2, 2, passes, 8, 128), jnp.float32),
            dma((7,)),
            dma((1,)),
            dma((1,)),
            dma((passes,)),
            dma((passes,)),
            dma((2 * count,)),
            dma((2 * count,)),
            dma((2 * count, levels, 2)),
            dma((2 * count, levels, 2)),
        ],
        compiler_params=pltpu.CompilerParams(
            collective_id=0, has_side_effects=True, vmem_limit_bytes=GATHER_VMEM
        ),
        name="gather",
    )(*(pltpu.with_memory_space_constraint(v, pltpu.HBM) for v in operands))


def merge_kernel(count, *refs):
    early_refs = refs[:count]
    rest_ref, grad_ref, pred_ref, out_ref, work, early_sems, rest_sems = refs[count:]
    height, at_once = early_refs[0].shape[1], work.shape[2]
    early = count * height

    def early_copy(n):
        return pltpu.make_async_copy(
            early_refs[n], out_ref.at[:, pl.ds(n * height, height)], early_sems.at[n]
        )

    def rest_copy(i):
        rows = pl.ds(early + at_once * i, at_once)
        return pltpu.make_async_copy(work.at[i], out_ref.at[:, rows], rest_sems.at[i])

    for n in range(count):
        early_copy(n).start()

    def pair(i, carry):
        def load(k, plane):
            return work[i, plane, k]

        def store(k, plane, value):
            work[i, plane, k] = value

        observed = []
        for k in range(at_once):
            observed.append(jnp.concatenate([rest_ref[:, at_once * i + k, :]] * 4, axis=0).T)
        shrink_pixels(observed, grad_ref, pred_ref, load, store)
        rest_copy(i).start()
        return carry

    lax.fori_loop(0, work.shape[0], pair, 0)
    for n in range(count):
        early_copy(n).wait()
    for i in range(work.shape[0]):
        rest_copy(i).wait()


def merge_profiles(early_parts, rest, grad, pred, shape):
    _, rows, cols, cells = shape
    at_once = 2
    steps = rest.shape[1] // at_once
    count = len(early_parts)
    vmem = pl.BlockSpec(memory_space=pltpu.VMEM)
    return pl.pallas_call(
        functools.partial(merge_kernel, count),
        in_specs=[vmem] * (count + 3),
        out_specs=pl.BlockSpec(memory_space=pl.ANY),
        out_shape=jax.ShapeDtypeStruct(shape, jnp.float32),
        scratch_shapes=[
            pltpu.VMEM((steps, 2, at_once, cols, cells), jnp.float32),
            pltpu.SemaphoreType.DMA((count,)),
            pltpu.SemaphoreType.DMA((steps,)),
        ],
        compiler_params=pltpu.CompilerParams(vmem_limit_bytes=MERGE_VMEM),
        name="merge",
    )(*early_parts, rest, grad, pred)


def split_high_low(matrix):
    high = matrix.astype(jnp.bfloat16)
    return high, (matrix - high.astype(jnp.float32)).astype(jnp.bfloat16)


def body(
    echo_record,
    along_track_kernel,
    slant_distance_kernel,
    vertical_lags,
    lateral_lags,
    orbit_source_survey,
    normal_spacings,
):
    ap_count = lax.axis_size("ap")
    pass_count = lax.axis_size("pass")
    rows = along_track_kernel.shape[1]
    cols = slant_distance_kernel.shape[2]
    strip = rows // ap_count
    own_rows = strip // pass_count
    chunks = max(1, min(CHUNKS, own_rows // 8))
    passes = normal_spacings.shape[0]
    swap = [(i, i ^ 1) for i in range(ap_count)]
    same_side = [[i for i in range(ap_count) if i % 2 == side] for side in range(2)]

    shape = (2, own_rows, cols, HEIGHT_CELLS)
    direct = (
        pass_count == 2 and own_rows == 32 and ap_count % 4 == 0 and cols % 128 == 0
        and cols == 256 and EARLY == 3 and passes == 16
    )
    if direct:
        *early_parts, rest, grad, pred = gather_images(
            echo_record, along_track_kernel, slant_distance_kernel, vertical_lags, lateral_lags,
            orbit_source_survey, normal_spacings, strip, ap_count // 4, EARLY,
        )
        return merge_profiles(early_parts, rest, grad, pred, shape)
    kernel_far = lax.ppermute(along_track_kernel, "ap", swap)
    focus = focus_range(echo_record, slant_distance_kernel, lateral_lags)
    focus_far = lax.ppermute(focus, "ap", swap)
    place, own_pass = lax.axis_index("ap"), lax.axis_index("pass")
    side = jnp.stack([place % 2, place // 2, own_pass]).astype(jnp.int32)

    inphase, quadrature = phasor_dictionary(normal_spacings, orbit_source_survey, HEIGHT_CELLS)
    adjoint = jnp.concatenate(
        [
            jnp.concatenate([inphase, -quadrature], axis=1),
            jnp.concatenate([quadrature, inphase], axis=1),
        ],
        axis=0,
    )
    grad_high, grad_low = split_high_low(adjoint / passes)
    grad = jnp.concatenate([grad_high, grad_high, grad_low, grad_low], axis=0)
    forward = (adjoint.T / HEIGHT_CELLS).astype(jnp.bfloat16)
    pred = jnp.concatenate([forward] * 4, axis=1)
    profile = None
    pieces = form_images(
        direct, along_track_kernel, kernel_far, focus, focus_far, vertical_lags, side,
        chunks, pass_count, strip,
    )

    arrived = []
    for piece in pieces:
        arrived.append(
            lax.all_to_all(
                piece, "ap", split_axis=0, concat_axis=0, axis_index_groups=same_side
            )
        )
    for c, received in enumerate(arrived):
        if profile is not None:
            received, profile = lax.optimization_barrier((received, profile))
        summed = jnp.sum(received.astype(jnp.float32), axis=0).astype(jnp.bfloat16)
        stacked = lax.all_to_all(summed, "pass", split_axis=2, concat_axis=1, tiled=True)
        y = stacked.reshape(2 * passes, -1)
        profile = shrink_chunk(c, chunks, y, grad, pred, profile, shape)
    return profile


def solution(mesh):
    return jax.shard_map(
        body,
        mesh=mesh,
        in_specs=(
            P(None, "pass", "ap", None),
            P(None, None, "ap"),
            P(),
            P("pass"),
            P("pass"),
            P(),
            P(),
        ),
        out_specs=P(None, ("ap", "pass"), None, None),
        check_vma=False,
    )
```

```python
import functools

import jax
import jax.numpy as jnp
from jax import lax
from jax.experimental import pallas as pl
from jax.experimental.pallas import tpu as pltpu
from jax.sharding import PartitionSpec as P

HEIGHT_CELLS = 512
ITERS = 4
SPAN = 2
CHUNKS = 4
EARLY = 3
GATHER_VMEM = 22 * 2**20
MERGE_VMEM = 9 * 2**20
MESH = pl.DeviceIdType.MESH

shrink_level = 0.1


def phasor_dictionary(normal_spacings, orbit_source_survey, height_cell_number):
    support_mask = (
        orbit_source_survey[:, None]
        == jnp.arange(normal_spacings.shape[0], dtype=jnp.int32)[None, :]
    ).astype(normal_spacings.dtype)
    chosen_height_cells = jnp.sum(support_mask * normal_spacings[None, :], axis=1)
    orbit_start_positions = (
        jnp.arange(height_cell_number).astype(normal_spacings.dtype) - height_cell_number // 2
    )
    phases = jnp.pi * chosen_height_cells[:, None] * orbit_start_positions[None, :]
    return (jnp.cos(phases), jnp.sin(phases))


def focus_kernel(lags_ref, echo_ref, slant_ref, out_ref):
    dot = functools.partial(jnp.dot, preferred_element_type=jnp.float32)
    echo_re, echo_im = echo_ref[0, 0], echo_ref[1, 0]
    slant_re, slant_im = slant_ref[0], slant_ref[1]
    lag = lags_ref[pl.program_id(0)]
    focus_re = dot(echo_re, slant_re) - dot(echo_im, slant_im)
    focus_im = dot(echo_re, slant_im) + dot(echo_im, slant_re)
    inside = lax.broadcasted_iota(jnp.int32, focus_re.shape, 1) >= lag
    for plane, values in enumerate((focus_re, focus_im)):
        moved = jnp.where(inside, pltpu.roll(values, lag, 1), 0.0)
        out_ref[plane, 0] = moved.astype(out_ref.dtype)


def focus_range(echo, slant, lateral_lags):
    _, passes, pulses, freqs = echo.shape
    cols = slant.shape[2]
    return pl.pallas_call(
        focus_kernel,
        grid_spec=pltpu.PrefetchScalarGridSpec(
            num_scalar_prefetch=1,
            grid=(passes,),
            in_specs=[
                pl.BlockSpec((2, 1, pulses, freqs), lambda p, lags: (0, p, 0, 0)),
                pl.BlockSpec((2, freqs, cols), lambda p, lags: (0, 0, 0)),
            ],
            out_specs=pl.BlockSpec((2, 1, pulses, cols), lambda p, lags: (0, p, 0, 0)),
        ),
        out_shape=jax.ShapeDtypeStruct((2, passes, pulses, cols), jnp.bfloat16),
        cost_estimate=pl.CostEstimate(
            flops=8 * passes * pulses * freqs * cols,
            bytes_accessed=6 * passes * pulses * freqs,
            transcendentals=0,
        ),
        name="focus",
    )(lateral_lags, echo, slant)


def image_kernel(direct, chunks, pass_count, strip, margin, lags_ref, side_ref, *refs):
    kernels, focuses = refs[0:2], refs[2:4]
    outs, padded = refs[4:-1], refs[-1]
    owners = kernels[0].shape[1] // strip // 2
    rows = kernels[0].shape[1]
    pulses = kernels[0].shape[2]
    cols = outs[0].shape[-1]

    @pl.when(pl.program_id(0) == 0)
    def _():
        for s in range(2):
            for plane in range(2):
                padded[2 * s + plane, 0:margin, :] = jnp.zeros((margin, pulses), jnp.float32)
                padded[2 * s + plane, margin : margin + rows, :] = kernels[s][plane].astype(
                    jnp.float32
                )

    base = margin - lags_ref[pl.program_id(0)] + side_ref[0] * strip
    half = strip // pass_count
    starts = []
    for o in range(owners):
        if direct:
            first = base + 2 * lax.rem(side_ref[1] + o, owners) * strip
            for q in range(pass_count):
                starts.append((first + lax.rem(side_ref[2] + q, pass_count) * half, half))
        else:
            starts.append((base + 2 * o * strip, strip))
    total_re = jnp.zeros((owners * strip, cols), jnp.float32)
    total_im = jnp.zeros((owners * strip, cols), jnp.float32)
    dot = functools.partial(jnp.dot, preferred_element_type=jnp.float32)
    for s in range(2):
        kernel_re, kernel_im = (
            jnp.concatenate(
                [padded[2 * s + plane, pl.ds(start, size), :] for start, size in starts],
                axis=0,
            ).astype(jnp.bfloat16)
            for plane in range(2)
        )
        focus_re, focus_im = focuses[s][0, 0], focuses[s][1, 0]
        if pulses % 128 == 0:
            both = jnp.concatenate([kernel_re, kernel_im], axis=1)
            total_re += dot(both, jnp.concatenate([focus_re, -focus_im], axis=0))
            total_im += dot(both, jnp.concatenate([focus_im, focus_re], axis=0))
        else:
            total_re += dot(kernel_re, focus_re) - dot(kernel_im, focus_im)
            total_im += dot(kernel_re, focus_im) + dot(kernel_im, focus_re)
    height = strip // pass_count // chunks
    for plane, total in enumerate((total_re, total_im)):
        if chunks == 1 and not direct:
            outs[0][:, plane, 0] = total.reshape(owners, strip, cols).astype(jnp.bfloat16)
        else:
            split = total.reshape(owners, pass_count, chunks, height, cols)
            for c in range(chunks):
                part = split[:, :, c].reshape(owners, pass_count * height, cols)
                part = part.astype(jnp.bfloat16)
                if direct:
                    for o in range(owners):
                        outs[c * owners + o][plane, 0] = part[o]
                else:
                    outs[c][:, plane, 0] = part


def form_images(direct, kernel, kernel_far, focus, focus_far, vertical_lags, side, chunks, pass_count, strip):
    _, rows, pulses = kernel.shape
    passes, cols = focus.shape[1], focus.shape[3]
    owners = rows // strip // 2
    margin = SPAN * strip
    piece = strip // chunks
    whole = pl.BlockSpec((2, rows, pulses), lambda p, *_: (0, 0, 0))
    one = pl.BlockSpec((2, 1, pulses, cols), lambda p, *_: (0, p, 0, 0))
    if direct:
        out_specs = [pl.BlockSpec((2, 1, piece, cols), lambda p, *_: (0, p, 0, 0))]
        out_shape = [jax.ShapeDtypeStruct((2, passes, piece, cols), jnp.bfloat16)]
        out_specs, out_shape = out_specs * (chunks * owners), out_shape * (chunks * owners)
    else:
        out_specs = [pl.BlockSpec((owners, 2, 1, piece, cols), lambda p, *_: (0, 0, p, 0, 0))]
        out_shape = [jax.ShapeDtypeStruct((owners, 2, passes, piece, cols), jnp.bfloat16)]
        out_specs, out_shape = out_specs * chunks, out_shape * chunks
    return pl.pallas_call(
        functools.partial(image_kernel, direct, chunks, pass_count, strip, margin),
        grid_spec=pltpu.PrefetchScalarGridSpec(
            num_scalar_prefetch=2,
            grid=(passes,),
            in_specs=[whole, whole, one, one],
            out_specs=out_specs,
            scratch_shapes=[pltpu.VMEM((4, margin + rows, pulses), jnp.float32)],
        ),
        out_shape=out_shape,
        cost_estimate=pl.CostEstimate(
            flops=8 * passes * pulses * rows * cols,
            bytes_accessed=2 * passes * rows * cols,
            transcendentals=0,
        ),
        name="image",
    )(vertical_lags, side, kernel, kernel_far, focus, focus_far)


def shrink_kernel(rows_at_once, y_ref, grad_ref, pred_ref, *refs):
    out_ref = refs[-1]
    cells = out_ref.shape[3]
    cols = out_ref.shape[2]
    width = grad_ref.shape[0]
    block = width // 4
    dot = functools.partial(jnp.dot, preferred_element_type=jnp.float32)
    coarse = (lax.broadcasted_iota(jnp.int32, (cols, width), 1) // block) % 2 == 0
    observed = []
    for i in range(rows_at_once):
        y = y_ref[:, i * cols : (i + 1) * cols].astype(jnp.float32)
        observed.append(jnp.concatenate([y] * 4, axis=0).T)
    resid = list(observed)
    for sweep in range(ITERS):
        for i in range(rows_at_once):
            high = resid[i].astype(jnp.bfloat16)
            low = (resid[i] - high.astype(jnp.float32)).astype(jnp.bfloat16)
            moving = jnp.where(coarse, high, low)
            planes = []
            for plane in range(2):
                v = dot(moving, grad_ref[:, plane * cells : (plane + 1) * cells])
                if sweep > 0:
                    v += out_ref[plane, i]
                u = v - jnp.clip(v, -shrink_level, shrink_level)
                out_ref[plane, i] = u
                planes.append(u.astype(jnp.bfloat16))
            if sweep < ITERS - 1:
                resid[i] = observed[i] - dot(jnp.concatenate(planes, axis=1), pred_ref[...])


def shrink_chunk(c, chunks, y, grad, pred, profile, shape):
    _, rows, cols, cells = shape
    height = rows // chunks
    rows_at_once = 2 if height % 2 == 0 else 1
    steps = height // rows_at_once
    width, span = grad.shape
    specs = [
        pl.BlockSpec((y.shape[0], rows_at_once * cols), lambda i: (0, i)),
        pl.BlockSpec((width, span), lambda i: (0, 0)),
        pl.BlockSpec((span, width), lambda i: (0, 0)),
    ]
    operands = [y, grad, pred]
    aliases = {}
    if profile is not None:
        specs.append(pl.BlockSpec(memory_space=pl.ANY))
        operands.append(profile)
        aliases = {3: 0}
    return pl.pallas_call(
        functools.partial(shrink_kernel, rows_at_once),
        grid=(steps,),
        in_specs=specs,
        out_specs=pl.BlockSpec(
            (2, rows_at_once, cols, cells), lambda i: (0, c * steps + i, 0, 0)
        ),
        out_shape=jax.ShapeDtypeStruct(shape, jnp.float32),
        input_output_aliases=aliases,
        cost_estimate=pl.CostEstimate(
            flops=7 * 2 * height * cols * span * 256,
            bytes_accessed=8 * height * cols * cells,
            transcendentals=0,
        ),
        name="shrink_%d" % c,
    )(*operands)


def shrink_pixels(observed, grad_ref, pred_ref, load, store):
    pixels, width = observed[0].shape
    cells = grad_ref.shape[1] // 2
    dot = functools.partial(jnp.dot, preferred_element_type=jnp.float32)
    coarse = (lax.broadcasted_iota(jnp.int32, (pixels, width), 1) // (width // 4)) % 2 == 0
    resid = list(observed)
    for sweep in range(ITERS):
        for i in range(len(observed)):
            high = resid[i].astype(jnp.bfloat16)
            low = (resid[i] - high.astype(jnp.float32)).astype(jnp.bfloat16)
            moving = jnp.where(coarse, high, low)
            planes = []
            for plane in range(2):
                v = dot(moving, grad_ref[:, plane * cells : (plane + 1) * cells])
                if sweep > 0:
                    v += load(i, plane)
                u = v - jnp.clip(v, -shrink_level, shrink_level)
                store(i, plane, u)
                planes.append(u.astype(jnp.bfloat16))
            if sweep < ITERS - 1:
                resid[i] = observed[i] - dot(jnp.concatenate(planes, axis=1), pred_ref[...])


def gather_kernel(
    sizes, *refs
):
    strip, own_rows, margin, levels, groups, halves, early = sizes
    sources, refs = refs[:7], refs[7:]
    early_refs, (rest_ref, grad_ref, pred_ref) = refs[:early], refs[early : early + 3]
    held, refs = refs[early + 3 : early + 10], refs[early + 10 :]
    lags_ref, side_lags_ref, survey_ref, spacings_ref, kernel_near, slant_ref, echo_ref = held
    (
        padded_near, padded_far, kernel_far, focus_near, focus_far,
        keep, send, land, mid, zland, ready,
    ) = refs[:11]
    l_in, k_out, k_in, f_out, f_in, x_out, x_in, z_out, z_in = refs[11:]
    copies = [
        pltpu.make_async_copy(source, target, l_in.at[n])
        for n, (source, target) in enumerate(zip(sources, held))
    ]
    for copy in copies[::-1]:
        copy.start()
    rows, pulses = kernel_far.shape[1:]
    passes, freqs, cols = echo_ref.shape[1], echo_ref.shape[3], slant_ref.shape[2]
    part = passes // 2
    place, plane_y = lax.axis_index("ap"), lax.axis_index("pass")
    core, x, z = place % 2, (place // 2) % 2, place // 4
    peer_core = (place + 1 - 2 * core, plane_y)
    peer_x = (place + 2 - 4 * x, plane_y)
    others = [(d, q) for d in range(levels) for q in range(2) if d + q > 0]
    peer = {
        (d, q): (lax.rem(z + d, levels) * 4 + place % 4, plane_y + q - 2 * q * plane_y)
        for d, q in others
    }
    barrier = pltpu.get_barrier_semaphore()
    for target in [peer_core, peer_x] + [peer[t] for t in others]:
        pl.semaphore_signal(barrier, inc=1, device_id=target, device_id_type=MESH)
    pl.semaphore_wait(barrier, len(others) + 2)

    def copy_focus(p):
        return pltpu.make_async_remote_copy(
            src_ref=focus_near.at[p], dst_ref=focus_far.at[p],
            send_sem=f_out.at[p], recv_sem=f_in.at[p],
            device_id=peer_core, device_id_type=MESH,
        )

    def copy_x(e):
        return pltpu.make_async_remote_copy(
            src_ref=send.at[e], dst_ref=land.at[e], send_sem=x_out.at[e], recv_sem=x_in.at[e],
            device_id=peer_x, device_id_type=MESH,
        )

    def copy_z(e, d, q):
        return pltpu.make_async_remote_copy(
            src_ref=mid.at[e, d, q], dst_ref=zland.at[e, d, q],
            send_sem=z_out.at[e, d, q], recv_sem=z_in.at[e, d, q],
            device_id=peer[d, q], device_id_type=MESH,
        )

    swap_kernel = pltpu.make_async_remote_copy(
        src_ref=sources[4], dst_ref=kernel_far, send_sem=k_out.at[0], recv_sem=k_in.at[0],
        device_id=peer_core, device_id_type=MESH,
    )
    swap_kernel.start()
    for copy in (copies[1], copies[5], copies[6]):
        copy.wait()
    dot = functools.partial(jnp.dot, preferred_element_type=jnp.float32)
    slant_re, slant_im = slant_ref[0], slant_ref[1]
    into = (
        jnp.concatenate([slant_re, -slant_im], axis=0),
        jnp.concatenate([slant_im, slant_re], axis=0),
    )
    at_once = 4 if passes % 4 == 0 else 1
    for first in range(0, passes, at_once):
        taken = jnp.concatenate(
            [echo_ref[n, first : first + at_once].reshape(at_once * pulses, freqs) for n in range(2)],
            axis=1,
        )
        for plane in range(2):
            values = dot(taken, into[plane])
            for n in range(at_once):
                lag = side_lags_ref[first + n]
                one = values[n * pulses : (n + 1) * pulses]
                inside = lax.broadcasted_iota(jnp.int32, one.shape, 1) >= lag
                moved = jnp.where(inside, pltpu.roll(one, lag, 1), 0.0)
                focus_near[first + n, plane] = moved.astype(jnp.bfloat16)
        for n in range(at_once):
            copy_focus(first + n).start()
    for copy in (copies[0], copies[2], copies[3], copies[4], swap_kernel):
        copy.wait()
    for target, source in ((padded_near, kernel_near), (padded_far, kernel_far)):
        for n in range(2):
            target[n, 0:margin, :] = jnp.zeros((margin, pulses), jnp.float32)
            target[n, margin : margin + rows, :] = source[n].astype(jnp.float32)

    def dictionary():
        total = survey_ref.shape[0]
        cells = grad_ref.shape[1] // 2
        own = lax.axis_index("pass")
        row = lax.broadcasted_iota(jnp.int32, (total, cells), 0)
        chosen = jnp.zeros((total, cells), jnp.float32)
        for k in range(total):
            value = spacings_ref[survey_ref[lax.rem(k + own * (total // 2), total)]]
            chosen = jnp.where(row == k, value, chosen)
        place = lax.broadcasted_iota(jnp.int32, (total, cells), 1) - cells // 2
        phases = jnp.pi * chosen * place.astype(jnp.float32)
        inphase, quadrature = jnp.cos(phases), jnp.sin(phases)
        adjoint = jnp.concatenate(
            [
                jnp.concatenate([inphase, -quadrature], axis=1),
                jnp.concatenate([quadrature, inphase], axis=1),
            ],
            axis=0,
        )
        high, low = split_high_low(adjoint / total)
        grad_ref[...] = jnp.concatenate([high, high, low, low], axis=0)
        pred_ref[...] = jnp.concatenate([adjoint / cells] * 4, axis=0).T.astype(jnp.bfloat16)

    def form(g):
        def one(n, p, carry):
            base = margin - lags_ref[p] + g * 8
            starts = []
            for side in range(2):
                for d in range(levels):
                    owner = lax.rem(z + d, levels) * 4 + lax.rem(x + side, 2) * 2 + core
                    for q in range(2):
                        starts.append(base + owner * strip + lax.rem(plane_y + q, 2) * own_rows)
            parts = []
            for ref in (padded_near, padded_far):
                for plane in range(2):
                    parts.append(
                        jnp.concatenate([ref[plane, pl.ds(start, 8), :] for start in starts], axis=0)
                        .astype(jnp.bfloat16)
                    )
            taken = jnp.concatenate(parts, axis=1)
            if g == 0:
                copy_focus(p).wait()
            near_re, near_im = focus_near[p, 0], focus_near[p, 1]
            far_re, far_im = focus_far[p, 0], focus_far[p, 1]
            out_re = dot(taken, jnp.concatenate([near_re, -near_im, far_re, -far_im], axis=0))
            out_im = dot(taken, jnp.concatenate([near_im, near_re, far_im, far_re], axis=0))
            for plane, out in enumerate((out_re, out_im)):
                out = out.astype(jnp.bfloat16)
                start = 0
                for buffer in (keep, send):
                    for d in range(levels):
                        for q in range(2):
                            for h in range(halves):
                                buffer[(2 * g + n) * halves + h, d, q, plane, p - n * part] = out[
                                    start : start + 8, 128 * h : 128 * h + 128
                                ]
                            start += 8
            return carry

        for n in range(2):
            lax.fori_loop(n * part, n * part + part, functools.partial(one, n), 0)
            for h in range(halves):
                copy_x((2 * g + n) * halves + h).start()

    def reduce_x(e):
        copy_x(e).wait()
        for d, q in others:
            total = keep[e, d, q].astype(jnp.float32) + land[e, d, q].astype(jnp.float32)
            mid[e, d, q] = total.astype(jnp.bfloat16)
        for d, q in others:
            copy_z(e, d, q).start()

    def reduce_z(e):
        c, n = e // (2 * halves) * halves + e % halves, e // halves % 2
        for d, q in others:
            copy_z(e, d, q).wait()
        for q in range(2):
            total = None if q else keep[e, 0, 0].astype(jnp.float32) + land[e, 0, 0].astype(jnp.float32)
            for d in range(1 - q, levels):
                term = zland[e, d, q].astype(jnp.float32)
                total = term if total is None else total + term
            ready[c, :, q, pl.ds(n * part, part)] = total.astype(jnp.bfloat16).astype(jnp.float32)

    def observe(c, r):
        y = ready[c, :, :, :, r, :].reshape(4 * passes, 128)
        return jnp.concatenate([y] * 4, axis=0).T

    def shrink(g, e):
        c, i = e // 2, e % 2
        h = c % halves
        early_ref = early_refs[g]

        def where(k):
            columns = pl.ds(pl.multiple_of(128 * h, 128), 128)
            return pl.ds(i * 4 + 2 * k, 2), columns

        def load(k, plane):
            rows_of, cols_of = where(k)
            return early_ref[plane, rows_of, cols_of, :].reshape(256, -1)

        def store(k, plane, value):
            rows_of, cols_of = where(k)
            early_ref[plane, rows_of, cols_of, :] = value.reshape(2, 128, -1)

        observed = []
        for k in range(2):
            r = i * 4 + 2 * k
            observed.append(jnp.concatenate([observe(c, r), observe(c, r + 1)], axis=0))
        shrink_pixels(observed, grad_ref, pred_ref, load, store)

    count = 2 * groups * halves

    form(0)
    reduce_x(0)
    form(1)
    reduce_x(1)
    dictionary()
    form(2)
    reduce_x(2)
    form(3)
    reduce_z(0)
    reduce_x(3)
    reduce_z(1)
    for g in range(early):

        def steady(e, carry):
            reduce_x(e)
            reduce_z(e - 2)
            shrink(g, e - 4)
            return carry

        lax.fori_loop(4 + 4 * g, 8 + 4 * g, steady, 0)
    reduce_z(count - 2)
    reduce_z(count - 1)
    for g in range(early, groups):
        for h in range(halves):
            rest_ref[:, (g - early) * 8 : (g - early) * 8 + 8, 128 * h : 128 * h + 128] = (
                ready[g * halves + h].reshape(4 * passes, 8, 128)
            )


def gather_images(
    echo, kernel, slant, vertical_lags, lateral_lags, survey, spacings, strip, levels, early
):
    _, rows, pulses = kernel.shape
    passes, cols, total = echo.shape[1], slant.shape[2], survey.shape[0]
    focus = jax.ShapeDtypeStruct((passes, 2, pulses, cols), jnp.bfloat16)
    operands = (vertical_lags, lateral_lags, survey, spacings, kernel, slant, echo)
    cells = HEIGHT_CELLS
    own_rows = strip // 2
    groups, halves = own_rows // 8, cols // 128
    count = groups * halves
    margin = SPAN * strip
    sizes = (strip, own_rows, margin, levels, groups, halves, early)
    vmem = pl.BlockSpec(memory_space=pltpu.VMEM)
    block = (2, passes // 2, 8, 128)
    dma = pltpu.SemaphoreType.DMA
    return pl.pallas_call(
        functools.partial(gather_kernel, sizes),
        in_specs=[pl.BlockSpec(memory_space=pltpu.HBM)] * 7,
        out_specs=[vmem] * (early + 3),
        out_shape=[
            jax.ShapeDtypeStruct((2, 8, cols, cells), jnp.float32)
            for _ in range(early)
        ] + [
            jax.ShapeDtypeStruct((4 * passes, (groups - early) * 8, cols), jnp.float32),
            jax.ShapeDtypeStruct((8 * total, 2 * cells), jnp.bfloat16),
            jax.ShapeDtypeStruct((2 * cells, 8 * total), jnp.bfloat16),
        ],
        scratch_shapes=[pltpu.SMEM(v.shape, v.dtype) for v in operands[:4]]
        + [pltpu.VMEM(v.shape, v.dtype) for v in operands[4:]]
        + [pltpu.VMEM((2, margin + rows, pulses), jnp.float32)] * 2
        + [pltpu.VMEM(kernel.shape, jnp.bfloat16)]
        + [pltpu.VMEM(focus.shape, jnp.bfloat16)] * 2
        + [pltpu.VMEM((2 * count, levels, 2) + block, jnp.bfloat16)] * 5
        + [
            pltpu.VMEM((count, 2, 2, passes, 8, 128), jnp.float32),
            dma((7,)),
            dma((1,)),
            dma((1,)),
            dma((passes,)),
            dma((passes,)),
            dma((2 * count,)),
            dma((2 * count,)),
            dma((2 * count, levels, 2)),
            dma((2 * count, levels, 2)),
        ],
        compiler_params=pltpu.CompilerParams(
            collective_id=0, has_side_effects=True, vmem_limit_bytes=GATHER_VMEM
        ),
        name="gather",
    )(*(pltpu.with_memory_space_constraint(v, pltpu.HBM) for v in operands))


def merge_kernel(count, *refs):
    early_refs = refs[:count]
    rest_ref, grad_ref, pred_ref, out_ref, work, early_sems, rest_sems = refs[count:]
    height, at_once = early_refs[0].shape[1], work.shape[2]
    early = count * height

    def early_copy(n):
        return pltpu.make_async_copy(
            early_refs[n], out_ref.at[:, pl.ds(n * height, height)], early_sems.at[n]
        )

    def rest_copy(i):
        rows = pl.ds(early + at_once * i, at_once)
        return pltpu.make_async_copy(work.at[i], out_ref.at[:, rows], rest_sems.at[i])

    for n in range(count):
        early_copy(n).start()

    def pair(i, carry):
        def load(k, plane):
            return work[i, plane, k]

        def store(k, plane, value):
            work[i, plane, k] = value

        observed = []
        for k in range(at_once):
            observed.append(jnp.concatenate([rest_ref[:, at_once * i + k, :]] * 4, axis=0).T)
        shrink_pixels(observed, grad_ref, pred_ref, load, store)
        rest_copy(i).start()
        return carry

    lax.fori_loop(0, work.shape[0], pair, 0)
    for n in range(count):
        early_copy(n).wait()
    for i in range(work.shape[0]):
        rest_copy(i).wait()


def merge_profiles(early_parts, rest, grad, pred, shape):
    _, rows, cols, cells = shape
    at_once = 2
    steps = rest.shape[1] // at_once
    count = len(early_parts)
    vmem = pl.BlockSpec(memory_space=pltpu.VMEM)
    return pl.pallas_call(
        functools.partial(merge_kernel, count),
        in_specs=[vmem] * (count + 3),
        out_specs=pl.BlockSpec(memory_space=pl.ANY),
        out_shape=jax.ShapeDtypeStruct(shape, jnp.float32),
        scratch_shapes=[
            pltpu.VMEM((steps, 2, at_once, cols, cells), jnp.float32),
            pltpu.SemaphoreType.DMA((count,)),
            pltpu.SemaphoreType.DMA((steps,)),
        ],
        compiler_params=pltpu.CompilerParams(vmem_limit_bytes=MERGE_VMEM),
        name="merge",
    )(*early_parts, rest, grad, pred)


def split_high_low(matrix):
    high = matrix.astype(jnp.bfloat16)
    return high, (matrix - high.astype(jnp.float32)).astype(jnp.bfloat16)


def body(
    echo_record,
    along_track_kernel,
    slant_distance_kernel,
    vertical_lags,
    lateral_lags,
    orbit_source_survey,
    normal_spacings,
):
    ap_count = lax.axis_size("ap")
    pass_count = lax.axis_size("pass")
    rows = along_track_kernel.shape[1]
    cols = slant_distance_kernel.shape[2]
    strip = rows // ap_count
    own_rows = strip // pass_count
    chunks = max(1, min(CHUNKS, own_rows // 8))
    passes = normal_spacings.shape[0]
    swap = [(i, i ^ 1) for i in range(ap_count)]
    same_side = [[i for i in range(ap_count) if i % 2 == side] for side in range(2)]

    shape = (2, own_rows, cols, HEIGHT_CELLS)
    direct = (
        pass_count == 2 and own_rows == 32 and ap_count % 4 == 0 and cols % 128 == 0
        and cols == 256 and EARLY == 3 and passes == 16
    )
    if direct:
        *early_parts, rest, grad, pred = gather_images(
            echo_record, along_track_kernel, slant_distance_kernel, vertical_lags, lateral_lags,
            orbit_source_survey, normal_spacings, strip, ap_count // 4, EARLY,
        )
        return merge_profiles(early_parts, rest, grad, pred, shape)
    kernel_far = lax.ppermute(along_track_kernel, "ap", swap)
    focus = focus_range(echo_record, slant_distance_kernel, lateral_lags)
    focus_far = lax.ppermute(focus, "ap", swap)
    place, own_pass = lax.axis_index("ap"), lax.axis_index("pass")
    side = jnp.stack([place % 2, place // 2, own_pass]).astype(jnp.int32)

    inphase, quadrature = phasor_dictionary(normal_spacings, orbit_source_survey, HEIGHT_CELLS)
    adjoint = jnp.concatenate(
        [
            jnp.concatenate([inphase, -quadrature], axis=1),
            jnp.concatenate([quadrature, inphase], axis=1),
        ],
        axis=0,
    )
    grad_high, grad_low = split_high_low(adjoint / passes)
    grad = jnp.concatenate([grad_high, grad_high, grad_low, grad_low], axis=0)
    forward = (adjoint.T / HEIGHT_CELLS).astype(jnp.bfloat16)
    pred = jnp.concatenate([forward] * 4, axis=1)
    profile = None
    pieces = form_images(
        direct, along_track_kernel, kernel_far, focus, focus_far, vertical_lags, side,
        chunks, pass_count, strip,
    )

    arrived = []
    for piece in pieces:
        arrived.append(
            lax.all_to_all(
                piece, "ap", split_axis=0, concat_axis=0, axis_index_groups=same_side
            )
        )
    for c, received in enumerate(arrived):
        if profile is not None:
            received, profile = lax.optimization_barrier((received, profile))
        summed = jnp.sum(received.astype(jnp.float32), axis=0).astype(jnp.bfloat16)
        stacked = lax.all_to_all(summed, "pass", split_axis=2, concat_axis=1, tiled=True)
        y = stacked.reshape(2 * passes, -1)
        profile = shrink_chunk(c, chunks, y, grad, pred, profile, shape)
    return profile


def solution(mesh):
    return jax.shard_map(
        body,
        mesh=mesh,
        in_specs=(
            P(None, "pass", "ap", None),
            P(None, None, "ap"),
            P(),
            P("pass"),
            P("pass"),
            P(),
            P(),
        ),
        out_specs=P(None, ("ap", "pass"), None, None),
        check_vma=False,
    )
```
